32 devices in a mesh: inst: 1 (over z), qy: 4 (over y), qx: 8 (over x, core).
Axes of the slice: x: 4, y: 4, z: 1, core: 2. Of those that a mesh axis runs over, the one named last changes fastest.
The devices are a block of a 4x4x8 slice.
Arguments:
- cost: float32 [2097152], P(('inst', 'qy', 'qx'))
- gamma: float32 [2, 3], P('inst')
- beta: float32 [2, 3], P('inst')
Outputs:
- output 1: float32 [2], P('inst')
- output 2: float32 [2, 6], P('inst')
All inputs are finite; a program needn't handle non-finite values.
Results may differ from the reference program's by a relative error of at most 0.001.
Values sent between devices are 32-bit elements.
A program may use at most 768 MiB of HBM per device.

```python
import functools
import jax
import jax.numpy as jnp
from jax import lax

QUBITS = 21
LAYERS = 3
DEGREE = 3


def bit_table(count):
    index = jnp.arange(2 ** count, dtype=jnp.int32)[:, None]
    return ((index >> jnp.arange(count, dtype=jnp.int32)[None, :]) & 1).astype(jnp.float32)


def cut_values(adjacency):
    low_count = QUBITS // 2
    high_count = QUBITS - low_count
    low_bits = bit_table(low_count)
    high_bits = bit_table(high_count)
    degrees = jnp.sum(adjacency, axis=1)
    highest = lax.Precision.HIGHEST
    low_term = jnp.dot(low_bits, degrees[:low_count], precision=highest) - jnp.sum(jnp.dot(low_bits, adjacency[:low_count, :low_count], precision=highest) * low_bits, axis=1)
    high_term = jnp.dot(high_bits, degrees[low_count:], precision=highest) - jnp.sum(jnp.dot(high_bits, adjacency[low_count:, low_count:], precision=highest) * high_bits, axis=1)
    cross_term = jnp.dot(jnp.dot(high_bits, adjacency[low_count:, :low_count], precision=highest), low_bits.T, precision=highest)
    cut = high_term[:, None] + low_term[None, :] - 2.0 * cross_term
    total_weight = 0.5 * jnp.sum(adjacency)
    spread = jnp.sqrt(0.5 * jnp.sum(adjacency * adjacency))
    return ((cut - 0.5 * total_weight) * (2.0 / spread)).reshape(-1)


def draw_cost(cost_key):
    key_dst, key_weight = jax.random.split(cost_key)
    num_edges = QUBITS * DEGREE // 2
    edge_src = jnp.arange(num_edges, dtype=jnp.int32) % QUBITS
    edge_dst = (edge_src + jax.random.randint(key_dst, (num_edges,), 1, QUBITS)) % QUBITS
    weight_tilt = 0.5 + (edge_src + edge_dst).astype(jnp.float32) / QUBITS
    edge_weight = jax.random.uniform(key_weight, (num_edges,), jnp.float32, 0.5, 1.5) * weight_tilt
    adjacency = jnp.zeros((QUBITS, QUBITS), jnp.float32).at[edge_src, edge_dst].add(edge_weight)
    return cut_values(adjacency + adjacency.T)


def setup_inputs(seed: int = 0, part: int = 0) -> dict:
    base_key = jax.random.fold_in(jax.random.key(seed), part)
    key_cost, key_gamma, key_beta = jax.random.split(base_key, 3)
    cost = draw_cost(key_cost)
    gamma = jax.random.uniform(key_gamma, (2, LAYERS), jnp.float32, 0.2, 1.0)
    beta = jax.random.uniform(key_beta, (2, LAYERS), jnp.float32, 0.6, 2.4)
    return {"cost": cost, "gamma": gamma, "beta": beta}


def flip_bit(amplitudes, qubit):
    return jnp.flip(amplitudes.reshape(-1, 2, 2 ** qubit), axis=1).reshape(-1)


def one_set(cost, angles):
    gamma_row, beta_row = angles
    start = jnp.full(cost.shape, 2.0 ** (-0.5 * QUBITS), jnp.float32)

    def forward_layer(state, layer_angles):
        psi_re, psi_im = state
        gamma_l, beta_l = layer_angles
        phase = gamma_l * cost
        cos_p = jnp.cos(phase)
        sin_p = jnp.sin(phase)
        psi_re, psi_im = psi_re * cos_p + psi_im * sin_p, psi_im * cos_p - psi_re * sin_p
        cos_b = jnp.cos(0.5 * beta_l)
        sin_b = jnp.sin(0.5 * beta_l)
        for qubit in range(QUBITS):
            flip_re = flip_bit(psi_re, qubit)
            flip_im = flip_bit(psi_im, qubit)
            psi_re, psi_im = cos_b * psi_re + sin_b * flip_im, cos_b * psi_im - sin_b * flip_re
        return (psi_re, psi_im), None

    final_state = lax.scan(forward_layer, (start, jnp.zeros_like(start)), (gamma_row, beta_row))[0]
    psi_re, psi_im = final_state
    energy = jnp.sum(cost * (psi_re * psi_re + psi_im * psi_im))

    def backward_layer(state, layer_angles):
        psi_re, psi_im, lam_re, lam_im = state
        gamma_l, beta_l = layer_angles
        cos_b = jnp.cos(0.5 * beta_l)
        sin_b = jnp.sin(0.5 * beta_l)
        beta_grad = jnp.zeros((), jnp.float32)
        for qubit in range(QUBITS):
            flip_psi_re = flip_bit(psi_re, qubit)
            flip_psi_im = flip_bit(psi_im, qubit)
            flip_lam_re = flip_bit(lam_re, qubit)
            flip_lam_im = flip_bit(lam_im, qubit)
            beta_grad = beta_grad + jnp.sum(lam_re * flip_psi_im - lam_im * flip_psi_re)
            psi_re, psi_im = cos_b * psi_re - sin_b * flip_psi_im, cos_b * psi_im + sin_b * flip_psi_re
            lam_re, lam_im = cos_b * lam_re - sin_b * flip_lam_im, cos_b * lam_im + sin_b * flip_lam_re
        gamma_grad = 2.0 * jnp.sum(cost * (lam_re * psi_im - lam_im * psi_re))
        phase = gamma_l * cost
        cos_p = jnp.cos(phase)
        sin_p = jnp.sin(phase)
        psi_re, psi_im = psi_re * cos_p - psi_im * sin_p, psi_im * cos_p + psi_re * sin_p
        lam_re, lam_im = lam_re * cos_p - lam_im * sin_p, lam_im * cos_p + lam_re * sin_p
        return (psi_re, psi_im, lam_re, lam_im), (gamma_grad, beta_grad)

    layer_grads = lax.scan(backward_layer, (psi_re, psi_im, cost * psi_re, cost * psi_im), (gamma_row, beta_row), reverse=True)[1]
    return energy, jnp.concatenate([layer_grads[0], layer_grads[1]])


def reference(cost, gamma, beta):
    energy, grad = lax.map(functools.partial(one_set, cost), (gamma, beta))
    return (energy, grad)
```

```python
import functools
import jax
import jax.numpy as jnp
from jax import lax
from jax.experimental import pallas as pl
from jax.experimental.pallas import tpu as pltpu
from jax.sharding import PartitionSpec as P

LANE = 128
LANE_BITS = 7
SUB = 8
MESH_ID = pl.DeviceIdType.MESH
F32 = jnp.float32
BF16 = jnp.bfloat16


def sincos(x):
    k = jnp.floor(x * 0.6366197723675814 + 0.5)
    r = ((x - k * 1.5703125) - k * 4.837512969970703125e-4) - k * 7.54978995489188216e-8
    z = r * r
    s = r + r * z * (-1.6666654611e-1 + z * (8.3321608736e-3 + z * -1.9515295891e-4))
    c = (1.0 - 0.5 * z) + z * z * (4.166664568298827e-2 + z * (-1.388731625493765e-3 + z * 2.443315711809948e-5))
    q = k.astype(jnp.int32)
    odd = (q & 1) != 0
    sin_v = jnp.where(odd, c, s)
    cos_v = jnp.where(odd, s, c)
    sin_v = jnp.where((q & 2) != 0, -sin_v, sin_v)
    cos_v = jnp.where(((q + 1) & 2) != 0, -cos_v, cos_v)
    return sin_v, cos_v


def split3(x):
    hi = x.astype(BF16)
    rest = x - hi.astype(F32)
    mid = rest.astype(BF16)
    low = (rest - mid.astype(F32)).astype(BF16)
    return hi, mid, low


def mm(a, b):
    return jnp.dot(a, b, preferred_element_type=F32)


def rot(pairs, stride, c, t):
    out = list(pairs)
    for j in range(len(pairs)):
        if j & stride:
            continue
        (ar, ai), (br, bi) = pairs[j], pairs[j | stride]
        out[j] = (c * ar + t * bi, c * ai - t * br)
        out[j | stride] = (c * br + t * ai, c * bi - t * ar)
    return out


def sub_flip(x, bit):
    if bit == 2:
        return pltpu.roll(x, 4, 0)
    row = lax.broadcasted_iota(jnp.int32, (SUB, LANE), 0)
    up = pltpu.roll(x, 1 << bit, 0)
    down = pltpu.roll(x, SUB - (1 << bit), 0)
    return jnp.where((row & (1 << bit)) != 0, up, down)


def make_kernel(ny, nx, num_sets, num_layers, rows, norm):
    n = ny * nx
    lo = 8
    hi = n // lo
    tiles = rows // SUB
    lo_bits = [1 << b for b in range(lo.bit_length() - 1)]
    hi_bits = [1 << b for b in range(hi.bit_length() - 1)]
    tile_bits = [1 << b for b in range(tiles.bit_length() - 1)]
    width_x = nx // 2

    def order(a):
        return 2 - a + (a // 2) * (7 - 2 * a)

    def kernel(cost_ref, gamma_ref, beta_ref, e_ref, g_ref,
               cost_b, src, dst, keep, tab, psi_b, psi_c, wmat, adj, dmat, ct, acc, mine, parts, tmp, send_sem, recv_sem):
        qy = lax.axis_index('qy')
        qx = lax.axis_index('qx')
        me = qy * nx + qx
        barrier = pltpu.get_barrier_semaphore()

        def each_peer(act):
            def body(i, _):
                ty = lax.rem(qy + order(i // (2 * width_x)), ny)
                tx = lax.rem(qx // 2 + order(lax.rem(i // 2, width_x)), width_x) * 2 + lax.rem(qx + 1 + i, 2)
                act(ty, tx)
                return 0
            lax.fori_loop(0, n - 1, body, 0)

        def greet(ty, tx):
            pl.semaphore_signal(barrier, inc=1, device_id={'qy': ty, 'qx': tx}, device_id_type=MESH_ID)
        each_peer(greet)

        def send(source, target, ids, ty, tx):
            pltpu.make_async_remote_copy(
                source, target, send_sem.at[ids], recv_sem.at[ids],
                device_id={'qy': ty, 'qx': tx}, device_id_type=MESH_ID).start()

        def exchange(source, target, ids):
            each_peer(lambda ty, tx: send(source.at[ty * nx + tx], target.at[me], ids, ty, tx))

        def wait_bytes(buf, sem):
            part = buf.at[pl.ds(0, n - 1)]
            pltpu.make_async_copy(part, part, sem).wait()

        def tile_d(r, _):
            a = lax.broadcasted_iota(jnp.int32, (SUB, LANE), 0) + r * SUB
            b = lax.broadcasted_iota(jnp.int32, (SUB, LANE), 1)
            x = a ^ b
            d = jnp.zeros_like(x)
            for k in range(LANE_BITS):
                d = d + ((x >> k) & 1)
            dmat[pl.ds(pl.multiple_of(r * SUB, SUB), SUB), :] = d
            return 0
        lax.fori_loop(0, LANE // SUB, tile_d, 0)
        one = (dmat[...] == 1).astype(F32).astype(BF16)
        zero = jnp.zeros((LANE, LANE), BF16)
        adj[0:LANE, 0:LANE] = one
        adj[0:LANE, LANE:] = zero
        adj[LANE:, 0:LANE] = zero
        adj[LANE:, LANE:] = one
        for s in range(num_sets):
            for l in range(num_layers):
                k = s * num_layers + l
                sin_h, cos_h = sincos(jnp.full((SUB, LANE), 0.5 * beta_ref[s, l], F32))
                ct[k, 0] = cos_h
                ct[k, 1] = sin_h
                ct[k, 2] = -sin_h

        def weights(k, slot):
            c, t = ct[k, 0], ct[k, 1]
            cp, tp = [jnp.ones_like(c)], [jnp.ones_like(c)]
            for _ in range(LANE_BITS):
                cp.append(cp[-1] * c)
                tp.append(tp[-1] * t)
            amp = [cp[LANE_BITS - d] * tp[d] for d in range(LANE_BITS + 1)]
            z = jnp.zeros_like(c)
            real = [z, z, z, z, z, z, z, z]
            imag = [z, z, z, z, z, z, z, z]
            for d in range(LANE_BITS + 1):
                if d % 4 == 0:
                    real[d] = amp[d]
                elif d % 4 == 1:
                    imag[d] = -amp[d]
                elif d % 4 == 2:
                    real[d] = -amp[d]
                else:
                    imag[d] = amp[d]

            def body(r, _):
                at = pl.multiple_of(r * 2 * SUB, 2 * SUB)
                rows_re, rows_im = [], []
                for h in range(2):
                    d = dmat[pl.ds(at + h * SUB, SUB), :]
                    re = z
                    im = z
                    for j in range(LANE_BITS + 1):
                        hit = d == j
                        if j % 2 == 0:
                            re = jnp.where(hit, real[j], re)
                        else:
                            im = jnp.where(hit, imag[j], im)
                    rows_re.append(re)
                    rows_im.append(im)
                re = jnp.concatenate(rows_re, axis=0)
                im = jnp.concatenate(rows_im, axis=0)
                for p, (a, b) in enumerate(zip(split3(re), split3(im))):
                    top = pl.ds(at, 2 * SUB)
                    bot = pl.ds(at + LANE, 2 * SUB)
                    wmat[slot, 0, p, top, 0:LANE] = a
                    wmat[slot, 0, p, top, LANE:] = b
                    wmat[slot, 0, p, bot, 0:LANE] = -b
                    wmat[slot, 0, p, bot, LANE:] = a
                    wmat[slot, 1, p, top, 0:LANE] = a
                    wmat[slot, 1, p, top, LANE:] = -b
                    wmat[slot, 1, p, bot, 0:LANE] = b
                    wmat[slot, 1, p, bot, LANE:] = a
                return 0
            lax.fori_loop(0, LANE // (2 * SUB), body, 0)

        def tile_rows(tile):
            return pl.ds(pl.multiple_of(tile * SUB, SUB), SUB)

        def load(ref, slot, tile):
            r = tile_rows(tile)
            return ref[slot, r, 0:LANE], ref[slot, r, LANE:]

        def store(ref, slot, tile, pair):
            r = tile_rows(tile)
            ref[slot, r, 0:LANE] = pair[0]
            ref[slot, r, LANE:] = pair[1]

        def mix_low(source, target, k, sign):
            c, t = ct[k, 0], ct[k, sign]

            def body(i, _):
                base, tile = (i // tiles) * lo, i % tiles
                v = [load(source, base + j, tile) for j in range(lo)]
                for b in lo_bits:
                    v = rot(v, b, c, t)
                for j in range(lo):
                    store(target, base + j, tile, v[j])
                return 0
            lax.fori_loop(0, hi * tiles, body, 0)

        def mid_pass(source, target, k_in, s_in, k_out, s_out, middle):
            if k_in is not None:
                c0, t0 = ct[k_in, 0], ct[k_in, s_in]
            if k_out is not None:
                c1, t1 = ct[k_out, 0], ct[k_out, s_out]

            def body(i, carry):
                base, tile = i // tiles, i % tiles
                slots = [base + j * lo for j in range(hi)]
                if source is None:
                    v = [None] * hi
                else:
                    v = [load(source, m, tile) for m in slots]
                if k_in is not None:
                    for b in hi_bits:
                        v = rot(v, b, c0, t0)
                v, carry = middle(v, slots, tile, carry)
                if k_out is not None:
                    for b in hi_bits:
                        v = rot(v, b, c1, t1)
                    for j in range(hi):
                        store(target, slots[j], tile, v[j])
                return carry
            return lax.fori_loop(0, lo * tiles, body, jnp.zeros((SUB, LANE), F32))

        def pre_mix(source, target, k, sign):
            c, t = ct[k, 0], ct[k, sign]

            def rows_body(i, _):
                base = i * lo
                v = [load(source, base + j // tiles, j % tiles) for j in range(lo * tiles)]
                for b in lo_bits:
                    v = rot(v, b * tiles, c, t)
                for b in tile_bits:
                    v = rot(v, b, c, t)
                for j in range(lo * tiles):
                    re, im = v[j]
                    for b in range(3):
                        fr, fi = sub_flip(re, b), sub_flip(im, b)
                        re, im = c * re + t * fi, c * im - t * fr
                    store(tmp, base + j // tiles, j % tiles, (re, im))
                return 0
            lax.fori_loop(0, hi, rows_body, 0)

            def lanes_body(i, _):
                at = pl.ds(pl.multiple_of(i * lo, lo), lo)
                x = tmp[at].reshape(lo * rows, 2 * LANE)
                xh, xm, xl = split3(x)
                w = [wmat[k, sign - 1, p] for p in range(3)]
                y = mm(xh, w[0]) + (mm(xh, w[1]) + mm(xm, w[0])) + (mm(xh, w[2]) + mm(xm, w[1]) + mm(xl, w[0]))
                target[at] = y.reshape(lo, rows, 2 * LANE)
                return 0
            lax.fori_loop(0, hi, lanes_body, 0)

        def im_dot(a, b):
            return a[0] * b[1] - a[1] * b[0]

        def slot_dot(bra, ket):
            def group(slots, tile, bits, a):
                x = [load(bra, m, tile) for m in slots]
                y = [load(ket, m, tile) for m in slots]
                for j in range(len(slots)):
                    re = sum(y[j ^ b][0] for b in bits[1:]) + y[j ^ bits[0]][0] if len(bits) > 1 else y[j ^ bits[0]][0]
                    im = sum(y[j ^ b][1] for b in bits[1:]) + y[j ^ bits[0]][1] if len(bits) > 1 else y[j ^ bits[0]][1]
                    a = a + im_dot(x[j], (re, im))
                return a

            def low(i, a):
                return group([(i // tiles) * lo + j for j in range(lo)], i % tiles, lo_bits, a)

            def high(i, a):
                return group([i // tiles + j * lo for j in range(hi)], i % tiles, hi_bits, a)
            a = lax.fori_loop(0, hi * tiles, low, jnp.zeros((SUB, LANE), F32))
            return lax.fori_loop(0, lo * tiles, high, a)

        def fold(x):
            while x.shape[0] > SUB:
                half = x.shape[0] // 2
                x = x[:half] + x[half:]
            return x

        def inner_x(x):
            xh, xm, xl = split3(x)
            y = mm(xh, adj[...]) + mm(xm, adj[...]) + mm(xl, adj[...])
            return y

        def tile_flips(v):
            out = []
            for j in range(len(v)):
                parts_ = []
                for comp in range(2):
                    x = v[j][comp]
                    f = sub_flip(x, 0) + sub_flip(x, 1) + sub_flip(x, 2)
                    for b in tile_bits:
                        f = f + v[j ^ b][comp]
                    parts_.append(f)
                out.append(tuple(parts_))
            return out

        def inner_apply(ket, target):
            def body(i, _):
                at = pl.ds(pl.multiple_of(i * lo, lo), lo)
                y = inner_x(ket[at].reshape(lo * rows, 2 * LANE))
                target[at] = y.reshape(lo, rows, 2 * LANE)
                return 0
            lax.fori_loop(0, hi, body, 0)

            def add(i, _):
                v = [load(ket, i, j) for j in range(tiles)]
                f = tile_flips(v)
                for j in range(tiles):
                    y = load(target, i, j)
                    store(target, i, j, (y[0] + f[j][0], y[1] + f[j][1]))
                return 0
            lax.fori_loop(0, n, add, 0)

        def inner_dots(bra, ket, cost):
            inner_apply(ket, tmp)

            def body(i, carry):
                a, g = carry
                for j in range(tiles):
                    x = load(bra, i, j)
                    a = a + im_dot(x, load(tmp, i, j))
                    g = g + cost[i, tile_rows(j), :] * im_dot(x, load(ket, i, j))
                return a, g
            z = jnp.zeros((SUB, LANE), F32)
            return lax.fori_loop(0, n, body, (z, z))

        def two_dots(bra, ket_b, ket_c):
            def body(i, carry):
                a, g = carry
                for j in range(tiles):
                    x = load(bra, i, j)
                    a = a + im_dot(x, load(ket_b, i, j))
                    g = g + im_dot(x, load(ket_c, i, j))
                return a, g
            z = jnp.zeros((SUB, LANE), F32)
            return lax.fori_loop(0, n, body, (z, z))

        def slot_x(source, target):
            def low(i, _):
                base, tile = (i // tiles) * lo, i % tiles
                y = [load(source, base + j, tile) for j in range(lo)]
                for j in range(lo):
                    o = load(target, base + j, tile)
                    store(target, base + j, tile, tuple(o[c] + (y[j ^ 1][c] + y[j ^ 2][c] + y[j ^ 4][c]) for c in range(2)))
                return 0
            lax.fori_loop(0, hi * tiles, low, 0)

            def high(i, _):
                base, tile = i // tiles, i % tiles
                y = [load(source, base + j * lo, tile) for j in range(hi)]
                for j in range(hi):
                    o = load(target, base + j * lo, tile)
                    store(target, base + j * lo, tile, tuple(o[c] + (y[j ^ 1][c] + y[j ^ 2][c]) for c in range(2)))
                return 0
            lax.fori_loop(0, lo * tiles, high, 0)

        def slot_mix_all(ref, k):
            mix_low(ref, ref, k, 1)
            mid_pass(ref, ref, None, 1, k, 1, lambda v, slots, tile, a: (v, a))

        def fill_table(ref, cost, s, l, scale):
            g = gamma_ref[s, l]

            def body(i, _):
                for j in range(tiles):
                    sn, cs = sincos(cost[i, tile_rows(j), :] * g)
                    if scale is None:
                        store(ref, i, j, (cs, sn))
                    else:
                        store(ref, i, j, (cs * scale, sn * -scale))
                return 0
            lax.fori_loop(0, n, body, 0)

        def own(source, target):
            target[me] = source[me]

        def stage(e, s, e_next, k_in, s_in, k_out, s_out, middle):
            wait_bytes(dst.at[e, s], recv_sem.at[e, s])
            mix_low(dst.at[e, s], tmp, k_in, s_in)
            a = mid_pass(tmp, tmp, k_in, s_in, k_out, s_out, middle)
            pre_mix(tmp, src.at[e_next, s], k_out, s_out)
            own(src.at[e_next, s], dst.at[e_next, s])
            exchange(src.at[e_next, s], dst.at[e_next, s], (e_next, s))
            return a

        def kk(s, l):
            return s * num_layers + l

        def add_acc(s, q, a, init=False):
            row = s * 8 + q
            acc[row] = a if init else acc[row] + a


        def set_weights(k, _):
            weights(k, k)
            return 0
        lax.fori_loop(0, num_sets * num_layers, set_weights, 0)
        pl.semaphore_wait(barrier, n - 1)
        exchange(cost_ref, cost_b, (6, 0))

        def each_set(f):
            lax.fori_loop(0, num_sets, lambda s, _: (f(s), 0)[1], 0)

        cost_b[me] = cost_ref[me]

        @each_set
        def _(s):
            fill_table(keep.at[0, s], cost_ref, s, 0, norm)
            mid_pass(keep.at[0, s], tmp, None, 1, kk(s, 0), 1, lambda v, slots, tile, a: (v, a))
            pre_mix(tmp, src.at[0, s], kk(s, 0), 1)
            own(src.at[0, s], dst.at[0, s])
            exchange(src.at[0, s], dst.at[0, s], (0, s))

        wait_bytes(cost_b, recv_sem.at[6, 0])
        @each_set
        def _(s):
            fill_table(tab.at[0, s], cost_b, s, 1, None)
        @each_set
        def _(s):
            fill_table(tab.at[1, s], cost_ref, s, 2, None)

        def forward_mid(before, after, table):
            def middle(v, slots, tile, a):
                out = []
                for m, (re, im) in zip(slots, v):
                    store(before, m, tile, (re, im))
                    cs, sn = load(table, m, tile)
                    p = (re * cs + im * sn, im * cs - re * sn)
                    store(after, m, tile, p)
                    out.append(p)
                return out, a
            return middle

        def backward_mid(before, after, table):
            def middle(v, slots, tile, a):
                out = []
                for m, (re, im) in zip(slots, v):
                    store(before, m, tile, (re, im))
                    cs, sn = load(table, m, tile)
                    p = (re * cs - im * sn, im * cs + re * sn)
                    store(after, m, tile, p)
                    out.append(p)
                return out, a
            return middle

        def turn_mid(psi, lam):
            def middle(v, slots, tile, a):
                out = []
                for m, (re, im) in zip(slots, v):
                    store(psi, m, tile, (re, im))
                    w = cost_b[m, tile_rows(tile), :]
                    p = (w * re, w * im)
                    a = a + (p[0] * re + p[1] * im)
                    store(lam, m, tile, p)
                    out.append(p)
                return out, a
            return middle

        @each_set
        def _(s):
            stage(0, s, 1, kk(s, 0), 1, kk(s, 1), 1, forward_mid(keep.at[1, s], keep.at[2, s], tab.at[0, s]))
        @each_set
        def _(s):
            stage(1, s, 2, kk(s, 1), 1, kk(s, 2), 1, forward_mid(keep.at[3, s], keep.at[4, s], tab.at[1, s]))
            inner_apply(keep.at[0, s], psi_b.at[s])
            slot_x(keep.at[0, s], psi_b.at[s])
            slot_mix_all(psi_b.at[s], kk(s, 0))

            def times_cost(i, _):
                for j in range(tiles):
                    re, im = load(keep.at[0, s], i, j)
                    w = cost_ref[i, tile_rows(j), :]
                    store(psi_c.at[s], i, j, (w * re, w * im))
                return 0
            lax.fori_loop(0, n, times_cost, 0)
            slot_mix_all(psi_c.at[s], kk(s, 0))
        @each_set
        def _(s):
            a = stage(2, s, 3, kk(s, 2), 1, kk(s, 2), 2, turn_mid(keep.at[5, s], keep.at[6, s]))
            add_acc(s, 0, a, True)
            add_acc(s, 6, slot_dot(keep.at[6, s], keep.at[5, s]), True)
        @each_set
        def _(s):
            stage(3, s, 4, kk(s, 2), 2, kk(s, 1), 2, backward_mid(keep.at[7, s], keep.at[8, s], tab.at[1, s]))
            b, g = inner_dots(keep.at[7, s], keep.at[4, s], cost_ref)
            add_acc(s, 6, b + slot_dot(keep.at[7, s], keep.at[4, s]))
            add_acc(s, 3, 2.0 * g, True)
            add_acc(s, 5, slot_dot(keep.at[8, s], keep.at[3, s]), True)
        @each_set
        def _(s):
            stage(4, s, 5, kk(s, 1), 2, kk(s, 0), 2, backward_mid(keep.at[9, s], keep.at[10, s], tab.at[0, s]))
            b, g = inner_dots(keep.at[9, s], keep.at[2, s], cost_b)
            add_acc(s, 5, b + slot_dot(keep.at[9, s], keep.at[2, s]))
            add_acc(s, 2, 2.0 * g, True)
            add_acc(s, 4, slot_dot(keep.at[10, s], keep.at[1, s]), True)
        @each_set
        def _(s):
            wait_bytes(dst.at[5, s], recv_sem.at[5, s])
            b, g = two_dots(dst.at[5, s], psi_b.at[s], psi_c.at[s])
            add_acc(s, 4, b)
            add_acc(s, 1, 2.0 * g, True)

        lane = lax.broadcasted_iota(jnp.int32, (1, LANE), 1)
        vec = jnp.zeros((1, LANE), F32)
        for s in range(num_sets):
            for q in range(1 + 2 * num_layers):
                total = jnp.sum(jnp.sum(acc[s * 8 + q], axis=0, keepdims=True), axis=1, keepdims=True)
                vec = jnp.where(lane == s * 8 + q, total, vec)
        mine[0] = jnp.broadcast_to(vec, (SUB, LANE))
        parts[me] = jnp.broadcast_to(vec, (SUB, LANE))
        each_peer(lambda ty, tx: send(mine.at[0], parts.at[me], (6, 1), ty, tx))
        wait_bytes(parts, recv_sem.at[6, 1])
        total = parts[0]
        for m in range(1, n):
            total = total + parts[m]
        for s in range(num_sets):
            e_ref[s] = total[0, s * 8]
            for q in range(2 * num_layers):
                g_ref[s, q] = total[0, s * 8 + 1 + q]

        for e in range(6):
            for s in range(num_sets):
                wait_bytes(src.at[e, s], send_sem.at[e, s])
        wait_bytes(cost_b, send_sem.at[6, 0])
        wait_bytes(parts, send_sem.at[6, 1])

    return kernel


def solution(mesh):
    ny, nx = mesh.shape['qy'], mesh.shape['qx']
    n = ny * nx

    def device_fn(cost, gamma, beta):
        size = cost.shape[0]
        num_sets, num_layers = gamma.shape
        rows = size // (LANE * n)
        bits = (size * n).bit_length() - 1
        norm = 2.0 ** (-0.5 * bits)
        state = (n, rows, 2 * LANE)
        smem = pl.BlockSpec(memory_space=pltpu.SMEM)
        energy, grad = pl.pallas_call(
            make_kernel(ny, nx, num_sets, num_layers, rows, norm),
            out_shape=(jax.ShapeDtypeStruct((num_sets,), F32), jax.ShapeDtypeStruct((num_sets, 2 * num_layers), F32)),
            in_specs=[pl.BlockSpec(memory_space=pltpu.VMEM), smem, smem],
            out_specs=(smem, smem),
            scratch_shapes=[
                pltpu.VMEM((n, rows, LANE), F32),
                pltpu.VMEM((6, num_sets) + state, F32),
                pltpu.VMEM((6, num_sets) + state, F32),
                pltpu.VMEM((11, num_sets) + state, F32),
                pltpu.VMEM((2, num_sets) + state, F32),
                pltpu.VMEM((num_sets,) + state, F32),
                pltpu.VMEM((num_sets,) + state, F32),
                pltpu.VMEM((num_sets * num_layers, 2, 3, 2 * LANE, 2 * LANE), BF16),
                pltpu.VMEM((2 * LANE, 2 * LANE), BF16),
                pltpu.VMEM((LANE, LANE), jnp.int32),
                pltpu.VMEM((num_sets * num_layers, 3, SUB, LANE), F32),
                pltpu.VMEM((num_sets * 8, SUB, LANE), F32),
                pltpu.VMEM((1, SUB, LANE), F32),
                pltpu.VMEM((n, SUB, LANE), F32),
                pltpu.VMEM(state, F32),
                pltpu.SemaphoreType.DMA((7, 2)),
                pltpu.SemaphoreType.DMA((7, 2)),
            ],
            compiler_params=pltpu.CompilerParams(collective_id=0, has_side_effects=True, vmem_limit_bytes=60 * 2 ** 20),
            name='qaoa',
        )(cost.reshape(n, rows, LANE), gamma, beta)
        return energy, grad

    cost_spec = P(('inst', 'qy', 'qx'))
    angle_spec = P('inst', None)
    return jax.shard_map(device_fn, mesh=mesh, in_specs=(cost_spec, angle_spec, angle_spec), out_specs=(P('inst'), angle_spec), check_vma=False)
```

```python
import functools
import jax
import jax.numpy as jnp
from jax import lax
from jax.experimental import pallas as pl
from jax.experimental.pallas import tpu as pltpu
from jax.sharding import PartitionSpec as P

LANE = 128
LANE_BITS = 7
SUB = 8
MESH_ID = pl.DeviceIdType.MESH
F32 = jnp.float32
BF16 = jnp.bfloat16


def sincos(x):
    k = jnp.floor(x * 0.6366197723675814 + 0.5)
    r = ((x - k * 1.5703125) - k * 4.837512969970703125e-4) - k * 7.54978995489188216e-8
    z = r * r
    s = r + r * z * (-1.6666654611e-1 + z * (8.3321608736e-3 + z * -1.9515295891e-4))
    c = (1.0 - 0.5 * z) + z * z * (4.166664568298827e-2 + z * (-1.388731625493765e-3 + z * 2.443315711809948e-5))
    q = k.astype(jnp.int32)
    odd = (q & 1) != 0
    sin_v = jnp.where(odd, c, s)
    cos_v = jnp.where(odd, s, c)
    sin_v = jnp.where((q & 2) != 0, -sin_v, sin_v)
    cos_v = jnp.where(((q + 1) & 2) != 0, -cos_v, cos_v)
    return sin_v, cos_v


def split3(x):
    hi = x.astype(BF16)
    rest = x - hi.astype(F32)
    mid = rest.astype(BF16)
    low = (rest - mid.astype(F32)).astype(BF16)
    return hi, mid, low


def mm(a, b):
    return jnp.dot(a, b, preferred_element_type=F32)


def rot(pairs, stride, c, t):
    out = list(pairs)
    for j in range(len(pairs)):
        if j & stride:
            continue
        (ar, ai), (br, bi) = pairs[j], pairs[j | stride]
        out[j] = (c * ar + t * bi, c * ai - t * br)
        out[j | stride] = (c * br + t * ai, c * bi - t * ar)
    return out


def sub_flip(x, bit):
    if bit == 2:
        return pltpu.roll(x, 4, 0)
    row = lax.broadcasted_iota(jnp.int32, (SUB, LANE), 0)
    up = pltpu.roll(x, 1 << bit, 0)
    down = pltpu.roll(x, SUB - (1 << bit), 0)
    return jnp.where((row & (1 << bit)) != 0, up, down)


def make_kernel(ny, nx, num_sets, num_layers, rows, norm):
    n = ny * nx
    lo = 8
    hi = n // lo
    tiles = rows // SUB
    lo_bits = [1 << b for b in range(lo.bit_length() - 1)]
    hi_bits = [1 << b for b in range(hi.bit_length() - 1)]
    tile_bits = [1 << b for b in range(tiles.bit_length() - 1)]
    width_x = nx // 2

    def kernel(cost_ref, gamma_ref, beta_ref, parts,
               cost_b, src, dst, keep, tab, psi_b, psi_c, wmat, adj, dmat, ct, acc, mine, tmp, send_sem, recv_sem):
        qy = lax.axis_index('qy')
        qx = lax.axis_index('qx')
        me = qy * nx + qx
        barrier = pltpu.get_barrier_semaphore()

        chip_x = [lax.rem(qx // 2 + dx, width_x) * 2 for dx in (1, 3, 2, 0)]

        def each_peer(act):
            def body(i, _):
                ty = lax.rem(qy + 1 + i, ny)
                core = lax.rem(qx + 1 + i // ny, 2)
                for tx in chip_x[:-1]:
                    act(ty, tx + core)

                @pl.when(i < 2 * ny - 1)
                def _():
                    act(ty, chip_x[-1] + core)
                return 0
            lax.fori_loop(0, 2 * ny, body, 0)

        def greet(ty, tx):
            pl.semaphore_signal(barrier, inc=1, device_id={'qy': ty, 'qx': tx}, device_id_type=MESH_ID)
        each_peer(greet)

        def send(source, target, ids, ty, tx):
            pltpu.make_async_remote_copy(
                source, target, send_sem.at[ids], recv_sem.at[ids],
                device_id={'qy': ty, 'qx': tx}, device_id_type=MESH_ID).start()

        def exchange(source, target, ids):
            each_peer(lambda ty, tx: send(source.at[ty * nx + tx], target.at[me], ids, ty, tx))

        def wait_bytes(buf, sem):
            part = buf.at[pl.ds(0, n - 1)]
            pltpu.make_async_copy(part, part, sem).wait()

        def tile_d(r, _):
            a = lax.broadcasted_iota(jnp.int32, (SUB, LANE), 0) + r * SUB
            b = lax.broadcasted_iota(jnp.int32, (SUB, LANE), 1)
            x = a ^ b
            d = jnp.zeros_like(x)
            for k in range(LANE_BITS):
                d = d + ((x >> k) & 1)
            dmat[pl.ds(pl.multiple_of(r * SUB, SUB), SUB), :] = d
            return 0
        lax.fori_loop(0, LANE // SUB, tile_d, 0)
        one = (dmat[...] == 1).astype(F32).astype(BF16)
        zero = jnp.zeros((LANE, LANE), BF16)
        adj[0:LANE, 0:LANE] = one
        adj[0:LANE, LANE:] = zero
        adj[LANE:, 0:LANE] = zero
        adj[LANE:, LANE:] = one
        for s in range(num_sets):
            for l in range(num_layers):
                k = s * num_layers + l
                sin_h, cos_h = sincos(jnp.full((SUB, LANE), 0.5 * beta_ref[s, l], F32))
                ct[k, 0] = cos_h
                ct[k, 1] = sin_h
                ct[k, 2] = -sin_h

        def weights(k, slot):
            c, t = ct[k, 0], ct[k, 1]
            cp, tp = [jnp.ones_like(c)], [jnp.ones_like(c)]
            for _ in range(LANE_BITS):
                cp.append(cp[-1] * c)
                tp.append(tp[-1] * t)
            amp = [cp[LANE_BITS - d] * tp[d] for d in range(LANE_BITS + 1)]
            z = jnp.zeros_like(c)
            real = [z, z, z, z, z, z, z, z]
            imag = [z, z, z, z, z, z, z, z]
            for d in range(LANE_BITS + 1):
                if d % 4 == 0:
                    real[d] = amp[d]
                elif d % 4 == 1:
                    imag[d] = -amp[d]
                elif d % 4 == 2:
                    real[d] = -amp[d]
                else:
                    imag[d] = amp[d]

            def body(r, _):
                at = pl.multiple_of(r * 2 * SUB, 2 * SUB)
                rows_re, rows_im = [], []
                for h in range(2):
                    d = dmat[pl.ds(at + h * SUB, SUB), :]
                    re = z
                    im = z
                    for j in range(LANE_BITS + 1):
                        hit = d == j
                        if j % 2 == 0:
                            re = jnp.where(hit, real[j], re)
                        else:
                            im = jnp.where(hit, imag[j], im)
                    rows_re.append(re)
                    rows_im.append(im)
                re = jnp.concatenate(rows_re, axis=0)
                im = jnp.concatenate(rows_im, axis=0)
                for p, (a, b) in enumerate(zip(split3(re), split3(im))):
                    top = pl.ds(at, 2 * SUB)
                    bot = pl.ds(at + LANE, 2 * SUB)
                    wmat[slot, 0, p, top, 0:LANE] = a
                    wmat[slot, 0, p, top, LANE:] = b
                    wmat[slot, 0, p, bot, 0:LANE] = -b
                    wmat[slot, 0, p, bot, LANE:] = a
                    wmat[slot, 1, p, top, 0:LANE] = a
                    wmat[slot, 1, p, top, LANE:] = -b
                    wmat[slot, 1, p, bot, 0:LANE] = b
                    wmat[slot, 1, p, bot, LANE:] = a
                return 0
            lax.fori_loop(0, LANE // (2 * SUB), body, 0)

        def tile_rows(tile):
            return pl.ds(pl.multiple_of(tile * SUB, SUB), SUB)

        def load(ref, slot, tile):
            r = tile_rows(tile)
            return ref[slot, r, 0:LANE], ref[slot, r, LANE:]

        def store(ref, slot, tile, pair):
            r = tile_rows(tile)
            ref[slot, r, 0:LANE] = pair[0]
            ref[slot, r, LANE:] = pair[1]

        def mix_low(source, target, k, sign):
            c, t = ct[k, 0], ct[k, sign]

            def body(i, _):
                base, tile = (i // tiles) * lo, i % tiles
                v = [load(source, base + j, tile) for j in range(lo)]
                for b in lo_bits:
                    v = rot(v, b, c, t)
                for j in range(lo):
                    store(target, base + j, tile, v[j])
                return 0
            lax.fori_loop(0, hi * tiles, body, 0)

        def mid_pass(source, target, k_in, s_in, k_out, s_out, middle):
            if k_in is not None:
                c0, t0 = ct[k_in, 0], ct[k_in, s_in]
            if k_out is not None:
                c1, t1 = ct[k_out, 0], ct[k_out, s_out]

            def body(i, carry):
                base, tile = i // tiles, i % tiles
                slots = [base + j * lo for j in range(hi)]
                if source is None:
                    v = [None] * hi
                else:
                    v = [load(source, m, tile) for m in slots]
                if k_in is not None:
                    for b in hi_bits:
                        v = rot(v, b, c0, t0)
                v, carry = middle(v, slots, tile, carry)
                if k_out is not None:
                    for b in hi_bits:
                        v = rot(v, b, c1, t1)
                    for j in range(hi):
                        store(target, slots[j], tile, v[j])
                return carry
            return lax.fori_loop(0, lo * tiles, body, jnp.zeros((SUB, LANE), F32))

        def pre_mix(source, target, k, sign):
            c, t = ct[k, 0], ct[k, sign]

            def rows_body(i, _):
                base = i * lo
                v = [load(source, base + j // tiles, j % tiles) for j in range(lo * tiles)]
                for b in lo_bits:
                    v = rot(v, b * tiles, c, t)
                for b in tile_bits:
                    v = rot(v, b, c, t)
                for j in range(lo * tiles):
                    re, im = v[j]
                    for b in range(3):
                        fr, fi = sub_flip(re, b), sub_flip(im, b)
                        re, im = c * re + t * fi, c * im - t * fr
                    store(tmp, base + j // tiles, j % tiles, (re, im))
                return 0
            lax.fori_loop(0, hi, rows_body, 0)

            def lanes_body(i, _):
                at = pl.ds(pl.multiple_of(i * 16, 16), 16)
                m = 16 * rows
                x = tmp[at].reshape(m, 2 * LANE)
                xh, xm, xl = split3(x)
                w = [wmat[k, sign - 1, p] for p in range(3)]
                a = mm(jnp.concatenate([xh, xm, xl], axis=0), w[0])
                b = mm(jnp.concatenate([xh, xm], axis=0), w[1])
                y = a[:m] + (b[:m] + a[m:2 * m]) + (mm(xh, w[2]) + b[m:] + a[2 * m:])
                target[at] = y.reshape(16, rows, 2 * LANE)
                return 0
            lax.fori_loop(0, n // 16, lanes_body, 0)

        def im_dot(a, b):
            return a[0] * b[1] - a[1] * b[0]

        def slot_dot(bra, ket):
            def group(slots, tile, bits, a):
                x = [load(bra, m, tile) for m in slots]
                y = [load(ket, m, tile) for m in slots]
                for j in range(len(slots)):
                    re = sum(y[j ^ b][0] for b in bits[1:]) + y[j ^ bits[0]][0] if len(bits) > 1 else y[j ^ bits[0]][0]
                    im = sum(y[j ^ b][1] for b in bits[1:]) + y[j ^ bits[0]][1] if len(bits) > 1 else y[j ^ bits[0]][1]
                    a = a + im_dot(x[j], (re, im))
                return a

            def low(i, a):
                return group([(i // tiles) * lo + j for j in range(lo)], i % tiles, lo_bits, a)

            def high(i, a):
                return group([i // tiles + j * lo for j in range(hi)], i % tiles, hi_bits, a)
            a = lax.fori_loop(0, hi * tiles, low, jnp.zeros((SUB, LANE), F32))
            return lax.fori_loop(0, lo * tiles, high, a)

        def fold(x):
            while x.shape[0] > SUB:
                half = x.shape[0] // 2
                x = x[:half] + x[half:]
            return x

        def inner_x(x):
            xh, xm, xl = split3(x)
            y = mm(xh, adj[...]) + mm(xm, adj[...]) + mm(xl, adj[...])
            return y

        def tile_flips(v):
            out = []
            for j in range(len(v)):
                parts_ = []
                for comp in range(2):
                    x = v[j][comp]
                    f = sub_flip(x, 0) + sub_flip(x, 1) + sub_flip(x, 2)
                    for b in tile_bits:
                        f = f + v[j ^ b][comp]
                    parts_.append(f)
                out.append(tuple(parts_))
            return out

        def inner_apply(ket, target):
            def body(i, _):
                at = pl.ds(pl.multiple_of(i * lo, lo), lo)
                y = inner_x(ket[at].reshape(lo * rows, 2 * LANE))
                target[at] = y.reshape(lo, rows, 2 * LANE)
                return 0
            lax.fori_loop(0, hi, body, 0)

            def add(i, _):
                v = [load(ket, i, j) for j in range(tiles)]
                f = tile_flips(v)
                for j in range(tiles):
                    y = load(target, i, j)
                    store(target, i, j, (y[0] + f[j][0], y[1] + f[j][1]))
                return 0
            lax.fori_loop(0, n, add, 0)

        def inner_dots(bra, ket, cost):
            inner_apply(ket, tmp)

            def body(i, carry):
                a, g = carry
                for j in range(tiles):
                    x = load(bra, i, j)
                    a = a + im_dot(x, load(tmp, i, j))
                    g = g + cost[i, tile_rows(j), :] * im_dot(x, load(ket, i, j))
                return a, g
            z = jnp.zeros((SUB, LANE), F32)
            return lax.fori_loop(0, n, body, (z, z))

        def two_dots(bra, ket_b, ket_c):
            def body(i, carry):
                a, g = carry
                for j in range(tiles):
                    x = load(bra, i, j)
                    a = a + im_dot(x, load(ket_b, i, j))
                    g = g + im_dot(x, load(ket_c, i, j))
                return a, g
            z = jnp.zeros((SUB, LANE), F32)
            return lax.fori_loop(0, n, body, (z, z))

        def slot_x(source, target):
            def low(i, _):
                base, tile = (i // tiles) * lo, i % tiles
                y = [load(source, base + j, tile) for j in range(lo)]
                for j in range(lo):
                    o = load(target, base + j, tile)
                    store(target, base + j, tile, tuple(o[c] + (y[j ^ 1][c] + y[j ^ 2][c] + y[j ^ 4][c]) for c in range(2)))
                return 0
            lax.fori_loop(0, hi * tiles, low, 0)

            def high(i, _):
                base, tile = i // tiles, i % tiles
                y = [load(source, base + j * lo, tile) for j in range(hi)]
                for j in range(hi):
                    o = load(target, base + j * lo, tile)
                    store(target, base + j * lo, tile, tuple(o[c] + (y[j ^ 1][c] + y[j ^ 2][c]) for c in range(2)))
                return 0
            lax.fori_loop(0, lo * tiles, high, 0)

        def slot_mix_all(ref, k):
            mix_low(ref, ref, k, 1)
            mid_pass(ref, ref, None, 1, k, 1, lambda v, slots, tile, a: (v, a))

        def fill_table(ref, cost, s, l, scale):
            g = gamma_ref[s, l]

            def body(i, _):
                for j in range(tiles):
                    sn, cs = sincos(cost[i, tile_rows(j), :] * g)
                    if scale is None:
                        store(ref, i, j, (cs, sn))
                    else:
                        store(ref, i, j, (cs * scale, sn * -scale))
                return 0
            lax.fori_loop(0, n, body, 0)

        def own(source, target):
            target[me] = source[me]

        def stage(e, s, e_next, k_in, s_in, k_out, s_out, middle):
            wait_bytes(dst.at[e, s], recv_sem.at[e, s])
            mix_low(dst.at[e, s], tmp, k_in, s_in)
            a = mid_pass(tmp, tmp, k_in, s_in, k_out, s_out, middle)
            pre_mix(tmp, src.at[e_next, s], k_out, s_out)
            own(src.at[e_next, s], dst.at[e_next, s])
            exchange(src.at[e_next, s], dst.at[e_next, s], (e_next, s))
            return a

        def kk(s, l):
            return s * num_layers + l

        def add_acc(s, q, a, init=False):
            row = s * 8 + q
            acc[row] = a if init else acc[row] + a


        def each_set(f):
            lax.fori_loop(0, num_sets, lambda s, _: (f(s), 0)[1], 0)

        def first_layer(s):
            weights(kk(s, 0), kk(s, 0))
            fill_table(keep.at[0, s], cost_ref, s, 0, norm)
            mid_pass(keep.at[0, s], tmp, None, 1, kk(s, 0), 1, lambda v, slots, tile, a: (v, a))
            pre_mix(tmp, src.at[0, s], kk(s, 0), 1)
            own(src.at[0, s], dst.at[0, s])

        first_layer(0)
        pl.semaphore_wait(barrier, n - 1)
        exchange(src.at[0, 0], dst.at[0, 0], (0, 0))
        exchange(cost_ref, cost_b, (6, 0))
        cost_b[me] = cost_ref[me]
        for s in range(1, num_sets):
            first_layer(s)
            exchange(src.at[0, s], dst.at[0, s], (0, s))

        def set_weights(i, _):
            k = (i // (num_layers - 1)) * num_layers + 1 + i % (num_layers - 1)
            weights(k, k)
            return 0
        lax.fori_loop(0, num_sets * (num_layers - 1), set_weights, 0)
        each_set(lambda s: fill_table(tab.at[1, s], cost_ref, s, 2, None))
        wait_bytes(cost_b, recv_sem.at[6, 0])
        each_set(lambda s: fill_table(tab.at[0, s], cost_b, s, 1, None))

        def forward_mid(before, after, table):
            def middle(v, slots, tile, a):
                out = []
                for m, (re, im) in zip(slots, v):
                    store(before, m, tile, (re, im))
                    cs, sn = load(table, m, tile)
                    p = (re * cs + im * sn, im * cs - re * sn)
                    store(after, m, tile, p)
                    out.append(p)
                return out, a
            return middle

        def backward_mid(before, after, table):
            def middle(v, slots, tile, a):
                out = []
                for m, (re, im) in zip(slots, v):
                    store(before, m, tile, (re, im))
                    cs, sn = load(table, m, tile)
                    p = (re * cs - im * sn, im * cs + re * sn)
                    store(after, m, tile, p)
                    out.append(p)
                return out, a
            return middle

        def turn_mid(psi, lam):
            def middle(v, slots, tile, a):
                out = []
                for m, (re, im) in zip(slots, v):
                    store(psi, m, tile, (re, im))
                    w = cost_b[m, tile_rows(tile), :]
                    p = (w * re, w * im)
                    a = a + (p[0] * re + p[1] * im)
                    store(lam, m, tile, p)
                    out.append(p)
                return out, a
            return middle

        @each_set
        def _(s):
            stage(0, s, 1, kk(s, 0), 1, kk(s, 1), 1, forward_mid(keep.at[1, s], keep.at[2, s], tab.at[0, s]))
        @each_set
        def _(s):
            stage(1, s, 2, kk(s, 1), 1, kk(s, 2), 1, forward_mid(keep.at[3, s], keep.at[4, s], tab.at[1, s]))
            inner_apply(keep.at[0, s], psi_b.at[s])
            slot_x(keep.at[0, s], psi_b.at[s])
            slot_mix_all(psi_b.at[s], kk(s, 0))

            def times_cost(i, _):
                for j in range(tiles):
                    re, im = load(keep.at[0, s], i, j)
                    w = cost_ref[i, tile_rows(j), :]
                    store(psi_c.at[s], i, j, (w * re, w * im))
                return 0
            lax.fori_loop(0, n, times_cost, 0)
            slot_mix_all(psi_c.at[s], kk(s, 0))
        @each_set
        def _(s):
            a = stage(2, s, 3, kk(s, 2), 1, kk(s, 2), 2, turn_mid(keep.at[5, s], keep.at[6, s]))
            add_acc(s, 0, a, True)
            add_acc(s, 6, slot_dot(keep.at[6, s], keep.at[5, s]), True)
        @each_set
        def _(s):
            stage(3, s, 4, kk(s, 2), 2, kk(s, 1), 2, backward_mid(keep.at[7, s], keep.at[8, s], tab.at[1, s]))
            b, g = inner_dots(keep.at[7, s], keep.at[4, s], cost_ref)
            add_acc(s, 6, b + slot_dot(keep.at[7, s], keep.at[4, s]))
            add_acc(s, 3, 2.0 * g, True)
            add_acc(s, 5, slot_dot(keep.at[8, s], keep.at[3, s]), True)
        @each_set
        def _(s):
            stage(4, s, 5, kk(s, 1), 2, kk(s, 0), 2, backward_mid(keep.at[9, s], keep.at[10, s], tab.at[0, s]))
            b, g = inner_dots(keep.at[9, s], keep.at[2, s], cost_b)
            add_acc(s, 5, b + slot_dot(keep.at[9, s], keep.at[2, s]))
            add_acc(s, 2, 2.0 * g, True)
            add_acc(s, 4, slot_dot(keep.at[10, s], keep.at[1, s]), True)
        @each_set
        def _(s):
            wait_bytes(dst.at[5, s], recv_sem.at[5, s])
            b, g = two_dots(dst.at[5, s], psi_b.at[s], psi_c.at[s])
            add_acc(s, 4, b)
            add_acc(s, 1, 2.0 * g, True)

        lane = lax.broadcasted_iota(jnp.int32, (1, LANE), 1)
        for s in range(num_sets):
            vec = jnp.zeros((1, LANE), F32)
            for q in range(1 + 2 * num_layers):
                total = jnp.sum(jnp.sum(acc[s * 8 + q], axis=0, keepdims=True), axis=1, keepdims=True)
                vec = jnp.where(lane == q, total, vec)
            mine[s:s + 1, :] = vec
        parts[me] = mine[...]
        each_peer(lambda ty, tx: send(mine, parts.at[me], (6, 1), ty, tx))
        wait_bytes(parts, recv_sem.at[6, 1])
        for e in range(6):
            for s in range(num_sets):
                wait_bytes(src.at[e, s], send_sem.at[e, s])
        wait_bytes(cost_b, send_sem.at[6, 0])
        wait_bytes(parts, send_sem.at[6, 1])

    return kernel


def solution(mesh):
    ny, nx = mesh.shape['qy'], mesh.shape['qx']
    n = ny * nx

    def device_fn(cost, gamma, beta):
        size = cost.shape[0]
        num_sets, num_layers = gamma.shape
        rows = size // (LANE * n)
        bits = (size * n).bit_length() - 1
        norm = 2.0 ** (-0.5 * bits)
        state = (n, rows, 2 * LANE)
        smem = pl.BlockSpec(memory_space=pltpu.SMEM)
        parts = pl.pallas_call(
            make_kernel(ny, nx, num_sets, num_layers, rows, norm),
            out_shape=jax.ShapeDtypeStruct((n, num_sets, LANE), F32),
            in_specs=[pl.BlockSpec(memory_space=pltpu.VMEM), smem, smem],
            out_specs=pl.BlockSpec(memory_space=pltpu.VMEM),
            scratch_shapes=[
                pltpu.VMEM((n, rows, LANE), F32),
                pltpu.VMEM((6, num_sets) + state, F32),
                pltpu.VMEM((6, num_sets) + state, F32),
                pltpu.VMEM((11, num_sets) + state, F32),
                pltpu.VMEM((2, num_sets) + state, F32),
                pltpu.VMEM((num_sets,) + state, F32),
                pltpu.VMEM((num_sets,) + state, F32),
                pltpu.VMEM((num_sets * num_layers, 2, 3, 2 * LANE, 2 * LANE), BF16),
                pltpu.VMEM((2 * LANE, 2 * LANE), BF16),
                pltpu.VMEM((LANE, LANE), jnp.int32),
                pltpu.VMEM((num_sets * num_layers, 3, SUB, LANE), F32),
                pltpu.VMEM((num_sets * 8, SUB, LANE), F32),
                pltpu.VMEM((num_sets, LANE), F32),
                pltpu.VMEM(state, F32),
                pltpu.SemaphoreType.DMA((7, 2)),
                pltpu.SemaphoreType.DMA((7, 2)),
            ],
            compiler_params=pltpu.CompilerParams(collective_id=0, has_side_effects=True, vmem_limit_bytes=60 * 2 ** 20),
            name='qaoa',
        )(cost.reshape(n, rows, LANE), gamma, beta)

        def finish(parts_ref, e_ref, g_ref):
            total = jnp.sum(parts_ref[...], axis=0)
            g_ref[...] = total[:, 1:1 + 2 * num_layers]
            for s in range(num_sets):
                e_ref[s] = total[s, 0]

        return pl.pallas_call(
            finish,
            out_shape=(jax.ShapeDtypeStruct((num_sets,), F32), jax.ShapeDtypeStruct((num_sets, 2 * num_layers), F32)),
            in_specs=[pl.BlockSpec(memory_space=pltpu.VMEM)],
            out_specs=(smem, pl.BlockSpec(memory_space=pltpu.VMEM)),
            name='finish',
        )(parts)

    cost_spec = P(('inst', 'qy', 'qx'))
    angle_spec = P('inst', None)
    return jax.shard_map(device_fn, mesh=mesh, in_specs=(cost_spec, angle_spec, angle_spec), out_specs=(P('inst'), angle_spec), check_vma=False)
```

```python
import functools
import jax
import jax.numpy as jnp
from jax import lax
from jax.experimental import pallas as pl
from jax.experimental.pallas import tpu as pltpu
from jax.sharding import PartitionSpec as P

LANE = 128
LANE_BITS = 7
SUB = 8
ORDER_OTHER = [(dy, dx) for dy in (1, 2, 3, 0) for dx in (1, 3, 2, 0)]
ORDER_LIKE = ORDER_OTHER[:-1]
MESH_ID = pl.DeviceIdType.MESH
F32 = jnp.float32
BF16 = jnp.bfloat16


def sincos(x):
    k = jnp.floor(x * 0.6366197723675814 + 0.5)
    r = ((x - k * 1.5703125) - k * 4.837512969970703125e-4) - k * 7.54978995489188216e-8
    z = r * r
    s = r + r * z * (-1.6666654611e-1 + z * (8.3321608736e-3 + z * -1.9515295891e-4))
    c = (1.0 - 0.5 * z) + z * z * (4.166664568298827e-2 + z * (-1.388731625493765e-3 + z * 2.443315711809948e-5))
    q = k.astype(jnp.int32)
    odd = (q & 1) != 0
    sin_v = jnp.where(odd, c, s)
    cos_v = jnp.where(odd, s, c)
    sin_v = jnp.where((q & 2) != 0, -sin_v, sin_v)
    cos_v = jnp.where(((q + 1) & 2) != 0, -cos_v, cos_v)
    return sin_v, cos_v


def split3(x):
    hi = x.astype(BF16)
    rest = x - hi.astype(F32)
    mid = rest.astype(BF16)
    low = (rest - mid.astype(F32)).astype(BF16)
    return hi, mid, low


def mm(a, b):
    return jnp.dot(a, b, preferred_element_type=F32)


def rot(pairs, stride, c, t):
    out = list(pairs)
    for j in range(len(pairs)):
        if j & stride:
            continue
        (ar, ai), (br, bi) = pairs[j], pairs[j | stride]
        out[j] = (c * ar + t * bi, c * ai - t * br)
        out[j | stride] = (c * br + t * ai, c * bi - t * ar)
    return out


def sub_flip(x, bit):
    if bit == 2:
        return pltpu.roll(x, 4, 0)
    row = lax.broadcasted_iota(jnp.int32, (SUB, LANE), 0)
    up = pltpu.roll(x, 1 << bit, 0)
    down = pltpu.roll(x, SUB - (1 << bit), 0)
    return jnp.where((row & (1 << bit)) != 0, up, down)


def make_kernel(ny, nx, num_sets, num_layers, rows, norm):
    n = ny * nx
    lo = 8
    hi = n // lo
    tiles = rows // SUB
    lo_bits = [1 << b for b in range(lo.bit_length() - 1)]
    hi_bits = [1 << b for b in range(hi.bit_length() - 1)]
    tile_bits = [1 << b for b in range(tiles.bit_length() - 1)]
    width_x = nx // 2

    def kernel(cost_ref, gamma_ref, beta_ref, parts,
               cost_b, src, dst, keep, tab, psi_b, psi_c, wmat, adj, dmat, ct, acc, mine, tmp, other, send_sem, recv_sem):
        qy = lax.axis_index('qy')
        qx = lax.axis_index('qx')
        me = qy * nx + qx
        barrier = pltpu.get_barrier_semaphore()

        me_core = lax.rem(qx, 2)

        def ring_x(order):
            return [lax.rem(qx // 2 + dx, width_x) * 2 for dx in order]
        chip_x = ring_x((1, 3, 2, 0))
        far_x = ring_x((2, 1, 3, 0))

        def peers_of_core(act, core, last):
            def body(i, _):
                ty = lax.rem(qy + 1 + i, ny)
                for tx in chip_x[:-1]:
                    act(ty, tx + core)

                @pl.when(i + last < ny)
                def _():
                    act(ty, chip_x[-1] + core)
                return 0
            lax.fori_loop(0, ny, body, 0)

        def peers_in_order(act, order, core):
            for dy, dx in order:
                act(lax.rem(qy + dy, ny), lax.rem(qx // 2 + dx, width_x) * 2 + core)

        def both_cores(f):
            lax.fori_loop(0, 2, lambda h, _: (f(lax.rem(me_core + 1 + h, 2), h), 0)[1], 0)

        def each_peer(act):
            both_cores(lambda core, last: peers_of_core(act, core, last))

        def each_peer_far_first(act):
            def body(i, _):
                a = i // 2
                ty = lax.rem(qy + 2 - a + (a // 2) * (7 - 2 * a), ny)
                core = lax.rem(qx + 1 + i, 2)
                for tx in far_x[:-1]:
                    act(ty, tx + core)

                @pl.when(i < 2 * ny - 1)
                def _():
                    act(ty, far_x[-1] + core)
                return 0
            lax.fori_loop(0, 2 * ny, body, 0)

        def greet(ty, tx):
            pl.semaphore_signal(barrier, inc=1, device_id={'qy': ty, 'qx': tx}, device_id_type=MESH_ID)
        each_peer_far_first(greet)

        def send(source, target, ids, ty, tx):
            pltpu.make_async_remote_copy(
                source, target, send_sem.at[ids], recv_sem.at[ids],
                device_id={'qy': ty, 'qx': tx}, device_id_type=MESH_ID).start()

        def by_core(ty, tx):
            return lax.rem(tx, 2) * (n // 2) + ty * width_x + tx // 2

        def wait_bytes(buf, sem):
            part = buf.at[pl.ds(0, n - 1)]
            pltpu.make_async_copy(part, part, sem).wait()

        def tile_d(r, _):
            a = lax.broadcasted_iota(jnp.int32, (SUB, LANE), 0) + r * SUB
            b = lax.broadcasted_iota(jnp.int32, (SUB, LANE), 1)
            x = a ^ b
            d = jnp.zeros_like(x)
            for k in range(LANE_BITS):
                d = d + ((x >> k) & 1)
            dmat[pl.ds(pl.multiple_of(r * SUB, SUB), SUB), :] = d
            return 0
        lax.fori_loop(0, LANE // SUB, tile_d, 0)
        one = (dmat[...] == 1).astype(F32).astype(BF16)
        zero = jnp.zeros((LANE, LANE), BF16)
        adj[0:LANE, 0:LANE] = one
        adj[0:LANE, LANE:] = zero
        adj[LANE:, 0:LANE] = zero
        adj[LANE:, LANE:] = one
        for s in range(num_sets):
            for l in range(num_layers):
                k = s * num_layers + l
                sin_h, cos_h = sincos(jnp.full((SUB, LANE), 0.5 * beta_ref[s, l], F32))
                ct[k, 0] = cos_h
                ct[k, 1] = sin_h
                ct[k, 2] = -sin_h

        def weights(k, slot):
            c, t = ct[k, 0], ct[k, 1]
            cp, tp = [jnp.ones_like(c)], [jnp.ones_like(c)]
            for _ in range(LANE_BITS):
                cp.append(cp[-1] * c)
                tp.append(tp[-1] * t)
            amp = [cp[LANE_BITS - d] * tp[d] for d in range(LANE_BITS + 1)]
            z = jnp.zeros_like(c)
            real = [z, z, z, z, z, z, z, z]
            imag = [z, z, z, z, z, z, z, z]
            for d in range(LANE_BITS + 1):
                if d % 4 == 0:
                    real[d] = amp[d]
                elif d % 4 == 1:
                    imag[d] = -amp[d]
                elif d % 4 == 2:
                    real[d] = -amp[d]
                else:
                    imag[d] = amp[d]

            def body(r, _):
                at = pl.multiple_of(r * 2 * SUB, 2 * SUB)
                rows_re, rows_im = [], []
                for h in range(2):
                    d = dmat[pl.ds(at + h * SUB, SUB), :]
                    re = z
                    im = z
                    for j in range(LANE_BITS + 1):
                        hit = d == j
                        if j % 2 == 0:
                            re = jnp.where(hit, real[j], re)
                        else:
                            im = jnp.where(hit, imag[j], im)
                    rows_re.append(re)
                    rows_im.append(im)
                re = jnp.concatenate(rows_re, axis=0)
                im = jnp.concatenate(rows_im, axis=0)
                for p, (a, b) in enumerate(zip(split3(re), split3(im))):
                    top = pl.ds(at, 2 * SUB)
                    bot = pl.ds(at + LANE, 2 * SUB)
                    wmat[slot, 0, p, top, 0:LANE] = a
                    wmat[slot, 0, p, top, LANE:] = b
                    wmat[slot, 0, p, bot, 0:LANE] = -b
                    wmat[slot, 0, p, bot, LANE:] = a
                    wmat[slot, 1, p, top, 0:LANE] = a
                    wmat[slot, 1, p, top, LANE:] = -b
                    wmat[slot, 1, p, bot, 0:LANE] = b
                    wmat[slot, 1, p, bot, LANE:] = a
                return 0
            lax.fori_loop(0, LANE // (2 * SUB), body, 0)

        def tile_rows(tile):
            return pl.ds(pl.multiple_of(tile * SUB, SUB), SUB)

        def load(ref, slot, tile):
            r = tile_rows(tile)
            return ref[slot, r, 0:LANE], ref[slot, r, LANE:]

        def store(ref, slot, tile, pair):
            r = tile_rows(tile)
            ref[slot, r, 0:LANE] = pair[0]
            ref[slot, r, LANE:] = pair[1]

        def mix_low(source, target, k, sign):
            c, t = ct[k, 0], ct[k, sign]

            def body(i, _):
                base, tile = (i // tiles) * lo, i % tiles
                v = [load(source, base + j, tile) for j in range(lo)]
                for b in lo_bits:
                    v = rot(v, b, c, t)
                for j in range(lo):
                    store(target, base + j, tile, v[j])
                return 0
            lax.fori_loop(0, hi * tiles, body, 0)

        def mid_pass(source, target, k_in, s_in, k_out, s_out, middle):
            if k_in is not None:
                c0, t0 = ct[k_in, 0], ct[k_in, s_in]
            if k_out is not None:
                c1, t1 = ct[k_out, 0], ct[k_out, s_out]

            def body(i, carry):
                base, tile = i // tiles, i % tiles
                slots = [base + j * lo for j in range(hi)]
                if source is None:
                    v = [None] * hi
                else:
                    v = [load(source, m, tile) for m in slots]
                if k_in is not None:
                    for b in hi_bits:
                        v = rot(v, b, c0, t0)
                v, carry = middle(v, slots, tile, carry)
                if k_out is not None:
                    for b in hi_bits:
                        v = rot(v, b, c1, t1)
                    for j in range(hi):
                        store(target, slots[j], tile, v[j])
                return carry
            return lax.fori_loop(0, lo * tiles, body, jnp.zeros((SUB, LANE), F32))

        def pre_mix_send(source, e, s, k, sign):
            c, t = ct[k, 0], ct[k, sign]
            half = n // 2

            def rows_body(i, _):
                base = i * lo
                v = [load(source, base + j // tiles, j % tiles) for j in range(lo * tiles)]
                for b in lo_bits:
                    v = rot(v, b * tiles, c, t)
                for b in tile_bits:
                    v = rot(v, b, c, t)
                for j in range(lo * tiles):
                    re, im = v[j]
                    for b in range(3):
                        fr, fi = sub_flip(re, b), sub_flip(im, b)
                        re, im = c * re + t * fi, c * im - t * fr
                    m = j // tiles
                    store(tmp, (m % 2) * half + i * (lo // 2) + m // 2, j % tiles, (re, im))
                return 0
            lax.fori_loop(0, hi, rows_body, 0)

            def lanes(core):
                at = pl.ds(pl.multiple_of(core * half, half), half)
                m = half * rows
                x = tmp[at].reshape(m, 2 * LANE)
                xh, xm, xl = split3(x)
                w = [wmat[k, sign - 1, p] for p in range(3)]
                a = mm(jnp.concatenate([xh, xm, xl], axis=0), w[0])
                b = mm(jnp.concatenate([xh, xm], axis=0), w[1])
                y = a[:m] + (b[:m] + a[m:2 * m]) + (mm(xh, w[2]) + b[m:] + a[2 * m:])
                src[e, s, at] = y.reshape(half, rows, 2 * LANE)

            def send_slot(ty, tx):
                send(src.at[e, s, by_core(ty, tx)], dst.at[e, s, me], (e, s), ty, tx)
            other_core = lax.rem(me_core + 1, 2)
            lanes(other_core)
            peers_in_order(send_slot, ORDER_OTHER, other_core)
            lanes(me_core)
            peers_in_order(send_slot, ORDER_LIKE, me_core)
            dst[e, s, me] = src[e, s, by_core(qy, qx)]

        def im_dot(a, b):
            return a[0] * b[1] - a[1] * b[0]

        def slot_dot(bra, ket):
            def group(slots, tile, bits, a):
                x = [load(bra, m, tile) for m in slots]
                y = [load(ket, m, tile) for m in slots]
                for j in range(len(slots)):
                    re = sum(y[j ^ b][0] for b in bits[1:]) + y[j ^ bits[0]][0] if len(bits) > 1 else y[j ^ bits[0]][0]
                    im = sum(y[j ^ b][1] for b in bits[1:]) + y[j ^ bits[0]][1] if len(bits) > 1 else y[j ^ bits[0]][1]
                    a = a + im_dot(x[j], (re, im))
                return a

            def low(i, a):
                return group([(i // tiles) * lo + j for j in range(lo)], i % tiles, lo_bits, a)

            def high(i, a):
                return group([i // tiles + j * lo for j in range(hi)], i % tiles, hi_bits, a)
            a = lax.fori_loop(0, hi * tiles, low, jnp.zeros((SUB, LANE), F32))
            return lax.fori_loop(0, lo * tiles, high, a)

        def fold(x):
            while x.shape[0] > SUB:
                half = x.shape[0] // 2
                x = x[:half] + x[half:]
            return x

        def inner_x(x):
            xh, xm, xl = split3(x)
            y = mm(xh, adj[...]) + mm(xm, adj[...]) + mm(xl, adj[...])
            return y

        def tile_flips(v):
            out = []
            for j in range(len(v)):
                parts_ = []
                for comp in range(2):
                    x = v[j][comp]
                    f = sub_flip(x, 0) + sub_flip(x, 1) + sub_flip(x, 2)
                    for b in tile_bits:
                        f = f + v[j ^ b][comp]
                    parts_.append(f)
                out.append(tuple(parts_))
            return out

        def inner_apply(ket, target):
            def body(i, _):
                at = pl.ds(pl.multiple_of(i * lo, lo), lo)
                y = inner_x(ket[at].reshape(lo * rows, 2 * LANE))
                target[at] = y.reshape(lo, rows, 2 * LANE)
                return 0
            lax.fori_loop(0, hi, body, 0)

            def add(i, _):
                v = [load(ket, i, j) for j in range(tiles)]
                f = tile_flips(v)
                for j in range(tiles):
                    y = load(target, i, j)
                    store(target, i, j, (y[0] + f[j][0], y[1] + f[j][1]))
                return 0
            lax.fori_loop(0, n, add, 0)

        def inner_dots(bra, ket, cost):
            inner_apply(ket, tmp)

            def body(i, carry):
                a, g = carry
                for j in range(tiles):
                    x = load(bra, i, j)
                    a = a + im_dot(x, load(tmp, i, j))
                    g = g + cost[i, tile_rows(j), :] * im_dot(x, load(ket, i, j))
                return a, g
            z = jnp.zeros((SUB, LANE), F32)
            return lax.fori_loop(0, n, body, (z, z))

        def two_dots(bra, ket_b, ket_c):
            def body(i, carry):
                a, g = carry
                for j in range(tiles):
                    x = load(bra, i, j)
                    a = a + im_dot(x, load(ket_b, i, j))
                    g = g + im_dot(x, load(ket_c, i, j))
                return a, g
            z = jnp.zeros((SUB, LANE), F32)
            return lax.fori_loop(0, n, body, (z, z))

        def slot_x(source, target):
            def low(i, _):
                base, tile = (i // tiles) * lo, i % tiles
                y = [load(source, base + j, tile) for j in range(lo)]
                for j in range(lo):
                    o = load(target, base + j, tile)
                    store(target, base + j, tile, tuple(o[c] + (y[j ^ 1][c] + y[j ^ 2][c] + y[j ^ 4][c]) for c in range(2)))
                return 0
            lax.fori_loop(0, hi * tiles, low, 0)

            def high(i, _):
                base, tile = i // tiles, i % tiles
                y = [load(source, base + j * lo, tile) for j in range(hi)]
                for j in range(hi):
                    o = load(target, base + j * lo, tile)
                    store(target, base + j * lo, tile, tuple(o[c] + (y[j ^ 1][c] + y[j ^ 2][c]) for c in range(2)))
                return 0
            lax.fori_loop(0, lo * tiles, high, 0)

        def slot_mix_all(ref, k):
            mix_low(ref, ref, k, 1)
            mid_pass(ref, ref, None, 1, k, 1, lambda v, slots, tile, a: (v, a))

        def fill_table(ref, cost, s, l, scale):
            g = gamma_ref[s, l]

            def body(i, _):
                for j in range(tiles):
                    sn, cs = sincos(cost[i, tile_rows(j), :] * g)
                    if scale is None:
                        store(ref, i, j, (cs, sn))
                    else:
                        store(ref, i, j, (cs * scale, sn * -scale))
                return 0
            lax.fori_loop(0, n, body, 0)

        def kk(s, l):
            return s * num_layers + l

        def add_acc(s, q, a, init=False):
            row = s * 8 + q
            acc[row] = a if init else acc[row] + a


        def each_set(f):
            lax.fori_loop(0, num_sets, lambda s, _: (f(s), 0)[1], 0)

        def first_state(s):
            weights(kk(s, 0), kk(s, 0))
            fill_table(keep.at[0, s], cost_ref, s, 0, norm)

        first_state(0)
        pl.semaphore_wait(barrier, n - 1)
        each_peer(lambda ty, tx: send(cost_ref.at[ty * nx + tx], cost_b.at[me], (6, 0), ty, tx))
        cost_b[me] = cost_ref[me]

        def set_weights(i, _):
            k = (i // (num_layers - 1)) * num_layers + 1 + i % (num_layers - 1)
            weights(k, k)
            return 0

        def forward_mid(before, after, table):
            def middle(v, slots, tile, a):
                out = []
                for m, (re, im) in zip(slots, v):
                    store(before, m, tile, (re, im))
                    cs, sn = load(table, m, tile)
                    p = (re * cs + im * sn, im * cs - re * sn)
                    store(after, m, tile, p)
                    out.append(p)
                return out, a
            return middle

        def backward_mid(before, after, table):
            def middle(v, slots, tile, a):
                out = []
                for m, (re, im) in zip(slots, v):
                    store(before, m, tile, (re, im))
                    cs, sn = load(table, m, tile)
                    p = (re * cs - im * sn, im * cs + re * sn)
                    store(after, m, tile, p)
                    out.append(p)
                return out, a
            return middle

        def turn_mid(psi, lam):
            def middle(v, slots, tile, a):
                out = []
                for m, (re, im) in zip(slots, v):
                    store(psi, m, tile, (re, im))
                    w = cost_b[m, tile_rows(tile), :]
                    p = (w * re, w * im)
                    a = a + (p[0] * re + p[1] * im)
                    store(lam, m, tile, p)
                    out.append(p)
                return out, a
            return middle

        def stage(e, s):
            k_out = kk(s, e - (e // 3) * (2 * e - 5))
            s_out = 1 + e // 3
            k_in = kk(s, e - 1 - (e // 4) * (2 * e - 7))
            s_in = 1 + e // 4
            before, after = keep.at[2 * e - 1, s], keep.at[2 * e, s]

            @pl.when(e == 0)
            def _():
                @pl.when(s > 0)
                def _():
                    first_state(s)
                mid_pass(keep.at[0, s], other, None, 1, k_out, s_out, lambda v, slots, tile, a: (v, a))

            @pl.when(e > 0)
            def _():
                wait_bytes(dst.at[e - 1, s], recv_sem.at[e - 1, s])
                mix_low(dst.at[e - 1, s], other, k_in, s_in)

                @pl.when(e < 3)
                def _():
                    mid_pass(other, other, k_in, s_in, k_out, s_out, forward_mid(before, after, tab.at[e - 1, s]))

                @pl.when(e == 3)
                def _():
                    add_acc(s, 0, mid_pass(other, other, k_in, s_in, k_out, s_out, turn_mid(before, after)), True)

                @pl.when(e > 3)
                def _():
                    mid_pass(other, other, k_in, s_in, k_out, s_out, backward_mid(before, after, tab.at[5 - e, s]))

            pre_mix_send(other, e, s, k_out, s_out)

            @pl.when(e * num_sets + s == 1)
            def _():
                lax.fori_loop(0, num_sets * (num_layers - 1), set_weights, 0)
                each_set(lambda i: fill_table(tab.at[1, i], cost_ref, i, 2, None))
                wait_bytes(cost_b, recv_sem.at[6, 0])
                each_set(lambda i: fill_table(tab.at[0, i], cost_b, i, 1, None))

            @pl.when(e == 2)
            def _():
                inner_apply(keep.at[0, s], psi_b.at[s])
                slot_x(keep.at[0, s], psi_b.at[s])
                slot_mix_all(psi_b.at[s], kk(s, 0))

                def times_cost(i, _):
                    for j in range(tiles):
                        re, im = load(keep.at[0, s], i, j)
                        w = cost_ref[i, tile_rows(j), :]
                        store(psi_c.at[s], i, j, (w * re, w * im))
                    return 0
                lax.fori_loop(0, n, times_cost, 0)
                slot_mix_all(psi_c.at[s], kk(s, 0))

            @pl.when(e == 3)
            def _():
                add_acc(s, 6, slot_dot(after, before), True)

            @pl.when(e > 3)
            def _():
                ket = keep.at[12 - 2 * e, s]
                ket_before = keep.at[11 - 2 * e, s]

                def add_dots(cost):
                    b, g = inner_dots(before, ket, cost)
                    acc[s * 8 + 10 - e] = acc[s * 8 + 10 - e] + (b + slot_dot(before, ket))
                    acc[s * 8 + 7 - e] = 2.0 * g
                    acc[s * 8 + 9 - e] = slot_dot(after, ket_before)
                pl.when(e == 4)(lambda: add_dots(cost_ref))
                pl.when(e == 5)(lambda: add_dots(cost_b))

        def each_exchange(e, _):
            each_set(lambda s: stage(e, s))
            return 0
        lax.fori_loop(0, 2 * num_layers, each_exchange, 0)

        lane = lax.broadcasted_iota(jnp.int32, (1, LANE), 1)

        def place(q, a):
            total = jnp.sum(jnp.sum(a, axis=0, keepdims=True), axis=1, keepdims=True)
            return jnp.where(lane == q, total, 0.0)

        def partial(s):
            wait_bytes(dst.at[5, s], recv_sem.at[5, s])
            b, g = two_dots(dst.at[5, s], psi_b.at[s], psi_c.at[s])
            return place(4, acc[s * 8 + 4] + b) + place(1, 2.0 * g)

        rest = []
        for s in range(num_sets):
            rest.append(sum(place(q, acc[s * 8 + q]) for q in (2, 3, 5, 6)) + place(0, acc[s * 8]))
        for s in range(num_sets):
            mine[s:s + 1, :] = rest[s] + partial(s)

        parts[me] = mine[...]
        each_peer_far_first(lambda ty, tx: send(mine, parts.at[me], (6, 1), ty, tx))
        wait_bytes(parts, recv_sem.at[6, 1])
        for e in range(6):
            for s in range(num_sets):
                wait_bytes(src.at[e, s], send_sem.at[e, s])
        wait_bytes(cost_b, send_sem.at[6, 0])
        wait_bytes(parts, send_sem.at[6, 1])

    return kernel


def solution(mesh):
    ny, nx = mesh.shape['qy'], mesh.shape['qx']
    n = ny * nx

    def device_fn(cost, gamma, beta):
        size = cost.shape[0]
        num_sets, num_layers = gamma.shape
        rows = size // (LANE * n)
        bits = (size * n).bit_length() - 1
        norm = 2.0 ** (-0.5 * bits)
        state = (n, rows, 2 * LANE)
        smem = pl.BlockSpec(memory_space=pltpu.SMEM)
        parts = pl.pallas_call(
            make_kernel(ny, nx, num_sets, num_layers, rows, norm),
            out_shape=jax.ShapeDtypeStruct((n, num_sets, LANE), F32),
            in_specs=[pl.BlockSpec(memory_space=pltpu.VMEM), smem, smem],
            out_specs=pl.BlockSpec(memory_space=pltpu.VMEM),
            scratch_shapes=[
                pltpu.VMEM((n, rows, LANE), F32),
                pltpu.VMEM((6, num_sets) + state, F32),
                pltpu.VMEM((6, num_sets) + state, F32),
                pltpu.VMEM((11, num_sets) + state, F32),
                pltpu.VMEM((2, num_sets) + state, F32),
                pltpu.VMEM((num_sets,) + state, F32),
                pltpu.VMEM((num_sets,) + state, F32),
                pltpu.VMEM((num_sets * num_layers, 2, 3, 2 * LANE, 2 * LANE), BF16),
                pltpu.VMEM((2 * LANE, 2 * LANE), BF16),
                pltpu.VMEM((LANE, LANE), jnp.int32),
                pltpu.VMEM((num_sets * num_layers, 3, SUB, LANE), F32),
                pltpu.VMEM((num_sets * 8, SUB, LANE), F32),
                pltpu.VMEM((num_sets, LANE), F32),
                pltpu.VMEM(state, F32),
                pltpu.VMEM(state, F32),
                pltpu.SemaphoreType.DMA((7, 2)),
                pltpu.SemaphoreType.DMA((7, 2)),
            ],
            compiler_params=pltpu.CompilerParams(collective_id=0, has_side_effects=True, vmem_limit_bytes=60 * 2 ** 20),
            name='qaoa',
        )(cost.reshape(n, rows, LANE), gamma, beta)

        def finish(parts_ref, e_ref, g_ref):
            total = jnp.sum(parts_ref[...], axis=0)
            g_ref[...] = total[:, 1:1 + 2 * num_layers]
            for s in range(num_sets):
                e_ref[s] = total[s, 0]

        return pl.pallas_call(
            finish,
            out_shape=(jax.ShapeDtypeStruct((num_sets,), F32), jax.ShapeDtypeStruct((num_sets, 2 * num_layers), F32)),
            in_specs=[pl.BlockSpec(memory_space=pltpu.VMEM)],
            out_specs=(smem, pl.BlockSpec(memory_space=pltpu.VMEM)),
            name='finish',
        )(parts)

    cost_spec = P(('inst', 'qy', 'qx'))
    angle_spec = P('inst', None)
    return jax.shard_map(device_fn, mesh=mesh, in_specs=(cost_spec, angle_spec, angle_spec), out_specs=(P('inst'), angle_spec), check_vma=False)
```

```python
import functools
import jax
import jax.numpy as jnp
from jax import lax
from jax.experimental import pallas as pl
from jax.experimental.pallas import tpu as pltpu
from jax.sharding import PartitionSpec as P

LANE = 128
LANE_BITS = 7
SUB = 8
ORDER_OTHER = [(1, 1), (1, 3), (1, 2), (1, 0), (2, 1), (2, 3), (2, 2), (2, 0), (3, 1), (3, 3), (3, 2), (3, 0), (0, 1), (0, 3), (0, 2), (0, 0)]
ORDER_LIKE = [(1, 1), (1, 3), (1, 2), (1, 0), (2, 1), (2, 3), (2, 2), (2, 0), (3, 1), (3, 3), (3, 2), (3, 0), (0, 1), (0, 3), (0, 2)]
MESH_ID = pl.DeviceIdType.MESH
F32 = jnp.float32
BF16 = jnp.bfloat16


def sincos(x):
    k = jnp.floor(x * 0.6366197723675814 + 0.5)
    r = ((x - k * 1.5703125) - k * 4.837512969970703125e-4) - k * 7.54978995489188216e-8
    z = r * r
    s = r + r * z * (-1.6666654611e-1 + z * (8.3321608736e-3 + z * -1.9515295891e-4))
    c = (1.0 - 0.5 * z) + z * z * (4.166664568298827e-2 + z * (-1.388731625493765e-3 + z * 2.443315711809948e-5))
    q = k.astype(jnp.int32)
    odd = (q & 1) != 0
    sin_v = jnp.where(odd, c, s)
    cos_v = jnp.where(odd, s, c)
    sin_v = jnp.where((q & 2) != 0, -sin_v, sin_v)
    cos_v = jnp.where(((q + 1) & 2) != 0, -cos_v, cos_v)
    return sin_v, cos_v


def split3(x):
    hi = x.astype(BF16)
    rest = x - hi.astype(F32)
    mid = rest.astype(BF16)
    low = (rest - mid.astype(F32)).astype(BF16)
    return hi, mid, low


def mm(a, b):
    return jnp.dot(a, b, preferred_element_type=F32)


def rot(pairs, stride, c, t):
    out = list(pairs)
    for j in range(len(pairs)):
        if j & stride:
            continue
        (ar, ai), (br, bi) = pairs[j], pairs[j | stride]
        out[j] = (c * ar + t * bi, c * ai - t * br)
        out[j | stride] = (c * br + t * ai, c * bi - t * ar)
    return out


def sub_flip(x, bit):
    if bit == 2:
        return pltpu.roll(x, 4, 0)
    row = lax.broadcasted_iota(jnp.int32, (SUB, LANE), 0)
    up = pltpu.roll(x, 1 << bit, 0)
    down = pltpu.roll(x, SUB - (1 << bit), 0)
    return jnp.where((row & (1 << bit)) != 0, up, down)


def make_kernel(ny, nx, num_sets, num_layers, rows, norm):
    n = ny * nx
    lo = 8
    hi = n // lo
    tiles = rows // SUB
    lo_bits = [1 << b for b in range(lo.bit_length() - 1)]
    hi_bits = [1 << b for b in range(hi.bit_length() - 1)]
    tile_bits = [1 << b for b in range(tiles.bit_length() - 1)]
    width_x = nx // 2

    def kernel(cost_ref, gamma_ref, beta_ref, parts,
               cost_b, src, dst, keep, tab, psi_b, psi_c, wmat, adj, dmat, ct, acc, mine, tmp, other, send_sem, recv_sem):
        qy = lax.axis_index('qy')
        qx = lax.axis_index('qx')
        me = qy * nx + qx
        barrier = pltpu.get_barrier_semaphore()

        me_core = lax.rem(qx, 2)

        def ring_x(order):
            return [lax.rem(qx // 2 + dx, width_x) * 2 for dx in order]
        chip_x = ring_x((1, 3, 2, 0))
        far_x = ring_x((2, 1, 3, 0))

        def peers_of_core(act, core, last):
            def body(i, _):
                ty = lax.rem(qy + 1 + i, ny)
                for tx in chip_x[:-1]:
                    act(ty, tx + core)

                @pl.when(i + last < ny)
                def _():
                    act(ty, chip_x[-1] + core)
                return 0
            lax.fori_loop(0, ny, body, 0)

        def peers_in_order(act, order, core):
            for part in range(tiles):
                for dy, dx in order:
                    act(lax.rem(qy + dy, ny), lax.rem(qx // 2 + dx, width_x) * 2 + core, part)

        def both_cores(f):
            lax.fori_loop(0, 2, lambda h, _: (f(lax.rem(me_core + 1 + h, 2), h), 0)[1], 0)

        def each_peer(act):
            both_cores(lambda core, last: peers_of_core(act, core, last))

        def each_peer_far_first(act):
            def body(i, _):
                a = i // 2
                ty = lax.rem(qy + 2 - a + (a // 2) * (7 - 2 * a), ny)
                core = lax.rem(qx + 1 + i, 2)
                for tx in far_x[:-1]:
                    act(ty, tx + core)

                @pl.when(i < 2 * ny - 1)
                def _():
                    act(ty, far_x[-1] + core)
                return 0
            lax.fori_loop(0, 2 * ny, body, 0)

        def greet(ty, tx):
            pl.semaphore_signal(barrier, inc=1, device_id={'qy': ty, 'qx': tx}, device_id_type=MESH_ID)
        each_peer_far_first(greet)

        def send(source, target, ids, ty, tx):
            pltpu.make_async_remote_copy(
                source, target, send_sem.at[ids], recv_sem.at[ids],
                device_id={'qy': ty, 'qx': tx}, device_id_type=MESH_ID).start()

        def by_core(ty, tx):
            return lax.rem(tx, 2) * (n // 2) + ty * width_x + tx // 2

        def wait_bytes(buf, sem):
            part = buf.at[pl.ds(0, n - 1)]
            pltpu.make_async_copy(part, part, sem).wait()

        def tile_d(r, _):
            a = lax.broadcasted_iota(jnp.int32, (SUB, LANE), 0) + r * SUB
            b = lax.broadcasted_iota(jnp.int32, (SUB, LANE), 1)
            x = a ^ b
            d = jnp.zeros_like(x)
            for k in range(LANE_BITS):
                d = d + ((x >> k) & 1)
            dmat[pl.ds(pl.multiple_of(r * SUB, SUB), SUB), :] = d
            return 0
        lax.fori_loop(0, LANE // SUB, tile_d, 0)
        one = (dmat[...] == 1).astype(F32).astype(BF16)
        zero = jnp.zeros((LANE, LANE), BF16)
        adj[0:LANE, 0:LANE] = one
        adj[0:LANE, LANE:] = zero
        adj[LANE:, 0:LANE] = zero
        adj[LANE:, LANE:] = one
        for s in range(num_sets):
            for l in range(num_layers):
                k = s * num_layers + l
                sin_h, cos_h = sincos(jnp.full((SUB, LANE), 0.5 * beta_ref[s, l], F32))
                ct[k, 0] = cos_h
                ct[k, 1] = sin_h
                ct[k, 2] = -sin_h

        def weights(k, slot):
            c, t = ct[k, 0], ct[k, 1]
            cp, tp = [jnp.ones_like(c)], [jnp.ones_like(c)]
            for _ in range(LANE_BITS):
                cp.append(cp[-1] * c)
                tp.append(tp[-1] * t)
            amp = [cp[LANE_BITS - d] * tp[d] for d in range(LANE_BITS + 1)]
            z = jnp.zeros_like(c)
            real = [z, z, z, z, z, z, z, z]
            imag = [z, z, z, z, z, z, z, z]
            for d in range(LANE_BITS + 1):
                if d % 4 == 0:
                    real[d] = amp[d]
                elif d % 4 == 1:
                    imag[d] = -amp[d]
                elif d % 4 == 2:
                    real[d] = -amp[d]
                else:
                    imag[d] = amp[d]

            def body(r, _):
                at = pl.multiple_of(r * 2 * SUB, 2 * SUB)
                rows_re, rows_im = [], []
                for h in range(2):
                    d = dmat[pl.ds(at + h * SUB, SUB), :]
                    re = z
                    im = z
                    for j in range(LANE_BITS + 1):
                        hit = d == j
                        if j % 2 == 0:
                            re = jnp.where(hit, real[j], re)
                        else:
                            im = jnp.where(hit, imag[j], im)
                    rows_re.append(re)
                    rows_im.append(im)
                re = jnp.concatenate(rows_re, axis=0)
                im = jnp.concatenate(rows_im, axis=0)
                for p, (a, b) in enumerate(zip(split3(re), split3(im))):
                    top = pl.ds(at, 2 * SUB)
                    bot = pl.ds(at + LANE, 2 * SUB)
                    wmat[slot, 0, p, top, 0:LANE] = a
                    wmat[slot, 0, p, top, LANE:] = b
                    wmat[slot, 0, p, bot, 0:LANE] = -b
                    wmat[slot, 0, p, bot, LANE:] = a
                    wmat[slot, 1, p, top, 0:LANE] = a
                    wmat[slot, 1, p, top, LANE:] = -b
                    wmat[slot, 1, p, bot, 0:LANE] = b
                    wmat[slot, 1, p, bot, LANE:] = a
                return 0
            lax.fori_loop(0, LANE // (2 * SUB), body, 0)

        def tile_rows(tile):
            return pl.ds(pl.multiple_of(tile * SUB, SUB), SUB)

        def load(ref, slot, tile):
            r = tile_rows(tile)
            return ref[slot, r, 0:LANE], ref[slot, r, LANE:]

        def store(ref, slot, tile, pair):
            r = tile_rows(tile)
            ref[slot, r, 0:LANE] = pair[0]
            ref[slot, r, LANE:] = pair[1]

        def mix_low(source, target, k, sign):
            c, t = ct[k, 0], ct[k, sign]

            def body(i, _):
                base, tile = (i // tiles) * lo, i % tiles
                v = [load(source, base + j, tile) for j in range(lo)]
                for b in lo_bits:
                    v = rot(v, b, c, t)
                for j in range(lo):
                    store(target, base + j, tile, v[j])
                return 0
            lax.fori_loop(0, hi * tiles, body, 0)

        def mid_pass(source, target, k_in, s_in, k_out, s_out, middle):
            if k_in is not None:
                c0, t0 = ct[k_in, 0], ct[k_in, s_in]
            if k_out is not None:
                c1, t1 = ct[k_out, 0], ct[k_out, s_out]

            def body(i, carry):
                base, tile = i // tiles, i % tiles
                slots = [base + j * lo for j in range(hi)]
                if source is None:
                    v = [None] * hi
                else:
                    v = [load(source, m, tile) for m in slots]
                if k_in is not None:
                    for b in hi_bits:
                        v = rot(v, b, c0, t0)
                v, carry = middle(v, slots, tile, carry)
                if k_out is not None:
                    for b in hi_bits:
                        v = rot(v, b, c1, t1)
                    for j in range(hi):
                        store(target, slots[j], tile, v[j])
                return carry
            return lax.fori_loop(0, lo * tiles, body, jnp.zeros((SUB, LANE), F32))

        def pre_mix_send(source, e, s, k, sign):
            c, t = ct[k, 0], ct[k, sign]
            half = n // 2

            def rows_body(i, _):
                base = i * lo
                v = [load(source, base + j // tiles, j % tiles) for j in range(lo * tiles)]
                for b in lo_bits:
                    v = rot(v, b * tiles, c, t)
                for b in tile_bits:
                    v = rot(v, b, c, t)
                for j in range(lo * tiles):
                    re, im = v[j]
                    for b in range(3):
                        fr, fi = sub_flip(re, b), sub_flip(im, b)
                        re, im = c * re + t * fi, c * im - t * fr
                    m = j // tiles
                    store(tmp, (m % 2) * half + i * (lo // 2) + m // 2, j % tiles, (re, im))
                return 0
            lax.fori_loop(0, hi, rows_body, 0)

            def lanes(core):
                at = pl.ds(pl.multiple_of(core * half, half), half)
                m = half * rows
                x = tmp[at].reshape(m, 2 * LANE)
                xh, xm, xl = split3(x)
                w = [wmat[k, sign - 1, p] for p in range(3)]
                a = mm(jnp.concatenate([xh, xm, xl], axis=0), w[0])
                b = mm(jnp.concatenate([xh, xm], axis=0), w[1])
                y = a[:m] + (b[:m] + a[m:2 * m]) + (mm(xh, w[2]) + b[m:] + a[2 * m:])
                src[e, s, at] = y.reshape(half, rows, 2 * LANE)

            def send_slot(ty, tx, part):
                r = pl.ds(part * SUB, SUB)
                send(src.at[e, s, by_core(ty, tx), r], dst.at[e, s, me, r], (e, s), ty, tx)
            other_core = lax.rem(me_core + 1, 2)
            lanes(other_core)
            lanes(me_core)
            peers_in_order(send_slot, ORDER_OTHER, other_core)
            peers_in_order(send_slot, ORDER_LIKE, me_core)
            dst[e, s, me] = src[e, s, by_core(qy, qx)]

        def im_dot(a, b):
            return a[0] * b[1] - a[1] * b[0]

        def slot_dot(bra, ket):
            def group(slots, tile, bits, a):
                x = [load(bra, m, tile) for m in slots]
                y = [load(ket, m, tile) for m in slots]
                for j in range(len(slots)):
                    re = sum(y[j ^ b][0] for b in bits[1:]) + y[j ^ bits[0]][0] if len(bits) > 1 else y[j ^ bits[0]][0]
                    im = sum(y[j ^ b][1] for b in bits[1:]) + y[j ^ bits[0]][1] if len(bits) > 1 else y[j ^ bits[0]][1]
                    a = a + im_dot(x[j], (re, im))
                return a

            def low(i, a):
                return group([(i // tiles) * lo + j for j in range(lo)], i % tiles, lo_bits, a)

            def high(i, a):
                return group([i // tiles + j * lo for j in range(hi)], i % tiles, hi_bits, a)
            a = lax.fori_loop(0, hi * tiles, low, jnp.zeros((SUB, LANE), F32))
            return lax.fori_loop(0, lo * tiles, high, a)

        def fold(x):
            while x.shape[0] > SUB:
                half = x.shape[0] // 2
                x = x[:half] + x[half:]
            return x

        def inner_x(x):
            xh, xm, xl = split3(x)
            y = mm(xh, adj[...]) + mm(xm, adj[...]) + mm(xl, adj[...])
            return y

        def tile_flips(v):
            out = []
            for j in range(len(v)):
                parts_ = []
                for comp in range(2):
                    x = v[j][comp]
                    f = sub_flip(x, 0) + sub_flip(x, 1) + sub_flip(x, 2)
                    for b in tile_bits:
                        f = f + v[j ^ b][comp]
                    parts_.append(f)
                out.append(tuple(parts_))
            return out

        def inner_apply(ket, target):
            def body(i, _):
                at = pl.ds(pl.multiple_of(i * lo, lo), lo)
                y = inner_x(ket[at].reshape(lo * rows, 2 * LANE))
                target[at] = y.reshape(lo, rows, 2 * LANE)
                return 0
            lax.fori_loop(0, hi, body, 0)

            def add(i, _):
                v = [load(ket, i, j) for j in range(tiles)]
                f = tile_flips(v)
                for j in range(tiles):
                    y = load(target, i, j)
                    store(target, i, j, (y[0] + f[j][0], y[1] + f[j][1]))
                return 0
            lax.fori_loop(0, n, add, 0)

        def inner_dots(bra, ket, cost):
            inner_apply(ket, tmp)

            def body(i, carry):
                a, g = carry
                for j in range(tiles):
                    x = load(bra, i, j)
                    a = a + im_dot(x, load(tmp, i, j))
                    g = g + cost[i, tile_rows(j), :] * im_dot(x, load(ket, i, j))
                return a, g
            z = jnp.zeros((SUB, LANE), F32)
            return lax.fori_loop(0, n, body, (z, z))

        def two_dots(bra, ket_b, ket_c):
            def body(i, carry):
                a, g = carry
                for j in range(tiles):
                    x = load(bra, i, j)
                    a = a + im_dot(x, load(ket_b, i, j))
                    g = g + im_dot(x, load(ket_c, i, j))
                return a, g
            z = jnp.zeros((SUB, LANE), F32)
            return lax.fori_loop(0, n, body, (z, z))

        def slot_x(source, target):
            def low(i, _):
                base, tile = (i // tiles) * lo, i % tiles
                y = [load(source, base + j, tile) for j in range(lo)]
                for j in range(lo):
                    o = load(target, base + j, tile)
                    store(target, base + j, tile, tuple(o[c] + (y[j ^ 1][c] + y[j ^ 2][c] + y[j ^ 4][c]) for c in range(2)))
                return 0
            lax.fori_loop(0, hi * tiles, low, 0)

            def high(i, _):
                base, tile = i // tiles, i % tiles
                y = [load(source, base + j * lo, tile) for j in range(hi)]
                for j in range(hi):
                    o = load(target, base + j * lo, tile)
                    store(target, base + j * lo, tile, tuple(o[c] + (y[j ^ 1][c] + y[j ^ 2][c]) for c in range(2)))
                return 0
            lax.fori_loop(0, lo * tiles, high, 0)

        def slot_mix_all(ref, k):
            mix_low(ref, ref, k, 1)
            mid_pass(ref, ref, None, 1, k, 1, lambda v, slots, tile, a: (v, a))

        def fill_table(ref, cost, s, l, scale):
            g = gamma_ref[s, l]

            def body(i, _):
                for j in range(tiles):
                    sn, cs = sincos(cost[i, tile_rows(j), :] * g)
                    if scale is None:
                        store(ref, i, j, (cs, sn))
                    else:
                        store(ref, i, j, (cs * scale, sn * -scale))
                return 0
            lax.fori_loop(0, n, body, 0)

        def kk(s, l):
            return s * num_layers + l

        def add_acc(s, q, a, init=False):
            row = s * 8 + q
            acc[row] = a if init else acc[row] + a


        def each_set(f):
            lax.fori_loop(0, num_sets, lambda s, _: (f(s), 0)[1], 0)

        def first_state(s):
            weights(kk(s, 0), kk(s, 0))
            fill_table(keep.at[0, s], cost_ref, s, 0, norm)

        first_state(0)
        pl.semaphore_wait(barrier, n - 1)
        each_peer(lambda ty, tx: send(cost_ref.at[ty * nx + tx], cost_b.at[me], (6, 0), ty, tx))
        cost_b[me] = cost_ref[me]

        def set_weights(i, _):
            k = (i // (num_layers - 1)) * num_layers + 1 + i % (num_layers - 1)
            weights(k, k)
            return 0

        def forward_mid(before, after, table):
            def middle(v, slots, tile, a):
                out = []
                for m, (re, im) in zip(slots, v):
                    store(before, m, tile, (re, im))
                    cs, sn = load(table, m, tile)
                    p = (re * cs + im * sn, im * cs - re * sn)
                    store(after, m, tile, p)
                    out.append(p)
                return out, a
            return middle

        def backward_mid(before, after, table):
            def middle(v, slots, tile, a):
                out = []
                for m, (re, im) in zip(slots, v):
                    store(before, m, tile, (re, im))
                    cs, sn = load(table, m, tile)
                    p = (re * cs - im * sn, im * cs + re * sn)
                    store(after, m, tile, p)
                    out.append(p)
                return out, a
            return middle

        def turn_mid(psi, lam):
            def middle(v, slots, tile, a):
                out = []
                for m, (re, im) in zip(slots, v):
                    store(psi, m, tile, (re, im))
                    w = cost_b[m, tile_rows(tile), :]
                    p = (w * re, w * im)
                    a = a + (p[0] * re + p[1] * im)
                    store(lam, m, tile, p)
                    out.append(p)
                return out, a
            return middle

        def stage(e, s):
            k_out = kk(s, e - (e // 3) * (2 * e - 5))
            s_out = 1 + e // 3
            k_in = kk(s, e - 1 - (e // 4) * (2 * e - 7))
            s_in = 1 + e // 4
            before, after = keep.at[2 * e - 1, s], keep.at[2 * e, s]

            @pl.when(e == 0)
            def _():
                @pl.when(s > 0)
                def _():
                    first_state(s)
                mid_pass(keep.at[0, s], other, None, 1, k_out, s_out, lambda v, slots, tile, a: (v, a))

            @pl.when(e > 0)
            def _():
                wait_bytes(dst.at[e - 1, s], recv_sem.at[e - 1, s])
                mix_low(dst.at[e - 1, s], other, k_in, s_in)

                @pl.when(e < 3)
                def _():
                    mid_pass(other, other, k_in, s_in, k_out, s_out, forward_mid(before, after, tab.at[e - 1, s]))

                @pl.when(e == 3)
                def _():
                    add_acc(s, 0, mid_pass(other, other, k_in, s_in, k_out, s_out, turn_mid(before, after)), True)

                @pl.when(e > 3)
                def _():
                    mid_pass(other, other, k_in, s_in, k_out, s_out, backward_mid(before, after, tab.at[5 - e, s]))

            pre_mix_send(other, e, s, k_out, s_out)

            @pl.when(e * num_sets + s == 1)
            def _():
                lax.fori_loop(0, num_sets * (num_layers - 1), set_weights, 0)
                each_set(lambda i: fill_table(tab.at[1, i], cost_ref, i, 2, None))
                wait_bytes(cost_b, recv_sem.at[6, 0])
                each_set(lambda i: fill_table(tab.at[0, i], cost_b, i, 1, None))

            @pl.when(e == 2)
            def _():
                inner_apply(keep.at[0, s], psi_b.at[s])
                slot_x(keep.at[0, s], psi_b.at[s])
                slot_mix_all(psi_b.at[s], kk(s, 0))

                def times_cost(i, _):
                    for j in range(tiles):
                        re, im = load(keep.at[0, s], i, j)
                        w = cost_ref[i, tile_rows(j), :]
                        store(psi_c.at[s], i, j, (w * re, w * im))
                    return 0
                lax.fori_loop(0, n, times_cost, 0)
                slot_mix_all(psi_c.at[s], kk(s, 0))

            @pl.when(e == 3)
            def _():
                add_acc(s, 6, slot_dot(after, before), True)

            @pl.when(e > 3)
            def _():
                ket = keep.at[12 - 2 * e, s]
                ket_before = keep.at[11 - 2 * e, s]

                def add_dots(cost):
                    b, g = inner_dots(before, ket, cost)
                    acc[s * 8 + 10 - e] = acc[s * 8 + 10 - e] + (b + slot_dot(before, ket))
                    acc[s * 8 + 7 - e] = 2.0 * g
                    acc[s * 8 + 9 - e] = slot_dot(after, ket_before)
                pl.when(e == 4)(lambda: add_dots(cost_ref))
                pl.when(e == 5)(lambda: add_dots(cost_b))

        def each_exchange(e, _):
            each_set(lambda s: stage(e, s))
            return 0
        lax.fori_loop(0, 2 * num_layers, each_exchange, 0)

        lane = lax.broadcasted_iota(jnp.int32, (1, LANE), 1)

        def place(q, a):
            total = jnp.sum(jnp.sum(a, axis=0, keepdims=True), axis=1, keepdims=True)
            return jnp.where(lane == q, total, 0.0)

        def partial(s):
            wait_bytes(dst.at[5, s], recv_sem.at[5, s])
            b, g = two_dots(dst.at[5, s], psi_b.at[s], psi_c.at[s])
            return place(4, acc[s * 8 + 4] + b) + place(1, 2.0 * g)

        rest = []
        for s in range(num_sets):
            rest.append(sum(place(q, acc[s * 8 + q]) for q in (2, 3, 5, 6)) + place(0, acc[s * 8]))
        for s in range(num_sets):
            mine[s:s + 1, :] = rest[s] + partial(s)

        parts[me] = mine[...]
        each_peer_far_first(lambda ty, tx: send(mine, parts.at[me], (6, 1), ty, tx))
        wait_bytes(parts, recv_sem.at[6, 1])
        for e in range(6):
            for s in range(num_sets):
                wait_bytes(src.at[e, s], send_sem.at[e, s])
        wait_bytes(cost_b, send_sem.at[6, 0])
        wait_bytes(parts, send_sem.at[6, 1])

    return kernel


def solution(mesh):
    ny, nx = mesh.shape['qy'], mesh.shape['qx']
    n = ny * nx

    def device_fn(cost, gamma, beta):
        size = cost.shape[0]
        num_sets, num_layers = gamma.shape
        rows = size // (LANE * n)
        bits = (size * n).bit_length() - 1
        norm = 2.0 ** (-0.5 * bits)
        state = (n, rows, 2 * LANE)
        smem = pl.BlockSpec(memory_space=pltpu.SMEM)
        parts = pl.pallas_call(
            make_kernel(ny, nx, num_sets, num_layers, rows, norm),
            out_shape=jax.ShapeDtypeStruct((n, num_sets, LANE), F32),
            in_specs=[pl.BlockSpec(memory_space=pltpu.VMEM), smem, smem],
            out_specs=pl.BlockSpec(memory_space=pltpu.VMEM),
            scratch_shapes=[
                pltpu.VMEM((n, rows, LANE), F32),
                pltpu.VMEM((6, num_sets) + state, F32),
                pltpu.VMEM((6, num_sets) + state, F32),
                pltpu.VMEM((11, num_sets) + state, F32),
                pltpu.VMEM((2, num_sets) + state, F32),
                pltpu.VMEM((num_sets,) + state, F32),
                pltpu.VMEM((num_sets,) + state, F32),
                pltpu.VMEM((num_sets * num_layers, 2, 3, 2 * LANE, 2 * LANE), BF16),
                pltpu.VMEM((2 * LANE, 2 * LANE), BF16),
                pltpu.VMEM((LANE, LANE), jnp.int32),
                pltpu.VMEM((num_sets * num_layers, 3, SUB, LANE), F32),
                pltpu.VMEM((num_sets * 8, SUB, LANE), F32),
                pltpu.VMEM((num_sets, LANE), F32),
                pltpu.VMEM(state, F32),
                pltpu.VMEM(state, F32),
                pltpu.SemaphoreType.DMA((7, 2)),
                pltpu.SemaphoreType.DMA((7, 2)),
            ],
            compiler_params=pltpu.CompilerParams(collective_id=0, has_side_effects=True, vmem_limit_bytes=60 * 2 ** 20),
            name='qaoa',
        )(cost.reshape(n, rows, LANE), gamma, beta)

        def finish(parts_ref, e_ref, g_ref):
            total = jnp.sum(parts_ref[...], axis=0)
            g_ref[...] = total[:, 1:1 + 2 * num_layers]
            for s in range(num_sets):
                e_ref[s] = total[s, 0]

        return pl.pallas_call(
            finish,
            out_shape=(jax.ShapeDtypeStruct((num_sets,), F32), jax.ShapeDtypeStruct((num_sets, 2 * num_layers), F32)),
            in_specs=[pl.BlockSpec(memory_space=pltpu.VMEM)],
            out_specs=(smem, pl.BlockSpec(memory_space=pltpu.VMEM)),
            name='finish',
        )(parts)

    cost_spec = P(('inst', 'qy', 'qx'))
    angle_spec = P('inst', None)
    return jax.shard_map(device_fn, mesh=mesh, in_specs=(cost_spec, angle_spec, angle_spec), out_specs=(P('inst'), angle_spec), check_vma=False)
```

```python
import functools
import jax
import jax.numpy as jnp
from jax import lax
from jax.experimental import pallas as pl
from jax.experimental.pallas import tpu as pltpu
from jax.sharding import PartitionSpec as P

LANE = 128
LANE_BITS = 7
SUB = 8
ORDER_OTHER = [(2, 1), (2, 3), (2, 2), (2, 0), (1, 1), (1, 3), (1, 2), (1, 0), (3, 1), (3, 3), (3, 2), (3, 0), (0, 1), (0, 3), (0, 2), (0, 0)]
ORDER_LIKE = [(2, 1), (2, 3), (2, 2), (2, 0), (1, 1), (1, 3), (1, 2), (1, 0), (3, 1), (3, 3), (3, 2), (3, 0), (0, 1), (0, 3), (0, 2)]
MESH_ID = pl.DeviceIdType.MESH
F32 = jnp.float32
BF16 = jnp.bfloat16


def sincos(x):
    k = jnp.floor(x * 0.6366197723675814 + 0.5)
    r = ((x - k * 1.5703125) - k * 4.837512969970703125e-4) - k * 7.54978995489188216e-8
    z = r * r
    s = r + r * z * (-1.6666654611e-1 + z * (8.3321608736e-3 + z * -1.9515295891e-4))
    c = (1.0 - 0.5 * z) + z * z * (4.166664568298827e-2 + z * (-1.388731625493765e-3 + z * 2.443315711809948e-5))
    q = k.astype(jnp.int32)
    odd = (q & 1) != 0
    sin_v = jnp.where(odd, c, s)
    cos_v = jnp.where(odd, s, c)
    sin_v = jnp.where((q & 2) != 0, -sin_v, sin_v)
    cos_v = jnp.where(((q + 1) & 2) != 0, -cos_v, cos_v)
    return sin_v, cos_v


def split3(x):
    hi = x.astype(BF16)
    rest = x - hi.astype(F32)
    mid = rest.astype(BF16)
    low = (rest - mid.astype(F32)).astype(BF16)
    return hi, mid, low


def mm(a, b):
    return jnp.dot(a, b, preferred_element_type=F32)


def rot(pairs, stride, c, t):
    out = list(pairs)
    for j in range(len(pairs)):
        if j & stride:
            continue
        (ar, ai), (br, bi) = pairs[j], pairs[j | stride]
        out[j] = (c * ar + t * bi, c * ai - t * br)
        out[j | stride] = (c * br + t * ai, c * bi - t * ar)
    return out


def sub_flip(x, bit):
    if bit == 2:
        return pltpu.roll(x, 4, 0)
    row = lax.broadcasted_iota(jnp.int32, (SUB, LANE), 0)
    up = pltpu.roll(x, 1 << bit, 0)
    down = pltpu.roll(x, SUB - (1 << bit), 0)
    return jnp.where((row & (1 << bit)) != 0, up, down)


def make_kernel(ny, nx, num_sets, num_layers, rows, norm):
    n = ny * nx
    lo = 8
    hi = n // lo
    tiles = rows // SUB
    lo_bits = [1 << b for b in range(lo.bit_length() - 1)]
    hi_bits = [1 << b for b in range(hi.bit_length() - 1)]
    tile_bits = [1 << b for b in range(tiles.bit_length() - 1)]
    width_x = nx // 2

    def kernel(cost_ref, gamma_ref, beta_ref, out_ref,
               cost_b, src, dst, keep, tab, psi_b, psi_c, wmat, adj, dmat, ct, acc, mine, parts, tmp, other, send_sem, recv_sem):
        qy = lax.axis_index('qy')
        qx = lax.axis_index('qx')
        me = qy * nx + qx
        barrier = pltpu.get_barrier_semaphore()

        me_core = lax.rem(qx, 2)

        def ring_x(order):
            return [lax.rem(qx // 2 + dx, width_x) * 2 for dx in order]
        chip_x = ring_x((1, 3, 2, 0))
        far_x = ring_x((2, 1, 3, 0))

        def peers_of_core(act, core, last):
            def body(i, _):
                ty = lax.rem(qy + 1 + i, ny)
                for tx in chip_x[:-1]:
                    act(ty, tx + core)

                @pl.when(i + last < ny)
                def _():
                    act(ty, chip_x[-1] + core)
                return 0
            lax.fori_loop(0, ny, body, 0)

        def peers_in_order(act, order, core):
            for part in range(tiles):
                for dy, dx in order:
                    act(lax.rem(qy + dy, ny), lax.rem(qx // 2 + dx, width_x) * 2 + core, part)

        def both_cores(f):
            lax.fori_loop(0, 2, lambda h, _: (f(lax.rem(me_core + 1 + h, 2), h), 0)[1], 0)

        def each_peer(act):
            both_cores(lambda core, last: peers_of_core(act, core, last))

        def each_peer_far_first(act):
            def body(i, _):
                a = i // 2
                ty = lax.rem(qy + 2 - a + (a // 2) * (7 - 2 * a), ny)
                core = lax.rem(qx + 1 + i, 2)
                for tx in far_x[:-1]:
                    act(ty, tx + core)

                @pl.when(i < 2 * ny - 1)
                def _():
                    act(ty, far_x[-1] + core)
                return 0
            lax.fori_loop(0, 2 * ny, body, 0)

        def greet(ty, tx):
            pl.semaphore_signal(barrier, inc=1, device_id={'qy': ty, 'qx': tx}, device_id_type=MESH_ID)
        each_peer_far_first(greet)

        def send(source, target, ids, ty, tx):
            pltpu.make_async_remote_copy(
                source, target, send_sem.at[ids], recv_sem.at[ids],
                device_id={'qy': ty, 'qx': tx}, device_id_type=MESH_ID).start()

        def by_core(ty, tx):
            return lax.rem(tx, 2) * (n // 2) + ty * width_x + tx // 2

        def wait_bytes(buf, sem):
            part = buf.at[pl.ds(0, n - 1)]
            pltpu.make_async_copy(part, part, sem).wait()

        def tile_d(r, _):
            a = lax.broadcasted_iota(jnp.int32, (SUB, LANE), 0) + r * SUB
            b = lax.broadcasted_iota(jnp.int32, (SUB, LANE), 1)
            x = a ^ b
            d = jnp.zeros_like(x)
            for k in range(LANE_BITS):
                d = d + ((x >> k) & 1)
            dmat[pl.ds(pl.multiple_of(r * SUB, SUB), SUB), :] = d
            return 0
        lax.fori_loop(0, LANE // SUB, tile_d, 0)
        one = (dmat[...] == 1).astype(F32).astype(BF16)
        zero = jnp.zeros((LANE, LANE), BF16)
        adj[0:LANE, 0:LANE] = one
        adj[0:LANE, LANE:] = zero
        adj[LANE:, 0:LANE] = zero
        adj[LANE:, LANE:] = one
        for s in range(num_sets):
            for l in range(num_layers):
                k = s * num_layers + l
                sin_h, cos_h = sincos(jnp.full((SUB, LANE), 0.5 * beta_ref[s, l], F32))
                ct[k, 0] = cos_h
                ct[k, 1] = sin_h
                ct[k, 2] = -sin_h

        def weights(k, slot):
            c, t = ct[k, 0], ct[k, 1]
            cp, tp = [jnp.ones_like(c)], [jnp.ones_like(c)]
            for _ in range(LANE_BITS):
                cp.append(cp[-1] * c)
                tp.append(tp[-1] * t)
            amp = [cp[LANE_BITS - d] * tp[d] for d in range(LANE_BITS + 1)]
            z = jnp.zeros_like(c)
            real = [z, z, z, z, z, z, z, z]
            imag = [z, z, z, z, z, z, z, z]
            for d in range(LANE_BITS + 1):
                if d % 4 == 0:
                    real[d] = amp[d]
                elif d % 4 == 1:
                    imag[d] = -amp[d]
                elif d % 4 == 2:
                    real[d] = -amp[d]
                else:
                    imag[d] = amp[d]

            def body(r, _):
                at = pl.multiple_of(r * 2 * SUB, 2 * SUB)
                rows_re, rows_im = [], []
                for h in range(2):
                    d = dmat[pl.ds(at + h * SUB, SUB), :]
                    re = z
                    im = z
                    for j in range(LANE_BITS + 1):
                        hit = d == j
                        if j % 2 == 0:
                            re = jnp.where(hit, real[j], re)
                        else:
                            im = jnp.where(hit, imag[j], im)
                    rows_re.append(re)
                    rows_im.append(im)
                re = jnp.concatenate(rows_re, axis=0)
                im = jnp.concatenate(rows_im, axis=0)
                for p, (a, b) in enumerate(zip(split3(re), split3(im))):
                    top = pl.ds(at, 2 * SUB)
                    bot = pl.ds(at + LANE, 2 * SUB)
                    wmat[slot, 0, p, top, 0:LANE] = a
                    wmat[slot, 0, p, top, LANE:] = b
                    wmat[slot, 0, p, bot, 0:LANE] = -b
                    wmat[slot, 0, p, bot, LANE:] = a
                    wmat[slot, 1, p, top, 0:LANE] = a
                    wmat[slot, 1, p, top, LANE:] = -b
                    wmat[slot, 1, p, bot, 0:LANE] = b
                    wmat[slot, 1, p, bot, LANE:] = a
                return 0
            lax.fori_loop(0, LANE // (2 * SUB), body, 0)

        def tile_rows(tile):
            return pl.ds(pl.multiple_of(tile * SUB, SUB), SUB)

        def load(ref, slot, tile):
            r = tile_rows(tile)
            return ref[slot, r, 0:LANE], ref[slot, r, LANE:]

        def store(ref, slot, tile, pair):
            r = tile_rows(tile)
            ref[slot, r, 0:LANE] = pair[0]
            ref[slot, r, LANE:] = pair[1]

        def mix_low(source, target, k, sign):
            c, t = ct[k, 0], ct[k, sign]

            def body(i, _):
                base, tile = (i // tiles) * lo, i % tiles
                v = [load(source, base + j, tile) for j in range(lo)]
                for b in lo_bits:
                    v = rot(v, b, c, t)
                for j in range(lo):
                    store(target, base + j, tile, v[j])
                return 0
            lax.fori_loop(0, hi * tiles, body, 0)

        def mid_pass(source, target, k_in, s_in, k_out, s_out, middle):
            if k_in is not None:
                c0, t0 = ct[k_in, 0], ct[k_in, s_in]
            if k_out is not None:
                c1, t1 = ct[k_out, 0], ct[k_out, s_out]

            def body(i, carry):
                base, tile = i // tiles, i % tiles
                slots = [base + j * lo for j in range(hi)]
                if source is None:
                    v = [None] * hi
                else:
                    v = [load(source, m, tile) for m in slots]
                if k_in is not None:
                    for b in hi_bits:
                        v = rot(v, b, c0, t0)
                v, carry = middle(v, slots, tile, carry)
                if k_out is not None:
                    for b in hi_bits:
                        v = rot(v, b, c1, t1)
                    for j in range(hi):
                        store(target, slots[j], tile, v[j])
                return carry
            return lax.fori_loop(0, lo * tiles, body, jnp.zeros((SUB, LANE), F32))

        def pre_mix_send(source, e, s, k, sign):
            c, t = ct[k, 0], ct[k, sign]
            half = n // 2

            def rows_body(i, _):
                base = i * lo
                v = [load(source, base + j // tiles, j % tiles) for j in range(lo * tiles)]
                for b in lo_bits:
                    v = rot(v, b * tiles, c, t)
                for b in tile_bits:
                    v = rot(v, b, c, t)
                for j in range(lo * tiles):
                    re, im = v[j]
                    for b in range(3):
                        fr, fi = sub_flip(re, b), sub_flip(im, b)
                        re, im = c * re + t * fi, c * im - t * fr
                    m = j // tiles
                    store(tmp, (m % 2) * half + i * (lo // 2) + m // 2, j % tiles, (re, im))
                return 0
            lax.fori_loop(0, hi, rows_body, 0)

            def lanes(core):
                at = pl.ds(pl.multiple_of(core * half, half), half)
                m = half * rows
                x = tmp[at].reshape(m, 2 * LANE)
                xh, xm, xl = split3(x)
                w = [wmat[k, sign - 1, p] for p in range(3)]
                a = mm(jnp.concatenate([xh, xm, xl], axis=0), w[0])
                b = mm(jnp.concatenate([xh, xm], axis=0), w[1])
                y = a[:m] + (b[:m] + a[m:2 * m]) + (mm(xh, w[2]) + b[m:] + a[2 * m:])
                src[e, s, at] = y.reshape(half, rows, 2 * LANE)

            def send_slot(ty, tx, part):
                r = pl.ds(part * SUB, SUB)
                send(src.at[e, s, by_core(ty, tx), r], dst.at[e, s, me, r], (e, s), ty, tx)
            other_core = lax.rem(me_core + 1, 2)
            lanes(other_core)
            lanes(me_core)
            peers_in_order(send_slot, ORDER_OTHER, other_core)
            peers_in_order(send_slot, ORDER_LIKE, me_core)
            dst[e, s, me] = src[e, s, by_core(qy, qx)]

        def im_dot(a, b):
            return a[0] * b[1] - a[1] * b[0]

        def slot_dot(bra, ket):
            def group(slots, tile, bits, a):
                x = [load(bra, m, tile) for m in slots]
                y = [load(ket, m, tile) for m in slots]
                for j in range(len(slots)):
                    re = sum(y[j ^ b][0] for b in bits[1:]) + y[j ^ bits[0]][0] if len(bits) > 1 else y[j ^ bits[0]][0]
                    im = sum(y[j ^ b][1] for b in bits[1:]) + y[j ^ bits[0]][1] if len(bits) > 1 else y[j ^ bits[0]][1]
                    a = a + im_dot(x[j], (re, im))
                return a

            def low(i, a):
                return group([(i // tiles) * lo + j for j in range(lo)], i % tiles, lo_bits, a)

            def high(i, a):
                return group([i // tiles + j * lo for j in range(hi)], i % tiles, hi_bits, a)
            a = lax.fori_loop(0, hi * tiles, low, jnp.zeros((SUB, LANE), F32))
            return lax.fori_loop(0, lo * tiles, high, a)

        def fold(x):
            while x.shape[0] > SUB:
                half = x.shape[0] // 2
                x = x[:half] + x[half:]
            return x

        def inner_x(x):
            xh, xm, xl = split3(x)
            y = mm(xh, adj[...]) + mm(xm, adj[...]) + mm(xl, adj[...])
            return y

        def tile_flips(v):
            out = []
            for j in range(len(v)):
                parts_ = []
                for comp in range(2):
                    x = v[j][comp]
                    f = sub_flip(x, 0) + sub_flip(x, 1) + sub_flip(x, 2)
                    for b in tile_bits:
                        f = f + v[j ^ b][comp]
                    parts_.append(f)
                out.append(tuple(parts_))
            return out

        def inner_apply(ket, target):
            def body(i, _):
                at = pl.ds(pl.multiple_of(i * lo, lo), lo)
                y = inner_x(ket[at].reshape(lo * rows, 2 * LANE))
                target[at] = y.reshape(lo, rows, 2 * LANE)
                return 0
            lax.fori_loop(0, hi, body, 0)

            def add(i, _):
                v = [load(ket, i, j) for j in range(tiles)]
                f = tile_flips(v)
                for j in range(tiles):
                    y = load(target, i, j)
                    store(target, i, j, (y[0] + f[j][0], y[1] + f[j][1]))
                return 0
            lax.fori_loop(0, n, add, 0)

        def inner_dots(bra, ket, cost):
            inner_apply(ket, tmp)

            def body(i, carry):
                a, g = carry
                for j in range(tiles):
                    x = load(bra, i, j)
                    a = a + im_dot(x, load(tmp, i, j))
                    g = g + cost[i, tile_rows(j), :] * im_dot(x, load(ket, i, j))
                return a, g
            z = jnp.zeros((SUB, LANE), F32)
            return lax.fori_loop(0, n, body, (z, z))

        def two_dots(bra, ket_b, ket_c):
            def body(i, carry):
                a, g = carry
                for j in range(tiles):
                    x = load(bra, i, j)
                    a = a + im_dot(x, load(ket_b, i, j))
                    g = g + im_dot(x, load(ket_c, i, j))
                return a, g
            z = jnp.zeros((SUB, LANE), F32)
            return lax.fori_loop(0, n, body, (z, z), unroll=4)

        def slot_x(source, target):
            def low(i, _):
                base, tile = (i // tiles) * lo, i % tiles
                y = [load(source, base + j, tile) for j in range(lo)]
                for j in range(lo):
                    o = load(target, base + j, tile)
                    store(target, base + j, tile, tuple(o[c] + (y[j ^ 1][c] + y[j ^ 2][c] + y[j ^ 4][c]) for c in range(2)))
                return 0
            lax.fori_loop(0, hi * tiles, low, 0)

            def high(i, _):
                base, tile = i // tiles, i % tiles
                y = [load(source, base + j * lo, tile) for j in range(hi)]
                for j in range(hi):
                    o = load(target, base + j * lo, tile)
                    store(target, base + j * lo, tile, tuple(o[c] + (y[j ^ 1][c] + y[j ^ 2][c]) for c in range(2)))
                return 0
            lax.fori_loop(0, lo * tiles, high, 0)

        def slot_mix_all(ref, k):
            mix_low(ref, ref, k, 1)
            mid_pass(ref, ref, None, 1, k, 1, lambda v, slots, tile, a: (v, a))

        def fill_table(ref, cost, s, l, scale):
            g = gamma_ref[s, l]

            def body(i, _):
                for j in range(tiles):
                    sn, cs = sincos(cost[i, tile_rows(j), :] * g)
                    if scale is None:
                        store(ref, i, j, (cs, sn))
                    else:
                        store(ref, i, j, (cs * scale, sn * -scale))
                return 0
            lax.fori_loop(0, n, body, 0)

        def kk(s, l):
            return s * num_layers + l

        def add_acc(s, q, a, init=False):
            row = s * 8 + q
            acc[row] = a if init else acc[row] + a


        def each_set(f):
            lax.fori_loop(0, num_sets, lambda s, _: (f(s), 0)[1], 0)

        def first_state(s):
            weights(kk(s, 0), kk(s, 0))
            fill_table(keep.at[0, s], cost_ref, s, 0, norm)

        first_state(0)
        pl.semaphore_wait(barrier, n - 1)
        each_peer(lambda ty, tx: send(cost_ref.at[ty * nx + tx], cost_b.at[me], (6, 0), ty, tx))
        cost_b[me] = cost_ref[me]

        def set_weights(i, _):
            k = (i // (num_layers - 1)) * num_layers + 1 + i % (num_layers - 1)
            weights(k, k)
            return 0

        def forward_mid(before, after, table):
            def middle(v, slots, tile, a):
                out = []
                for m, (re, im) in zip(slots, v):
                    store(before, m, tile, (re, im))
                    cs, sn = load(table, m, tile)
                    p = (re * cs + im * sn, im * cs - re * sn)
                    store(after, m, tile, p)
                    out.append(p)
                return out, a
            return middle

        def backward_mid(before, after, table):
            def middle(v, slots, tile, a):
                out = []
                for m, (re, im) in zip(slots, v):
                    store(before, m, tile, (re, im))
                    cs, sn = load(table, m, tile)
                    p = (re * cs - im * sn, im * cs + re * sn)
                    store(after, m, tile, p)
                    out.append(p)
                return out, a
            return middle

        def turn_mid(psi, lam):
            def middle(v, slots, tile, a):
                out = []
                for m, (re, im) in zip(slots, v):
                    store(psi, m, tile, (re, im))
                    w = cost_b[m, tile_rows(tile), :]
                    p = (w * re, w * im)
                    a = a + (p[0] * re + p[1] * im)
                    store(lam, m, tile, p)
                    out.append(p)
                return out, a
            return middle

        def stage(e, s):
            k_out = kk(s, e - (e // 3) * (2 * e - 5))
            s_out = 1 + e // 3
            k_in = kk(s, e - 1 - (e // 4) * (2 * e - 7))
            s_in = 1 + e // 4
            before, after = keep.at[2 * e - 1, s], keep.at[2 * e, s]

            @pl.when(e == 0)
            def _():
                @pl.when(s > 0)
                def _():
                    first_state(s)
                mid_pass(keep.at[0, s], other, None, 1, k_out, s_out, lambda v, slots, tile, a: (v, a))

            @pl.when(e > 0)
            def _():
                wait_bytes(dst.at[e - 1, s], recv_sem.at[e - 1, s])
                mix_low(dst.at[e - 1, s], other, k_in, s_in)

                @pl.when(e < 3)
                def _():
                    mid_pass(other, other, k_in, s_in, k_out, s_out, forward_mid(before, after, tab.at[e - 1, s]))

                @pl.when(e == 3)
                def _():
                    add_acc(s, 0, mid_pass(other, other, k_in, s_in, k_out, s_out, turn_mid(before, after)), True)

                @pl.when(e > 3)
                def _():
                    mid_pass(other, other, k_in, s_in, k_out, s_out, backward_mid(before, after, tab.at[5 - e, s]))

            pre_mix_send(other, e, s, k_out, s_out)

            @pl.when(e * num_sets + s == 1)
            def _():
                lax.fori_loop(0, num_sets * (num_layers - 1), set_weights, 0)
                each_set(lambda i: fill_table(tab.at[1, i], cost_ref, i, 2, None))
                wait_bytes(cost_b, recv_sem.at[6, 0])
                each_set(lambda i: fill_table(tab.at[0, i], cost_b, i, 1, None))

            @pl.when(e == 2)
            def _():
                inner_apply(keep.at[0, s], psi_b.at[s])
                slot_x(keep.at[0, s], psi_b.at[s])
                slot_mix_all(psi_b.at[s], kk(s, 0))

                def times_cost(i, _):
                    for j in range(tiles):
                        re, im = load(keep.at[0, s], i, j)
                        w = cost_ref[i, tile_rows(j), :]
                        store(psi_c.at[s], i, j, (w * re, w * im))
                    return 0
                lax.fori_loop(0, n, times_cost, 0)
                slot_mix_all(psi_c.at[s], kk(s, 0))

            @pl.when(e == 3)
            def _():
                add_acc(s, 6, slot_dot(after, before), True)

            @pl.when(e > 3)
            def _():
                ket = keep.at[12 - 2 * e, s]
                ket_before = keep.at[11 - 2 * e, s]

                def add_dots(cost):
                    b, g = inner_dots(before, ket, cost)
                    acc[s * 8 + 10 - e] = acc[s * 8 + 10 - e] + (b + slot_dot(before, ket))
                    acc[s * 8 + 7 - e] = 2.0 * g
                    acc[s * 8 + 9 - e] = slot_dot(after, ket_before)
                pl.when(e == 4)(lambda: add_dots(cost_ref))
                pl.when(e == 5)(lambda: add_dots(cost_b))

        def each_exchange(e, _):
            each_set(lambda s: stage(e, s))
            return 0
        lax.fori_loop(0, 2 * num_layers, each_exchange, 0)

        lane = lax.broadcasted_iota(jnp.int32, (1, LANE), 1)

        def place(q, a):
            total = jnp.sum(jnp.sum(a, axis=0, keepdims=True), axis=1, keepdims=True)
            return jnp.where(lane == q, total, 0.0)

        def partial(s):
            wait_bytes(dst.at[5, s], recv_sem.at[5, s])
            b, g = two_dots(dst.at[5, s], psi_b.at[s], psi_c.at[s])
            return place(4, acc[s * 8 + 4] + b) + place(1, 2.0 * g)

        rest = []
        for s in range(num_sets):
            rest.append(sum(place(q, acc[s * 8 + q]) for q in (2, 3, 5, 6)) + place(0, acc[s * 8]))
        for s in range(num_sets):
            mine[s:s + 1, :] = rest[s] + partial(s)

        parts[me] = mine[...]
        each_peer_far_first(lambda ty, tx: send(mine, parts.at[me], (6, 1), ty, tx))
        wait_bytes(parts, recv_sem.at[6, 1])
        out_ref[...] = jnp.sum(parts[...], axis=0)
        for e in range(6):
            for s in range(num_sets):
                wait_bytes(src.at[e, s], send_sem.at[e, s])
        wait_bytes(cost_b, send_sem.at[6, 0])
        wait_bytes(parts, send_sem.at[6, 1])

    return kernel


def solution(mesh):
    ny, nx = mesh.shape['qy'], mesh.shape['qx']
    n = ny * nx

    def device_fn(cost, gamma, beta):
        size = cost.shape[0]
        num_sets, num_layers = gamma.shape
        rows = size // (LANE * n)
        bits = (size * n).bit_length() - 1
        norm = 2.0 ** (-0.5 * bits)
        state = (n, rows, 2 * LANE)
        smem = pl.BlockSpec(memory_space=pltpu.SMEM)
        parts = pl.pallas_call(
            make_kernel(ny, nx, num_sets, num_layers, rows, norm),
            out_shape=jax.ShapeDtypeStruct((num_sets, LANE), F32),
            in_specs=[pl.BlockSpec(memory_space=pltpu.VMEM), smem, smem],
            out_specs=pl.BlockSpec(memory_space=pltpu.VMEM),
            scratch_shapes=[
                pltpu.VMEM((n, rows, LANE), F32),
                pltpu.VMEM((6, num_sets) + state, F32),
                pltpu.VMEM((6, num_sets) + state, F32),
                pltpu.VMEM((11, num_sets) + state, F32),
                pltpu.VMEM((2, num_sets) + state, F32),
                pltpu.VMEM((num_sets,) + state, F32),
                pltpu.VMEM((num_sets,) + state, F32),
                pltpu.VMEM((num_sets * num_layers, 2, 3, 2 * LANE, 2 * LANE), BF16),
                pltpu.VMEM((2 * LANE, 2 * LANE), BF16),
                pltpu.VMEM((LANE, LANE), jnp.int32),
                pltpu.VMEM((num_sets * num_layers, 3, SUB, LANE), F32),
                pltpu.VMEM((num_sets * 8, SUB, LANE), F32),
                pltpu.VMEM((num_sets, LANE), F32),
                pltpu.VMEM((n, num_sets, LANE), F32),
                pltpu.VMEM(state, F32),
                pltpu.VMEM(state, F32),
                pltpu.SemaphoreType.DMA((7, 2)),
                pltpu.SemaphoreType.DMA((7, 2)),
            ],
            compiler_params=pltpu.CompilerParams(collective_id=0, has_side_effects=True, vmem_limit_bytes=60 * 2 ** 20),
            name='qaoa',
        )(cost.reshape(n, rows, LANE), gamma, beta)

        def finish(parts_ref, e_ref, g_ref):
            total = parts_ref[...]
            g_ref[...] = total[:, 1:1 + 2 * num_layers]
            for s in range(num_sets):
                e_ref[s] = total[s, 0]

        return pl.pallas_call(
            finish,
            out_shape=(jax.ShapeDtypeStruct((num_sets,), F32), jax.ShapeDtypeStruct((num_sets, 2 * num_layers), F32)),
            in_specs=[pl.BlockSpec(memory_space=pltpu.VMEM)],
            out_specs=(smem, pl.BlockSpec(memory_space=pltpu.VMEM)),
            name='finish',
        )(parts)

    cost_spec = P(('inst', 'qy', 'qx'))
    angle_spec = P('inst', None)
    return jax.shard_map(device_fn, mesh=mesh, in_specs=(cost_spec, angle_spec, angle_spec), out_specs=(P('inst'), angle_spec), check_vma=False)
```

```python
import functools
import jax
import jax.numpy as jnp
from jax import lax
from jax.experimental import pallas as pl
from jax.experimental.pallas import tpu as pltpu
from jax.sharding import PartitionSpec as P

LANE = 128
LANE_BITS = 7
SUB = 8
ORDER_OTHER = [(1, 1), (1, 3), (1, 2), (1, 0), (2, 1), (2, 3), (2, 2), (2, 0), (3, 1), (3, 3), (3, 2), (3, 0), (0, 1), (0, 3), (0, 2), (0, 0)]
ORDER_LIKE = [(1, 1), (1, 3), (1, 2), (1, 0), (2, 1), (2, 3), (2, 2), (2, 0), (3, 1), (3, 3), (3, 2), (3, 0), (0, 1), (0, 3), (0, 2)]
MESH_ID = pl.DeviceIdType.MESH
F32 = jnp.float32
BF16 = jnp.bfloat16


def sincos(x):
    k = jnp.floor(x * 0.6366197723675814 + 0.5)
    r = ((x - k * 1.5703125) - k * 4.837512969970703125e-4) - k * 7.54978995489188216e-8
    z = r * r
    s = r + r * z * (-1.6666654611e-1 + z * (8.3321608736e-3 + z * -1.9515295891e-4))
    c = (1.0 - 0.5 * z) + z * z * (4.166664568298827e-2 + z * (-1.388731625493765e-3 + z * 2.443315711809948e-5))
    q = k.astype(jnp.int32)
    odd = (q & 1) != 0
    sin_v = jnp.where(odd, c, s)
    cos_v = jnp.where(odd, s, c)
    sin_v = jnp.where((q & 2) != 0, -sin_v, sin_v)
    cos_v = jnp.where(((q + 1) & 2) != 0, -cos_v, cos_v)
    return sin_v, cos_v


def split3(x):
    hi = x.astype(BF16)
    rest = x - hi.astype(F32)
    mid = rest.astype(BF16)
    low = (rest - mid.astype(F32)).astype(BF16)
    return hi, mid, low


def mm(a, b):
    return jnp.dot(a, b, preferred_element_type=F32)


def rot(pairs, stride, c, t):
    out = list(pairs)
    for j in range(len(pairs)):
        if j & stride:
            continue
        (ar, ai), (br, bi) = pairs[j], pairs[j | stride]
        out[j] = (c * ar + t * bi, c * ai - t * br)
        out[j | stride] = (c * br + t * ai, c * bi - t * ar)
    return out


def sub_flip(x, bit):
    if bit == 2:
        return pltpu.roll(x, 4, 0)
    row = lax.broadcasted_iota(jnp.int32, (SUB, LANE), 0)
    up = pltpu.roll(x, 1 << bit, 0)
    down = pltpu.roll(x, SUB - (1 << bit), 0)
    return jnp.where((row & (1 << bit)) != 0, up, down)


def make_kernel(ny, nx, num_sets, num_layers, rows, norm):
    n = ny * nx
    lo = 8
    hi = n // lo
    tiles = rows // SUB
    lo_bits = [1 << b for b in range(lo.bit_length() - 1)]
    hi_bits = [1 << b for b in range(hi.bit_length() - 1)]
    tile_bits = [1 << b for b in range(tiles.bit_length() - 1)]
    width_x = nx // 2

    def kernel(cost_ref, gamma_ref, beta_ref, out_ref,
               cost_b, src, dst, keep, tab, psi_b, psi_c, wmat, adj, dmat, ct, acc, mine, parts, tmp, other, send_sem, recv_sem, row_sem):
        qy = lax.axis_index('qy')
        qx = lax.axis_index('qx')
        me = qy * nx + qx
        barrier = pltpu.get_barrier_semaphore()

        me_core = lax.rem(qx, 2)

        def ring_x(order):
            return [lax.rem(qx // 2 + dx, width_x) * 2 for dx in order]
        chip_x = ring_x((1, 3, 2, 0))
        far_x = ring_x((2, 1, 3, 0))

        def peers_of_core(act, core, last):
            def body(i, _):
                ty = lax.rem(qy + 1 + i, ny)
                for tx in chip_x[:-1]:
                    act(ty, tx + core)

                @pl.when(i + last < ny)
                def _():
                    act(ty, chip_x[-1] + core)
                return 0
            lax.fori_loop(0, ny, body, 0)

        def peers_in_order(act, order, core):
            for part in range(tiles):
                for dy, dx in order:
                    act(lax.rem(qy + dy, ny), lax.rem(qx // 2 + dx, width_x) * 2 + core, part)

        def both_cores(f):
            lax.fori_loop(0, 2, lambda h, _: (f(lax.rem(me_core + 1 + h, 2), h), 0)[1], 0)

        def each_peer(act):
            both_cores(lambda core, last: peers_of_core(act, core, last))

        def each_peer_far_first(act):
            def body(i, _):
                a = i // 2
                ty = lax.rem(qy + 2 - a + (a // 2) * (7 - 2 * a), ny)
                core = lax.rem(qx + 1 + i, 2)
                for tx in far_x[:-1]:
                    act(ty, tx + core)

                @pl.when(i < 2 * ny - 1)
                def _():
                    act(ty, far_x[-1] + core)
                return 0
            lax.fori_loop(0, 2 * ny, body, 0)

        def greet(ty, tx):
            pl.semaphore_signal(barrier, inc=1, device_id={'qy': ty, 'qx': tx}, device_id_type=MESH_ID)
        def line_peers(act):
            def row(i, _):
                act(qy, lax.rem(qx + i, nx))
                return 0
            lax.fori_loop(1, nx, row, 0)

            def column(i, _):
                act(lax.rem(qy + i, ny), qx)
                act(lax.rem(qy + i, ny), qx + 1 - 2 * me_core)
                return 0
            lax.fori_loop(1, ny, column, 0)

        def cross_peers(act):
            def body(i, _):
                ty = lax.rem(qy + 1 + i // 2, ny)
                core = lax.rem(qx + 1 + i, 2)
                for dx in (1, 3, 2):
                    act(ty, lax.rem(qx // 2 + dx, width_x) * 2 + core)
                return 0
            lax.fori_loop(0, 2 * (ny - 1), body, 0)

        line_peers(greet)

        def send(source, target, ids, ty, tx):
            pltpu.make_async_remote_copy(
                source, target, send_sem.at[ids], recv_sem.at[ids],
                device_id={'qy': ty, 'qx': tx}, device_id_type=MESH_ID).start()

        def by_core(ty, tx):
            return lax.rem(tx, 2) * (n // 2) + ty * width_x + tx // 2

        def wait_bytes(buf, sem):
            part = buf.at[pl.ds(0, n - 1)]
            pltpu.make_async_copy(part, part, sem).wait()

        def tile_d(r, _):
            a = lax.broadcasted_iota(jnp.int32, (SUB, LANE), 0) + r * SUB
            b = lax.broadcasted_iota(jnp.int32, (SUB, LANE), 1)
            x = a ^ b
            d = jnp.zeros_like(x)
            for k in range(LANE_BITS):
                d = d + ((x >> k) & 1)
            dmat[pl.ds(pl.multiple_of(r * SUB, SUB), SUB), :] = d
            return 0
        lax.fori_loop(0, LANE // SUB, tile_d, 0)
        one = (dmat[...] == 1).astype(F32).astype(BF16)
        zero = jnp.zeros((LANE, LANE), BF16)
        adj[0:LANE, 0:LANE] = one
        adj[0:LANE, LANE:] = zero
        adj[LANE:, 0:LANE] = zero
        adj[LANE:, LANE:] = one
        for s in range(num_sets):
            for l in range(num_layers):
                k = s * num_layers + l
                sin_h, cos_h = sincos(jnp.full((SUB, LANE), 0.5 * beta_ref[s, l], F32))
                ct[k, 0] = cos_h
                ct[k, 1] = sin_h
                ct[k, 2] = -sin_h

        def weights(k, slot):
            c, t = ct[k, 0], ct[k, 1]
            cp, tp = [jnp.ones_like(c)], [jnp.ones_like(c)]
            for _ in range(LANE_BITS):
                cp.append(cp[-1] * c)
                tp.append(tp[-1] * t)
            amp = [cp[LANE_BITS - d] * tp[d] for d in range(LANE_BITS + 1)]
            z = jnp.zeros_like(c)
            real = [z, z, z, z, z, z, z, z]
            imag = [z, z, z, z, z, z, z, z]
            for d in range(LANE_BITS + 1):
                if d % 4 == 0:
                    real[d] = amp[d]
                elif d % 4 == 1:
                    imag[d] = -amp[d]
                elif d % 4 == 2:
                    real[d] = -amp[d]
                else:
                    imag[d] = amp[d]

            def body(r, _):
                at = pl.multiple_of(r * 2 * SUB, 2 * SUB)
                rows_re, rows_im = [], []
                for h in range(2):
                    d = dmat[pl.ds(at + h * SUB, SUB), :]
                    re = z
                    im = z
                    for j in range(LANE_BITS + 1):
                        hit = d == j
                        if j % 2 == 0:
                            re = jnp.where(hit, real[j], re)
                        else:
                            im = jnp.where(hit, imag[j], im)
                    rows_re.append(re)
                    rows_im.append(im)
                re = jnp.concatenate(rows_re, axis=0)
                im = jnp.concatenate(rows_im, axis=0)
                for p, (a, b) in enumerate(zip(split3(re), split3(im))):
                    top = pl.ds(at, 2 * SUB)
                    bot = pl.ds(at + LANE, 2 * SUB)
                    wmat[slot, 0, p, top, 0:LANE] = a
                    wmat[slot, 0, p, top, LANE:] = b
                    wmat[slot, 0, p, bot, 0:LANE] = -b
                    wmat[slot, 0, p, bot, LANE:] = a
                    wmat[slot, 1, p, top, 0:LANE] = a
                    wmat[slot, 1, p, top, LANE:] = -b
                    wmat[slot, 1, p, bot, 0:LANE] = b
                    wmat[slot, 1, p, bot, LANE:] = a
                return 0
            lax.fori_loop(0, LANE // (2 * SUB), body, 0)

        def tile_rows(tile):
            return pl.ds(pl.multiple_of(tile * SUB, SUB), SUB)

        def load(ref, slot, tile):
            r = tile_rows(tile)
            return ref[slot, r, 0:LANE], ref[slot, r, LANE:]

        def store(ref, slot, tile, pair):
            r = tile_rows(tile)
            ref[slot, r, 0:LANE] = pair[0]
            ref[slot, r, LANE:] = pair[1]

        def mix_low(source, target, k, sign):
            c, t = ct[k, 0], ct[k, sign]

            def body(i, _):
                base, tile = (i // tiles) * lo, i % tiles
                v = [load(source, base + j, tile) for j in range(lo)]
                for b in lo_bits:
                    v = rot(v, b, c, t)
                for j in range(lo):
                    store(target, base + j, tile, v[j])
                return 0
            lax.fori_loop(0, hi * tiles, body, 0, unroll=2)

        def mid_pass(source, target, k_in, s_in, k_out, s_out, middle):
            if k_in is not None:
                c0, t0 = ct[k_in, 0], ct[k_in, s_in]
            if k_out is not None:
                c1, t1 = ct[k_out, 0], ct[k_out, s_out]

            def body(i, carry):
                base, tile = i // tiles, i % tiles
                slots = [base + j * lo for j in range(hi)]
                if source is None:
                    v = [None] * hi
                else:
                    v = [load(source, m, tile) for m in slots]
                if k_in is not None:
                    for b in hi_bits:
                        v = rot(v, b, c0, t0)
                v, carry = middle(v, slots, tile, carry)
                if k_out is not None:
                    for b in hi_bits:
                        v = rot(v, b, c1, t1)
                    for j in range(hi):
                        store(target, slots[j], tile, v[j])
                return carry
            return lax.fori_loop(0, lo * tiles, body, jnp.zeros((SUB, LANE), F32), unroll=2)

        def pre_mix_send(source, e, s, k, sign):
            c, t = ct[k, 0], ct[k, sign]
            half = n // 2

            def rows_body(i, _):
                base = i * lo
                v = [load(source, base + j // tiles, j % tiles) for j in range(lo * tiles)]
                for b in lo_bits:
                    v = rot(v, b * tiles, c, t)
                for b in tile_bits:
                    v = rot(v, b, c, t)
                for j in range(lo * tiles):
                    re, im = v[j]
                    for b in range(3):
                        fr, fi = sub_flip(re, b), sub_flip(im, b)
                        re, im = c * re + t * fi, c * im - t * fr
                    m = j // tiles
                    store(tmp, (m % 2) * half + i * (lo // 2) + m // 2, j % tiles, (re, im))
                return 0
            lax.fori_loop(0, hi, rows_body, 0)

            def lanes(core):
                at = pl.ds(pl.multiple_of(core * half, half), half)
                m = half * rows
                x = tmp[at].reshape(m, 2 * LANE)
                xh, xm, xl = split3(x)
                w = [wmat[k, sign - 1, p] for p in range(3)]
                a = mm(jnp.concatenate([xh, xm, xl], axis=0), w[0])
                b = mm(jnp.concatenate([xh, xm], axis=0), w[1])
                y = a[:m] + (b[:m] + a[m:2 * m]) + (mm(xh, w[2]) + b[m:] + a[2 * m:])
                src[e, s, at] = y.reshape(half, rows, 2 * LANE)

            def send_slot(ty, tx, part):
                r = pl.ds(part * SUB, SUB)
                send(src.at[e, s, by_core(ty, tx), r], dst.at[e, s, me, r], (e, s), ty, tx)
            other_core = lax.rem(me_core + 1, 2)
            lanes(other_core)
            lanes(me_core)
            def near(order, want):
                return [o for o in order if (o[0] == 0 or o[1] == 0) == want]
            peers_in_order(send_slot, near(ORDER_OTHER, True), other_core)
            peers_in_order(send_slot, near(ORDER_LIKE, True), me_core)

            @pl.when(e + s == 0)
            def _():
                hear_rows()
            peers_in_order(send_slot, near(ORDER_OTHER, False), other_core)
            peers_in_order(send_slot, near(ORDER_LIKE, False), me_core)
            dst[e, s, me] = src[e, s, by_core(qy, qx)]

        def im_dot(a, b):
            return a[0] * b[1] - a[1] * b[0]

        def slot_dot(bra, ket):
            def group(slots, tile, bits, a):
                x = [load(bra, m, tile) for m in slots]
                y = [load(ket, m, tile) for m in slots]
                for j in range(len(slots)):
                    re = sum(y[j ^ b][0] for b in bits[1:]) + y[j ^ bits[0]][0] if len(bits) > 1 else y[j ^ bits[0]][0]
                    im = sum(y[j ^ b][1] for b in bits[1:]) + y[j ^ bits[0]][1] if len(bits) > 1 else y[j ^ bits[0]][1]
                    a = a + im_dot(x[j], (re, im))
                return a

            def low(i, a):
                return group([(i // tiles) * lo + j for j in range(lo)], i % tiles, lo_bits, a)

            def high(i, a):
                return group([i // tiles + j * lo for j in range(hi)], i % tiles, hi_bits, a)
            a = lax.fori_loop(0, hi * tiles, low, jnp.zeros((SUB, LANE), F32))
            return lax.fori_loop(0, lo * tiles, high, a)

        def fold(x):
            while x.shape[0] > SUB:
                half = x.shape[0] // 2
                x = x[:half] + x[half:]
            return x

        def inner_x(x):
            xh, xm, xl = split3(x)
            y = mm(xh, adj[...]) + mm(xm, adj[...]) + mm(xl, adj[...])
            return y

        def tile_flips(v):
            out = []
            for j in range(len(v)):
                parts_ = []
                for comp in range(2):
                    x = v[j][comp]
                    f = sub_flip(x, 0) + sub_flip(x, 1) + sub_flip(x, 2)
                    for b in tile_bits:
                        f = f + v[j ^ b][comp]
                    parts_.append(f)
                out.append(tuple(parts_))
            return out

        def inner_apply(ket, target):
            def body(i, _):
                at = pl.ds(pl.multiple_of(i * lo, lo), lo)
                y = inner_x(ket[at].reshape(lo * rows, 2 * LANE))
                target[at] = y.reshape(lo, rows, 2 * LANE)
                return 0
            lax.fori_loop(0, hi, body, 0)

            def add(i, _):
                v = [load(ket, i, j) for j in range(tiles)]
                f = tile_flips(v)
                for j in range(tiles):
                    y = load(target, i, j)
                    store(target, i, j, (y[0] + f[j][0], y[1] + f[j][1]))
                return 0
            lax.fori_loop(0, n, add, 0)

        def inner_dots(bra, ket, cost):
            inner_apply(ket, tmp)

            def body(i, carry):
                a, g = carry
                for j in range(tiles):
                    x = load(bra, i, j)
                    a = a + im_dot(x, load(tmp, i, j))
                    g = g + cost[i, tile_rows(j), :] * im_dot(x, load(ket, i, j))
                return a, g
            z = jnp.zeros((SUB, LANE), F32)
            return lax.fori_loop(0, n, body, (z, z))

        def two_dots(bra, ket_b, ket_c):
            def body(i, carry):
                a, g = carry
                for j in range(tiles):
                    x = load(bra, i, j)
                    a = a + im_dot(x, load(ket_b, i, j))
                    g = g + im_dot(x, load(ket_c, i, j))
                return a, g
            z = jnp.zeros((SUB, LANE), F32)
            return lax.fori_loop(0, n, body, (z, z), unroll=4)

        def slot_x(source, target):
            def low(i, _):
                base, tile = (i // tiles) * lo, i % tiles
                y = [load(source, base + j, tile) for j in range(lo)]
                for j in range(lo):
                    o = load(target, base + j, tile)
                    store(target, base + j, tile, tuple(o[c] + (y[j ^ 1][c] + y[j ^ 2][c] + y[j ^ 4][c]) for c in range(2)))
                return 0
            lax.fori_loop(0, hi * tiles, low, 0)

            def high(i, _):
                base, tile = i // tiles, i % tiles
                y = [load(source, base + j * lo, tile) for j in range(hi)]
                for j in range(hi):
                    o = load(target, base + j * lo, tile)
                    store(target, base + j * lo, tile, tuple(o[c] + (y[j ^ 1][c] + y[j ^ 2][c]) for c in range(2)))
                return 0
            lax.fori_loop(0, lo * tiles, high, 0)

        def slot_mix_all(ref, k):
            mix_low(ref, ref, k, 1)
            mid_pass(ref, ref, None, 1, k, 1, lambda v, slots, tile, a: (v, a))

        def fill_table(ref, cost, s, l, scale):
            g = gamma_ref[s, l]

            def body(i, _):
                for j in range(tiles):
                    sn, cs = sincos(cost[i, tile_rows(j), :] * g)
                    if scale is None:
                        store(ref, i, j, (cs, sn))
                    else:
                        store(ref, i, j, (cs * scale, sn * -scale))
                return 0
            lax.fori_loop(0, n, body, 0)

        def kk(s, l):
            return s * num_layers + l

        def add_acc(s, q, a, init=False):
            row = s * 8 + q
            acc[row] = a if init else acc[row] + a


        def each_set(f):
            lax.fori_loop(0, num_sets, lambda s, _: (f(s), 0)[1], 0)

        def first_state(s):
            weights(kk(s, 0), kk(s, 0))
            fill_table(keep.at[0, s], cost_ref, s, 0, norm)

        first_state(0)
        pl.semaphore_wait(barrier, nx - 1 + 2 * (ny - 1))

        def tell(i, _):
            pl.semaphore_signal(row_sem, inc=1, device_id={'qy': lax.rem(qy + i, ny), 'qx': qx}, device_id_type=MESH_ID)
            return 0
        lax.fori_loop(1, ny, tell, 0)

        def send_cost(ty, tx):
            send(cost_ref.at[ty * nx + tx], cost_b.at[me], (6, 0), ty, tx)
        line_peers(send_cost)
        cost_b[me] = cost_ref[me]

        def hear_rows():
            pl.semaphore_wait(row_sem, ny - 1)
            cross_peers(send_cost)


        def set_weights(i, _):
            k = (i // (num_layers - 1)) * num_layers + 1 + i % (num_layers - 1)
            weights(k, k)
            return 0

        def forward_mid(before, after, table):
            def middle(v, slots, tile, a):
                out = []
                for m, (re, im) in zip(slots, v):
                    store(before, m, tile, (re, im))
                    cs, sn = load(table, m, tile)
                    p = (re * cs + im * sn, im * cs - re * sn)
                    store(after, m, tile, p)
                    out.append(p)
                return out, a
            return middle

        def backward_mid(before, after, table):
            def middle(v, slots, tile, a):
                out = []
                for m, (re, im) in zip(slots, v):
                    store(before, m, tile, (re, im))
                    cs, sn = load(table, m, tile)
                    p = (re * cs - im * sn, im * cs + re * sn)
                    store(after, m, tile, p)
                    out.append(p)
                return out, a
            return middle

        def turn_mid(psi, lam):
            def middle(v, slots, tile, a):
                out = []
                for m, (re, im) in zip(slots, v):
                    store(psi, m, tile, (re, im))
                    w = cost_b[m, tile_rows(tile), :]
                    p = (w * re, w * im)
                    a = a + (p[0] * re + p[1] * im)
                    store(lam, m, tile, p)
                    out.append(p)
                return out, a
            return middle

        def stage(e, s):
            k_out = kk(s, e - (e // 3) * (2 * e - 5))
            s_out = 1 + e // 3
            k_in = kk(s, e - 1 - (e // 4) * (2 * e - 7))
            s_in = 1 + e // 4
            before, after = keep.at[2 * e - 1, s], keep.at[2 * e, s]

            @pl.when(e == 0)
            def _():
                @pl.when(s > 0)
                def _():
                    first_state(s)
                mid_pass(keep.at[0, s], other, None, 1, k_out, s_out, lambda v, slots, tile, a: (v, a))

            @pl.when(e > 0)
            def _():
                wait_bytes(dst.at[e - 1, s], recv_sem.at[e - 1, s])
                mix_low(dst.at[e - 1, s], other, k_in, s_in)

                @pl.when(e < 3)
                def _():
                    mid_pass(other, other, k_in, s_in, k_out, s_out, forward_mid(before, after, tab.at[e - 1, s]))

                @pl.when(e == 3)
                def _():
                    add_acc(s, 0, mid_pass(other, other, k_in, s_in, k_out, s_out, turn_mid(before, after)), True)

                @pl.when(e > 3)
                def _():
                    mid_pass(other, other, k_in, s_in, k_out, s_out, backward_mid(before, after, tab.at[5 - e, s]))

            pre_mix_send(other, e, s, k_out, s_out)

            @pl.when(e * num_sets + s == 1)
            def _():
                lax.fori_loop(0, num_sets * (num_layers - 1), set_weights, 0)
                each_set(lambda i: fill_table(tab.at[1, i], cost_ref, i, 2, None))
                wait_bytes(cost_b, recv_sem.at[6, 0])
                each_set(lambda i: fill_table(tab.at[0, i], cost_b, i, 1, None))

            @pl.when(e == 2)
            def _():
                inner_apply(keep.at[0, s], psi_b.at[s])
                slot_x(keep.at[0, s], psi_b.at[s])
                slot_mix_all(psi_b.at[s], kk(s, 0))

                def times_cost(i, _):
                    for j in range(tiles):
                        re, im = load(keep.at[0, s], i, j)
                        w = cost_ref[i, tile_rows(j), :]
                        store(psi_c.at[s], i, j, (w * re, w * im))
                    return 0
                lax.fori_loop(0, n, times_cost, 0)
                slot_mix_all(psi_c.at[s], kk(s, 0))

            @pl.when(e == 3)
            def _():
                add_acc(s, 6, slot_dot(after, before), True)

            @pl.when(e > 3)
            def _():
                ket = keep.at[12 - 2 * e, s]
                ket_before = keep.at[11 - 2 * e, s]

                def add_dots(cost):
                    b, g = inner_dots(before, ket, cost)
                    acc[s * 8 + 10 - e] = acc[s * 8 + 10 - e] + (b + slot_dot(before, ket))
                    acc[s * 8 + 7 - e] = 2.0 * g
                    acc[s * 8 + 9 - e] = slot_dot(after, ket_before)
                pl.when(e == 4)(lambda: add_dots(cost_ref))
                pl.when(e == 5)(lambda: add_dots(cost_b))

        def each_exchange(e, _):
            each_set(lambda s: stage(e, s))
            return 0
        lax.fori_loop(0, 2 * num_layers, each_exchange, 0)

        lane = lax.broadcasted_iota(jnp.int32, (1, LANE), 1)

        def place(q, a):
            total = jnp.sum(jnp.sum(a, axis=0, keepdims=True), axis=1, keepdims=True)
            return jnp.where(lane == q, total, 0.0)

        def partial(s):
            wait_bytes(dst.at[5, s], recv_sem.at[5, s])
            b, g = two_dots(dst.at[5, s], psi_b.at[s], psi_c.at[s])
            return place(4, acc[s * 8 + 4] + b) + place(1, 2.0 * g)

        rest = []
        for s in range(num_sets):
            rest.append(sum(place(q, acc[s * 8 + q]) for q in (2, 3, 5, 6)) + place(0, acc[s * 8]))
        for s in range(num_sets):
            mine[s:s + 1, :] = rest[s] + partial(s)

        parts[me] = mine[...]
        each_peer_far_first(lambda ty, tx: send(mine, parts.at[me], (6, 1), ty, tx))
        wait_bytes(parts, recv_sem.at[6, 1])
        out_ref[...] = jnp.sum(parts[...], axis=0)
        for e in range(6):
            for s in range(num_sets):
                wait_bytes(src.at[e, s], send_sem.at[e, s])
        wait_bytes(cost_b, send_sem.at[6, 0])
        wait_bytes(parts, send_sem.at[6, 1])

    return kernel


def solution(mesh):
    ny, nx = mesh.shape['qy'], mesh.shape['qx']
    n = ny * nx

    def device_fn(cost, gamma, beta):
        size = cost.shape[0]
        num_sets, num_layers = gamma.shape
        rows = size // (LANE * n)
        bits = (size * n).bit_length() - 1
        norm = 2.0 ** (-0.5 * bits)
        state = (n, rows, 2 * LANE)
        smem = pl.BlockSpec(memory_space=pltpu.SMEM)
        parts = pl.pallas_call(
            make_kernel(ny, nx, num_sets, num_layers, rows, norm),
            out_shape=jax.ShapeDtypeStruct((num_sets, LANE), F32),
            in_specs=[pl.BlockSpec(memory_space=pltpu.VMEM), smem, smem],
            out_specs=pl.BlockSpec(memory_space=pltpu.VMEM),
            scratch_shapes=[
                pltpu.VMEM((n, rows, LANE), F32),
                pltpu.VMEM((6, num_sets) + state, F32),
                pltpu.VMEM((6, num_sets) + state, F32),
                pltpu.VMEM((11, num_sets) + state, F32),
                pltpu.VMEM((2, num_sets) + state, F32),
                pltpu.VMEM((num_sets,) + state, F32),
                pltpu.VMEM((num_sets,) + state, F32),
                pltpu.VMEM((num_sets * num_layers, 2, 3, 2 * LANE, 2 * LANE), BF16),
                pltpu.VMEM((2 * LANE, 2 * LANE), BF16),
                pltpu.VMEM((LANE, LANE), jnp.int32),
                pltpu.VMEM((num_sets * num_layers, 3, SUB, LANE), F32),
                pltpu.VMEM((num_sets * 8, SUB, LANE), F32),
                pltpu.VMEM((num_sets, LANE), F32),
                pltpu.VMEM((n, num_sets, LANE), F32),
                pltpu.VMEM(state, F32),
                pltpu.VMEM(state, F32),
                pltpu.SemaphoreType.DMA((7, 2)),
                pltpu.SemaphoreType.DMA((7, 2)),
                pltpu.SemaphoreType.REGULAR,
            ],
            compiler_params=pltpu.CompilerParams(collective_id=0, has_side_effects=True, vmem_limit_bytes=60 * 2 ** 20),
            name='qaoa',
        )(cost.reshape(n, rows, LANE), gamma, beta)

        def finish(parts_ref, e_ref, g_ref):
            total = parts_ref[...]
            g_ref[...] = total[:, 1:1 + 2 * num_layers]
            for s in range(num_sets):
                e_ref[s] = total[s, 0]

        return pl.pallas_call(
            finish,
            out_shape=(jax.ShapeDtypeStruct((num_sets,), F32), jax.ShapeDtypeStruct((num_sets, 2 * num_layers), F32)),
            in_specs=[pl.BlockSpec(memory_space=pltpu.VMEM)],
            out_specs=(smem, pl.BlockSpec(memory_space=pltpu.VMEM)),
            name='finish',
        )(parts)

    cost_spec = P(('inst', 'qy', 'qx'))
    angle_spec = P('inst', None)
    return jax.shard_map(device_fn, mesh=mesh, in_specs=(cost_spec, angle_spec, angle_spec), out_specs=(P('inst'), angle_spec), check_vma=False)
```

```python
import functools
import jax
import jax.numpy as jnp
from jax import lax
from jax.experimental import pallas as pl
from jax.experimental.pallas import tpu as pltpu
from jax.sharding import PartitionSpec as P

LANE = 128
LANE_BITS = 7
SUB = 8
ORDER_OTHER = [(1, 1), (1, 3), (1, 2), (1, 0), (2, 1), (2, 3), (2, 2), (2, 0), (3, 1), (3, 3), (3, 2), (3, 0), (0, 1), (0, 3), (0, 2), (0, 0)]
ORDER_LIKE = [(1, 1), (1, 3), (1, 2), (1, 0), (2, 1), (2, 3), (2, 2), (2, 0), (3, 1), (3, 3), (3, 2), (3, 0), (0, 1), (0, 3), (0, 2)]
MESH_ID = pl.DeviceIdType.MESH
F32 = jnp.float32
BF16 = jnp.bfloat16


def sincos(x):
    k = jnp.floor(x * 0.6366197723675814 + 0.5)
    r = ((x - k * 1.5703125) - k * 4.837512969970703125e-4) - k * 7.54978995489188216e-8
    z = r * r
    s = r + r * z * (-1.6666654611e-1 + z * (8.3321608736e-3 + z * -1.9515295891e-4))
    c = (1.0 - 0.5 * z) + z * z * (4.166664568298827e-2 + z * (-1.388731625493765e-3 + z * 2.443315711809948e-5))
    q = k.astype(jnp.int32)
    odd = (q & 1) != 0
    sin_v = jnp.where(odd, c, s)
    cos_v = jnp.where(odd, s, c)
    sin_v = jnp.where((q & 2) != 0, -sin_v, sin_v)
    cos_v = jnp.where(((q + 1) & 2) != 0, -cos_v, cos_v)
    return sin_v, cos_v


def split3(x):
    hi = x.astype(BF16)
    rest = x - hi.astype(F32)
    mid = rest.astype(BF16)
    low = (rest - mid.astype(F32)).astype(BF16)
    return hi, mid, low


def mm(a, b):
    return jnp.dot(a, b, preferred_element_type=F32)


def rot(pairs, stride, c, t):
    out = list(pairs)
    for j in range(len(pairs)):
        if j & stride:
            continue
        (ar, ai), (br, bi) = pairs[j], pairs[j | stride]
        out[j] = (c * ar + t * bi, c * ai - t * br)
        out[j | stride] = (c * br + t * ai, c * bi - t * ar)
    return out


def sub_flip(x, bit):
    if bit == 2:
        return pltpu.roll(x, 4, 0)
    row = lax.broadcasted_iota(jnp.int32, (SUB, LANE), 0)
    up = pltpu.roll(x, 1 << bit, 0)
    down = pltpu.roll(x, SUB - (1 << bit), 0)
    return jnp.where((row & (1 << bit)) != 0, up, down)


def make_kernel(ny, nx, num_sets, num_layers, rows, norm):
    n = ny * nx
    lo = 8
    hi = n // lo
    tiles = rows // SUB
    lo_bits = [1 << b for b in range(lo.bit_length() - 1)]
    hi_bits = [1 << b for b in range(hi.bit_length() - 1)]
    tile_bits = [1 << b for b in range(tiles.bit_length() - 1)]
    width_x = nx // 2

    def kernel(cost_ref, gamma_ref, beta_ref, out_ref,
               cost_b, src, dst, keep, tab, psi_b, psi_c, wmat, adj, dmat, ct, acc, mine, parts, tmp, other, send_sem, recv_sem, row_sem):
        qy = lax.axis_index('qy')
        qx = lax.axis_index('qx')
        me = qy * nx + qx
        barrier = pltpu.get_barrier_semaphore()

        me_core = lax.rem(qx, 2)

        def ring_x(order):
            return [lax.rem(qx // 2 + dx, width_x) * 2 for dx in order]
        chip_x = ring_x((1, 3, 2, 0))
        far_x = ring_x((2, 1, 3, 0))

        def peers_of_core(act, core, last):
            def body(i, _):
                ty = lax.rem(qy + 1 + i, ny)
                for tx in chip_x[:-1]:
                    act(ty, tx + core)

                @pl.when(i + last < ny)
                def _():
                    act(ty, chip_x[-1] + core)
                return 0
            lax.fori_loop(0, ny, body, 0)

        def peers_in_order(act, order, core):
            for part in range(tiles):
                for dy, dx in order:
                    act(lax.rem(qy + dy, ny), lax.rem(qx // 2 + dx, width_x) * 2 + core, part)

        def both_cores(f):
            lax.fori_loop(0, 2, lambda h, _: (f(lax.rem(me_core + 1 + h, 2), h), 0)[1], 0)

        def each_peer(act):
            both_cores(lambda core, last: peers_of_core(act, core, last))

        def each_peer_far_first(act):
            def body(i, _):
                a = i // 2
                ty = lax.rem(qy + 2 - a + (a // 2) * (7 - 2 * a), ny)
                core = lax.rem(qx + 1 + i, 2)
                for tx in far_x[:-1]:
                    act(ty, tx + core)

                @pl.when(i < 2 * ny - 1)
                def _():
                    act(ty, far_x[-1] + core)
                return 0
            lax.fori_loop(0, 2 * ny, body, 0)

        def greet(ty, tx):
            pl.semaphore_signal(barrier, inc=1, device_id={'qy': ty, 'qx': tx}, device_id_type=MESH_ID)
        def line_peers(act):
            def row(i, _):
                act(qy, lax.rem(qx + i, nx))
                return 0
            lax.fori_loop(1, nx, row, 0)

            def column(i, _):
                act(lax.rem(qy + i, ny), qx)
                act(lax.rem(qy + i, ny), qx + 1 - 2 * me_core)
                return 0
            lax.fori_loop(1, ny, column, 0)

        def cross_peers(act):
            def body(i, _):
                ty = lax.rem(qy + 1 + i // 2, ny)
                core = lax.rem(qx + 1 + i, 2)
                for dx in (1, 3, 2):
                    act(ty, lax.rem(qx // 2 + dx, width_x) * 2 + core)
                return 0
            lax.fori_loop(0, 2 * (ny - 1), body, 0)

        line_peers(greet)

        def send(source, target, ids, ty, tx):
            pltpu.make_async_remote_copy(
                source, target, send_sem.at[ids], recv_sem.at[ids],
                device_id={'qy': ty, 'qx': tx}, device_id_type=MESH_ID).start()

        def by_core(ty, tx):
            return lax.rem(tx, 2) * (n // 2) + ty * width_x + tx // 2

        def wait_bytes(buf, sem):
            part = buf.at[pl.ds(0, n - 1)]
            pltpu.make_async_copy(part, part, sem).wait()

        def tile_d(r, _):
            a = lax.broadcasted_iota(jnp.int32, (SUB, LANE), 0) + r * SUB
            b = lax.broadcasted_iota(jnp.int32, (SUB, LANE), 1)
            x = a ^ b
            d = jnp.zeros_like(x)
            for k in range(LANE_BITS):
                d = d + ((x >> k) & 1)
            dmat[pl.ds(pl.multiple_of(r * SUB, SUB), SUB), :] = d
            return 0
        lax.fori_loop(0, LANE // SUB, tile_d, 0)
        one = (dmat[...] == 1).astype(F32).astype(BF16)
        zero = jnp.zeros((LANE, LANE), BF16)
        adj[0:LANE, 0:LANE] = one
        adj[0:LANE, LANE:] = zero
        adj[LANE:, 0:LANE] = zero
        adj[LANE:, LANE:] = one
        for s in range(num_sets):
            for l in range(num_layers):
                k = s * num_layers + l
                sin_h, cos_h = sincos(jnp.full((SUB, LANE), 0.5 * beta_ref[s, l], F32))
                ct[k, 0] = cos_h
                ct[k, 1] = sin_h
                ct[k, 2] = -sin_h

        def weights(k, slot):
            c, t = ct[k, 0], ct[k, 1]
            cp, tp = [jnp.ones_like(c)], [jnp.ones_like(c)]
            for _ in range(LANE_BITS):
                cp.append(cp[-1] * c)
                tp.append(tp[-1] * t)
            amp = [cp[LANE_BITS - d] * tp[d] for d in range(LANE_BITS + 1)]
            z = jnp.zeros_like(c)
            real = [z, z, z, z, z, z, z, z]
            imag = [z, z, z, z, z, z, z, z]
            for d in range(LANE_BITS + 1):
                if d % 4 == 0:
                    real[d] = amp[d]
                elif d % 4 == 1:
                    imag[d] = -amp[d]
                elif d % 4 == 2:
                    real[d] = -amp[d]
                else:
                    imag[d] = amp[d]

            def body(r, _):
                at = pl.multiple_of(r * 2 * SUB, 2 * SUB)
                rows_re, rows_im = [], []
                for h in range(2):
                    d = dmat[pl.ds(at + h * SUB, SUB), :]
                    re = z
                    im = z
                    for j in range(LANE_BITS + 1):
                        hit = d == j
                        if j % 2 == 0:
                            re = jnp.where(hit, real[j], re)
                        else:
                            im = jnp.where(hit, imag[j], im)
                    rows_re.append(re)
                    rows_im.append(im)
                re = jnp.concatenate(rows_re, axis=0)
                im = jnp.concatenate(rows_im, axis=0)
                for p, (a, b) in enumerate(zip(split3(re), split3(im))):
                    top = pl.ds(at, 2 * SUB)
                    bot = pl.ds(at + LANE, 2 * SUB)
                    wmat[slot, 0, p, top, 0:LANE] = a
                    wmat[slot, 0, p, top, LANE:] = b
                    wmat[slot, 0, p, bot, 0:LANE] = -b
                    wmat[slot, 0, p, bot, LANE:] = a
                    wmat[slot, 1, p, top, 0:LANE] = a
                    wmat[slot, 1, p, top, LANE:] = -b
                    wmat[slot, 1, p, bot, 0:LANE] = b
                    wmat[slot, 1, p, bot, LANE:] = a
                return 0
            lax.fori_loop(0, LANE // (2 * SUB), body, 0)

        def tile_rows(tile):
            return pl.ds(pl.multiple_of(tile * SUB, SUB), SUB)

        def load(ref, slot, tile):
            r = tile_rows(tile)
            return ref[slot, r, 0:LANE], ref[slot, r, LANE:]

        def store(ref, slot, tile, pair):
            r = tile_rows(tile)
            ref[slot, r, 0:LANE] = pair[0]
            ref[slot, r, LANE:] = pair[1]

        def mix_low(source, target, k, sign):
            c, t = ct[k, 0], ct[k, sign]

            def body(i, _):
                base, tile = (i // tiles) * lo, i % tiles
                v = [load(source, base + j, tile) for j in range(lo)]
                for b in lo_bits:
                    v = rot(v, b, c, t)
                for j in range(lo):
                    store(target, base + j, tile, v[j])
                return 0
            lax.fori_loop(0, hi * tiles, body, 0, unroll=2)

        def mid_pass(source, target, k_in, s_in, k_out, s_out, middle):
            if k_in is not None:
                c0, t0 = ct[k_in, 0], ct[k_in, s_in]
            if k_out is not None:
                c1, t1 = ct[k_out, 0], ct[k_out, s_out]

            def body(i, carry):
                base, tile = i // tiles, i % tiles
                slots = [base + j * lo for j in range(hi)]
                if source is None:
                    v = [None] * hi
                else:
                    v = [load(source, m, tile) for m in slots]
                if k_in is not None:
                    for b in hi_bits:
                        v = rot(v, b, c0, t0)
                v, carry = middle(v, slots, tile, carry)
                if k_out is not None:
                    for b in hi_bits:
                        v = rot(v, b, c1, t1)
                    for j in range(hi):
                        store(target, slots[j], tile, v[j])
                return carry
            return lax.fori_loop(0, lo * tiles, body, jnp.zeros((SUB, LANE), F32), unroll=2)

        def pre_mix_send(source, e, s, k, sign):
            c, t = ct[k, 0], ct[k, sign]
            half = n // 2

            def rows_body(i, _):
                base = i * lo
                v = [load(source, base + j // tiles, j % tiles) for j in range(lo * tiles)]
                for b in lo_bits:
                    v = rot(v, b * tiles, c, t)
                for b in tile_bits:
                    v = rot(v, b, c, t)
                for j in range(lo * tiles):
                    re, im = v[j]
                    for b in range(3):
                        fr, fi = sub_flip(re, b), sub_flip(im, b)
                        re, im = c * re + t * fi, c * im - t * fr
                    m = j // tiles
                    store(tmp, (m % 2) * half + i * (lo // 2) + m // 2, j % tiles, (re, im))
                return 0
            lax.fori_loop(0, hi, rows_body, 0)

            def lanes(core):
                at = pl.ds(pl.multiple_of(core * half, half), half)
                m = half * rows
                x = tmp[at].reshape(m, 2 * LANE)
                xh, xm, xl = split3(x)
                w = [wmat[k, sign - 1, p] for p in range(3)]
                a = mm(jnp.concatenate([xh, xm, xl], axis=0), w[0])
                b = mm(jnp.concatenate([xh, xm], axis=0), w[1])
                y = a[:m] + (b[:m] + a[m:2 * m]) + (mm(xh, w[2]) + b[m:] + a[2 * m:])
                src[e, s, at] = y.reshape(half, rows, 2 * LANE)

            def send_slot(ty, tx, part):
                r = pl.ds(part * SUB, SUB)
                send(src.at[e, s, by_core(ty, tx), r], dst.at[e, s, me, r], (e, s), ty, tx)
            other_core = lax.rem(me_core + 1, 2)
            lanes(other_core)
            lanes(me_core)
            def near(order, want):
                return [o for o in order if (o[0] == 0 or o[1] == 0) == want]
            peers_in_order(send_slot, near(ORDER_OTHER, True), other_core)
            peers_in_order(send_slot, near(ORDER_LIKE, True), me_core)

            @pl.when(e + s == 0)
            def _():
                hear_rows()
            peers_in_order(send_slot, near(ORDER_OTHER, False), other_core)
            peers_in_order(send_slot, near(ORDER_LIKE, False), me_core)
            dst[e, s, me] = src[e, s, by_core(qy, qx)]

        def im_dot(a, b):
            return a[0] * b[1] - a[1] * b[0]

        def slot_dot(bra, ket):
            def group(slots, tile, bits, a):
                x = [load(bra, m, tile) for m in slots]
                y = [load(ket, m, tile) for m in slots]
                for j in range(len(slots)):
                    re = sum(y[j ^ b][0] for b in bits[1:]) + y[j ^ bits[0]][0] if len(bits) > 1 else y[j ^ bits[0]][0]
                    im = sum(y[j ^ b][1] for b in bits[1:]) + y[j ^ bits[0]][1] if len(bits) > 1 else y[j ^ bits[0]][1]
                    a = a + im_dot(x[j], (re, im))
                return a

            def low(i, a):
                return group([(i // tiles) * lo + j for j in range(lo)], i % tiles, lo_bits, a)

            def high(i, a):
                return group([i // tiles + j * lo for j in range(hi)], i % tiles, hi_bits, a)
            a = lax.fori_loop(0, hi * tiles, low, jnp.zeros((SUB, LANE), F32))
            return lax.fori_loop(0, lo * tiles, high, a)

        def fold(x):
            while x.shape[0] > SUB:
                half = x.shape[0] // 2
                x = x[:half] + x[half:]
            return x

        def inner_x(x):
            xh, xm, xl = split3(x)
            y = mm(xh, adj[...]) + mm(xm, adj[...]) + mm(xl, adj[...])
            return y

        def tile_flips(v):
            out = []
            for j in range(len(v)):
                parts_ = []
                for comp in range(2):
                    x = v[j][comp]
                    f = sub_flip(x, 0) + sub_flip(x, 1) + sub_flip(x, 2)
                    for b in tile_bits:
                        f = f + v[j ^ b][comp]
                    parts_.append(f)
                out.append(tuple(parts_))
            return out

        def inner_apply(ket, target):
            def body(i, _):
                at = pl.ds(pl.multiple_of(i * lo, lo), lo)
                y = inner_x(ket[at].reshape(lo * rows, 2 * LANE))
                target[at] = y.reshape(lo, rows, 2 * LANE)
                return 0
            lax.fori_loop(0, hi, body, 0)

            def add(i, _):
                v = [load(ket, i, j) for j in range(tiles)]
                f = tile_flips(v)
                for j in range(tiles):
                    y = load(target, i, j)
                    store(target, i, j, (y[0] + f[j][0], y[1] + f[j][1]))
                return 0
            lax.fori_loop(0, n, add, 0)

        def inner_dots(bra, ket, cost):
            inner_apply(ket, tmp)

            def body(i, carry):
                a, g = carry
                for j in range(tiles):
                    x = load(bra, i, j)
                    a = a + im_dot(x, load(tmp, i, j))
                    g = g + cost[i, tile_rows(j), :] * im_dot(x, load(ket, i, j))
                return a, g
            z = jnp.zeros((SUB, LANE), F32)
            return lax.fori_loop(0, n, body, (z, z))

        def two_dots(bra, ket_b, ket_c):
            def body(i, carry):
                a, g = carry
                for j in range(tiles):
                    x = load(bra, i, j)
                    a = a + im_dot(x, load(ket_b, i, j))
                    g = g + im_dot(x, load(ket_c, i, j))
                return a, g
            z = jnp.zeros((SUB, LANE), F32)
            return lax.fori_loop(0, n, body, (z, z), unroll=8)

        def slot_x(source, target):
            def low(i, _):
                base, tile = (i // tiles) * lo, i % tiles
                y = [load(source, base + j, tile) for j in range(lo)]
                for j in range(lo):
                    o = load(target, base + j, tile)
                    store(target, base + j, tile, tuple(o[c] + (y[j ^ 1][c] + y[j ^ 2][c] + y[j ^ 4][c]) for c in range(2)))
                return 0
            lax.fori_loop(0, hi * tiles, low, 0)

            def high(i, _):
                base, tile = i // tiles, i % tiles
                y = [load(source, base + j * lo, tile) for j in range(hi)]
                for j in range(hi):
                    o = load(target, base + j * lo, tile)
                    store(target, base + j * lo, tile, tuple(o[c] + (y[j ^ 1][c] + y[j ^ 2][c]) for c in range(2)))
                return 0
            lax.fori_loop(0, lo * tiles, high, 0)

        def slot_mix_all(ref, k):
            mix_low(ref, ref, k, 1)
            mid_pass(ref, ref, None, 1, k, 1, lambda v, slots, tile, a: (v, a))

        def fill_table(ref, cost, s, l, scale):
            g = gamma_ref[s, l]

            def body(i, _):
                for j in range(tiles):
                    sn, cs = sincos(cost[i, tile_rows(j), :] * g)
                    if scale is None:
                        store(ref, i, j, (cs, sn))
                    else:
                        store(ref, i, j, (cs * scale, sn * -scale))
                return 0
            lax.fori_loop(0, n, body, 0)

        def kk(s, l):
            return s * num_layers + l

        def add_acc(s, q, a, init=False):
            row = s * 8 + q
            acc[row] = a if init else acc[row] + a


        def each_set(f):
            lax.fori_loop(0, num_sets, lambda s, _: (f(s), 0)[1], 0)

        def first_state(s):
            weights(kk(s, 0), kk(s, 0))
            fill_table(keep.at[0, s], cost_ref, s, 0, norm)

        first_state(0)
        pl.semaphore_wait(barrier, nx - 1 + 2 * (ny - 1))

        def tell(i, _):
            pl.semaphore_signal(row_sem, inc=1, device_id={'qy': lax.rem(qy + i, ny), 'qx': qx}, device_id_type=MESH_ID)
            return 0
        lax.fori_loop(1, ny, tell, 0)

        def send_cost(ty, tx):
            send(cost_ref.at[ty * nx + tx], cost_b.at[me], (6, 0), ty, tx)
        line_peers(send_cost)
        cost_b[me] = cost_ref[me]

        def hear_rows():
            pl.semaphore_wait(row_sem, ny - 1)
            cross_peers(send_cost)


        def set_weights(i, _):
            k = (i // (num_layers - 1)) * num_layers + 1 + i % (num_layers - 1)
            weights(k, k)
            return 0

        def forward_mid(before, after, table):
            def middle(v, slots, tile, a):
                out = []
                for m, (re, im) in zip(slots, v):
                    store(before, m, tile, (re, im))
                    cs, sn = load(table, m, tile)
                    p = (re * cs + im * sn, im * cs - re * sn)
                    store(after, m, tile, p)
                    out.append(p)
                return out, a
            return middle

        def backward_mid(before, after, table):
            def middle(v, slots, tile, a):
                out = []
                for m, (re, im) in zip(slots, v):
                    store(before, m, tile, (re, im))
                    cs, sn = load(table, m, tile)
                    p = (re * cs - im * sn, im * cs + re * sn)
                    store(after, m, tile, p)
                    out.append(p)
                return out, a
            return middle

        def turn_mid(psi, lam):
            def middle(v, slots, tile, a):
                out = []
                for m, (re, im) in zip(slots, v):
                    store(psi, m, tile, (re, im))
                    w = cost_b[m, tile_rows(tile), :]
                    p = (w * re, w * im)
                    a = a + (p[0] * re + p[1] * im)
                    store(lam, m, tile, p)
                    out.append(p)
                return out, a
            return middle

        def stage(e, s):
            k_out = kk(s, e - (e // 3) * (2 * e - 5))
            s_out = 1 + e // 3
            k_in = kk(s, e - 1 - (e // 4) * (2 * e - 7))
            s_in = 1 + e // 4
            before, after = keep.at[2 * e - 1, s], keep.at[2 * e, s]

            @pl.when(e == 0)
            def _():
                @pl.when(s > 0)
                def _():
                    first_state(s)
                mid_pass(keep.at[0, s], other, None, 1, k_out, s_out, lambda v, slots, tile, a: (v, a))

            @pl.when(e > 0)
            def _():
                wait_bytes(dst.at[e - 1, s], recv_sem.at[e - 1, s])
                mix_low(dst.at[e - 1, s], other, k_in, s_in)

                @pl.when(e < 3)
                def _():
                    mid_pass(other, other, k_in, s_in, k_out, s_out, forward_mid(before, after, tab.at[e - 1, s]))

                @pl.when(e == 3)
                def _():
                    add_acc(s, 0, mid_pass(other, other, k_in, s_in, k_out, s_out, turn_mid(before, after)), True)

                @pl.when(e > 3)
                def _():
                    mid_pass(other, other, k_in, s_in, k_out, s_out, backward_mid(before, after, tab.at[5 - e, s]))

            pre_mix_send(other, e, s, k_out, s_out)

            @pl.when(e * num_sets + s == 1)
            def _():
                lax.fori_loop(0, num_sets * (num_layers - 1), set_weights, 0)
                each_set(lambda i: fill_table(tab.at[1, i], cost_ref, i, 2, None))
                wait_bytes(cost_b, recv_sem.at[6, 0])
                each_set(lambda i: fill_table(tab.at[0, i], cost_b, i, 1, None))

            @pl.when(e == 2)
            def _():
                inner_apply(keep.at[0, s], psi_b.at[s])
                slot_x(keep.at[0, s], psi_b.at[s])
                slot_mix_all(psi_b.at[s], kk(s, 0))

                def times_cost(i, _):
                    for j in range(tiles):
                        re, im = load(keep.at[0, s], i, j)
                        w = cost_ref[i, tile_rows(j), :]
                        store(psi_c.at[s], i, j, (w * re, w * im))
                    return 0
                lax.fori_loop(0, n, times_cost, 0)
                slot_mix_all(psi_c.at[s], kk(s, 0))

            @pl.when(e == 3)
            def _():
                add_acc(s, 6, slot_dot(after, before), True)

            @pl.when(e > 3)
            def _():
                ket = keep.at[12 - 2 * e, s]
                ket_before = keep.at[11 - 2 * e, s]

                def add_dots(cost):
                    b, g = inner_dots(before, ket, cost)
                    acc[s * 8 + 10 - e] = acc[s * 8 + 10 - e] + (b + slot_dot(before, ket))
                    acc[s * 8 + 7 - e] = 2.0 * g
                    acc[s * 8 + 9 - e] = slot_dot(after, ket_before)
                pl.when(e == 4)(lambda: add_dots(cost_ref))
                pl.when(e == 5)(lambda: add_dots(cost_b))

        def each_exchange(e, _):
            each_set(lambda s: stage(e, s))
            return 0
        lax.fori_loop(0, 2 * num_layers, each_exchange, 0)

        lane = lax.broadcasted_iota(jnp.int32, (1, LANE), 1)

        def place(q, a):
            total = jnp.sum(jnp.sum(a, axis=0, keepdims=True), axis=1, keepdims=True)
            return jnp.where(lane == q, total, 0.0)

        def partial(s):
            wait_bytes(dst.at[5, s], recv_sem.at[5, s])
            b, g = two_dots(dst.at[5, s], psi_b.at[s], psi_c.at[s])
            return place(4, acc[s * 8 + 4] + b) + place(1, 2.0 * g)

        rest = []
        for s in range(num_sets):
            rest.append(sum(place(q, acc[s * 8 + q]) for q in (2, 3, 5, 6)) + place(0, acc[s * 8]))
        for s in range(num_sets):
            mine[s:s + 1, :] = rest[s] + partial(s)

        parts[me] = mine[...]
        each_peer_far_first(lambda ty, tx: send(mine, parts.at[me], (6, 1), ty, tx))
        wait_bytes(parts, recv_sem.at[6, 1])
        out_ref[...] = jnp.sum(parts[...], axis=0)
        for e in range(6):
            for s in range(num_sets):
                wait_bytes(src.at[e, s], send_sem.at[e, s])
        wait_bytes(cost_b, send_sem.at[6, 0])
        wait_bytes(parts, send_sem.at[6, 1])

    return kernel


def solution(mesh):
    ny, nx = mesh.shape['qy'], mesh.shape['qx']
    n = ny * nx

    def device_fn(cost, gamma, beta):
        size = cost.shape[0]
        num_sets, num_layers = gamma.shape
        rows = size // (LANE * n)
        bits = (size * n).bit_length() - 1
        norm = 2.0 ** (-0.5 * bits)
        state = (n, rows, 2 * LANE)
        smem = pl.BlockSpec(memory_space=pltpu.SMEM)
        parts = pl.pallas_call(
            make_kernel(ny, nx, num_sets, num_layers, rows, norm),
            out_shape=jax.ShapeDtypeStruct((num_sets, LANE), F32),
            in_specs=[pl.BlockSpec(memory_space=pltpu.VMEM), smem, smem],
            out_specs=pl.BlockSpec(memory_space=pltpu.VMEM),
            scratch_shapes=[
                pltpu.VMEM((n, rows, LANE), F32),
                pltpu.VMEM((6, num_sets) + state, F32),
                pltpu.VMEM((6, num_sets) + state, F32),
                pltpu.VMEM((11, num_sets) + state, F32),
                pltpu.VMEM((2, num_sets) + state, F32),
                pltpu.VMEM((num_sets,) + state, F32),
                pltpu.VMEM((num_sets,) + state, F32),
                pltpu.VMEM((num_sets * num_layers, 2, 3, 2 * LANE, 2 * LANE), BF16),
                pltpu.VMEM((2 * LANE, 2 * LANE), BF16),
                pltpu.VMEM((LANE, LANE), jnp.int32),
                pltpu.VMEM((num_sets * num_layers, 3, SUB, LANE), F32),
                pltpu.VMEM((num_sets * 8, SUB, LANE), F32),
                pltpu.VMEM((num_sets, LANE), F32),
                pltpu.VMEM((n, num_sets, LANE), F32),
                pltpu.VMEM(state, F32),
                pltpu.VMEM(state, F32),
                pltpu.SemaphoreType.DMA((7, 2)),
                pltpu.SemaphoreType.DMA((7, 2)),
                pltpu.SemaphoreType.REGULAR,
            ],
            compiler_params=pltpu.CompilerParams(collective_id=0, has_side_effects=True, vmem_limit_bytes=60 * 2 ** 20),
            name='qaoa',
        )(cost.reshape(n, rows, LANE), gamma, beta)

        def finish(parts_ref, e_ref, g_ref):
            for s in range(num_sets):
                e_ref[s] = parts_ref[s, 0]
                for q in range(2 * num_layers):
                    g_ref[s, q] = parts_ref[s, 1 + q]

        return pl.pallas_call(
            finish,
            out_shape=(jax.ShapeDtypeStruct((num_sets,), F32), jax.ShapeDtypeStruct((num_sets, 2 * num_layers), F32)),
            in_specs=[smem],
            out_specs=(smem, smem),
            name='finish',
        )(parts)

    cost_spec = P(('inst', 'qy', 'qx'))
    angle_spec = P('inst', None)
    return jax.shard_map(device_fn, mesh=mesh, in_specs=(cost_spec, angle_spec, angle_spec), out_specs=(P('inst'), angle_spec), check_vma=False)
```

```python
import functools
import jax
import jax.numpy as jnp
from jax import lax
from jax.experimental import pallas as pl
from jax.experimental.pallas import tpu as pltpu
from jax.sharding import PartitionSpec as P

LANE = 128
LANE_BITS = 7
SUB = 8
ORDER_OTHER = [(1, 1), (1, 3), (1, 2), (1, 0), (2, 1), (2, 3), (2, 2), (2, 0), (3, 1), (3, 3), (3, 2), (3, 0), (0, 1), (0, 3), (0, 2), (0, 0)]
ORDER_LIKE = [(1, 1), (1, 3), (1, 2), (1, 0), (2, 1), (2, 3), (2, 2), (2, 0), (3, 1), (3, 3), (3, 2), (3, 0), (0, 1), (0, 3), (0, 2)]
MESH_ID = pl.DeviceIdType.MESH
F32 = jnp.float32
BF16 = jnp.bfloat16


def sincos(x):
    k = jnp.floor(x * 0.6366197723675814 + 0.5)
    r = ((x - k * 1.5703125) - k * 4.837512969970703125e-4) - k * 7.54978995489188216e-8
    z = r * r
    s = r + r * z * (-1.6666654611e-1 + z * (8.3321608736e-3 + z * -1.9515295891e-4))
    c = (1.0 - 0.5 * z) + z * z * (4.166664568298827e-2 + z * (-1.388731625493765e-3 + z * 2.443315711809948e-5))
    q = k.astype(jnp.int32)
    odd = (q & 1) != 0
    sin_v = jnp.where(odd, c, s)
    cos_v = jnp.where(odd, s, c)
    sin_v = jnp.where((q & 2) != 0, -sin_v, sin_v)
    cos_v = jnp.where(((q + 1) & 2) != 0, -cos_v, cos_v)
    return sin_v, cos_v


def split3(x):
    hi = x.astype(BF16)
    rest = x - hi.astype(F32)
    mid = rest.astype(BF16)
    low = (rest - mid.astype(F32)).astype(BF16)
    return hi, mid, low


def mm(a, b):
    return jnp.dot(a, b, preferred_element_type=F32)


def rot(pairs, stride, c, t):
    out = list(pairs)
    for j in range(len(pairs)):
        if j & stride:
            continue
        (ar, ai), (br, bi) = pairs[j], pairs[j | stride]
        out[j] = (c * ar + t * bi, c * ai - t * br)
        out[j | stride] = (c * br + t * ai, c * bi - t * ar)
    return out


def sub_flip(x, bit):
    if bit == 2:
        return pltpu.roll(x, 4, 0)
    row = lax.broadcasted_iota(jnp.int32, (SUB, LANE), 0)
    up = pltpu.roll(x, 1 << bit, 0)
    down = pltpu.roll(x, SUB - (1 << bit), 0)
    return jnp.where((row & (1 << bit)) != 0, up, down)


def make_kernel(ny, nx, num_sets, num_layers, rows, norm):
    n = ny * nx
    lo = 8
    hi = n // lo
    tiles = rows // SUB
    lo_bits = [1 << b for b in range(lo.bit_length() - 1)]
    hi_bits = [1 << b for b in range(hi.bit_length() - 1)]
    tile_bits = [1 << b for b in range(tiles.bit_length() - 1)]
    width_x = nx // 2

    def kernel(cost_ref, gamma_ref, beta_ref, out_ref,
               cost_b, src, dst, keep, tab, psi_b, psi_c, wmat, adj, dmat, ct, acc, mine, parts, tmp, other, send_sem, recv_sem, row_sem):
        qy = lax.axis_index('qy')
        qx = lax.axis_index('qx')
        me = qy * nx + qx
        barrier = pltpu.get_barrier_semaphore()

        me_core = lax.rem(qx, 2)

        def ring_x(order):
            return [lax.rem(qx // 2 + dx, width_x) * 2 for dx in order]
        chip_x = ring_x((1, 3, 2, 0))
        far_x = ring_x((2, 1, 3, 0))

        def peers_of_core(act, core, last):
            def body(i, _):
                ty = lax.rem(qy + 1 + i, ny)
                for tx in chip_x[:-1]:
                    act(ty, tx + core)

                @pl.when(i + last < ny)
                def _():
                    act(ty, chip_x[-1] + core)
                return 0
            lax.fori_loop(0, ny, body, 0)

        def peers_in_order(act, order, core):
            for part in range(tiles):
                for dy, dx in order:
                    act(lax.rem(qy + dy, ny), lax.rem(qx // 2 + dx, width_x) * 2 + core, part)

        def both_cores(f):
            lax.fori_loop(0, 2, lambda h, _: (f(lax.rem(me_core + 1 + h, 2), h), 0)[1], 0)

        def each_peer(act):
            both_cores(lambda core, last: peers_of_core(act, core, last))

        def each_peer_far_first(act):
            def body(i, _):
                a = i // 2
                ty = lax.rem(qy + 2 - a + (a // 2) * (7 - 2 * a), ny)
                core = lax.rem(qx + 1 + i, 2)
                for tx in far_x[:-1]:
                    act(ty, tx + core)

                @pl.when(i < 2 * ny - 1)
                def _():
                    act(ty, far_x[-1] + core)
                return 0
            lax.fori_loop(0, 2 * ny, body, 0)

        def greet(ty, tx):
            pl.semaphore_signal(barrier, inc=1, device_id={'qy': ty, 'qx': tx}, device_id_type=MESH_ID)
        def line_peers(act):
            def row(i, _):
                act(qy, lax.rem(qx + i, nx))
                return 0
            lax.fori_loop(1, nx, row, 0)

            def column(i, _):
                act(lax.rem(qy + i, ny), qx)
                act(lax.rem(qy + i, ny), qx + 1 - 2 * me_core)
                return 0
            lax.fori_loop(1, ny, column, 0)

        def cross_peers(act):
            def body(i, _):
                ty = lax.rem(qy + 1 + i // 2, ny)
                core = lax.rem(qx + 1 + i, 2)
                for dx in (1, 3, 2):
                    act(ty, lax.rem(qx // 2 + dx, width_x) * 2 + core)
                return 0
            lax.fori_loop(0, 2 * (ny - 1), body, 0)

        line_peers(greet)

        def send(source, target, ids, ty, tx):
            pltpu.make_async_remote_copy(
                source, target, send_sem.at[ids], recv_sem.at[ids],
                device_id={'qy': ty, 'qx': tx}, device_id_type=MESH_ID).start()

        def by_core(ty, tx):
            return lax.rem(tx, 2) * (n // 2) + ty * width_x + tx // 2

        def wait_bytes(buf, sem):
            part = buf.at[pl.ds(0, n - 1)]
            pltpu.make_async_copy(part, part, sem).wait()

        def tile_d(r, _):
            a = lax.broadcasted_iota(jnp.int32, (SUB, LANE), 0) + r * SUB
            b = lax.broadcasted_iota(jnp.int32, (SUB, LANE), 1)
            x = a ^ b
            d = jnp.zeros_like(x)
            for k in range(LANE_BITS):
                d = d + ((x >> k) & 1)
            dmat[pl.ds(pl.multiple_of(r * SUB, SUB), SUB), :] = d
            return 0
        lax.fori_loop(0, LANE // SUB, tile_d, 0)
        one = (dmat[...] == 1).astype(F32).astype(BF16)
        zero = jnp.zeros((LANE, LANE), BF16)
        adj[0:LANE, 0:LANE] = one
        adj[0:LANE, LANE:] = zero
        adj[LANE:, 0:LANE] = zero
        adj[LANE:, LANE:] = one
        for s in range(num_sets):
            for l in range(num_layers):
                k = s * num_layers + l
                sin_h, cos_h = sincos(jnp.full((SUB, LANE), 0.5 * beta_ref[s, l], F32))
                ct[k, 0] = cos_h
                ct[k, 1] = sin_h
                ct[k, 2] = -sin_h

        def weights(k, slot):
            c, t = ct[k, 0], ct[k, 1]
            cp, tp = [jnp.ones_like(c)], [jnp.ones_like(c)]
            for _ in range(LANE_BITS):
                cp.append(cp[-1] * c)
                tp.append(tp[-1] * t)
            amp = [cp[LANE_BITS - d] * tp[d] for d in range(LANE_BITS + 1)]
            z = jnp.zeros_like(c)
            real = [z, z, z, z, z, z, z, z]
            imag = [z, z, z, z, z, z, z, z]
            for d in range(LANE_BITS + 1):
                if d % 4 == 0:
                    real[d] = amp[d]
                elif d % 4 == 1:
                    imag[d] = -amp[d]
                elif d % 4 == 2:
                    real[d] = -amp[d]
                else:
                    imag[d] = amp[d]

            def body(r, _):
                at = pl.multiple_of(r * 2 * SUB, 2 * SUB)
                rows_re, rows_im = [], []
                for h in range(2):
                    d = dmat[pl.ds(at + h * SUB, SUB), :]
                    re = z
                    im = z
                    for j in range(LANE_BITS + 1):
                        hit = d == j
                        if j % 2 == 0:
                            re = jnp.where(hit, real[j], re)
                        else:
                            im = jnp.where(hit, imag[j], im)
                    rows_re.append(re)
                    rows_im.append(im)
                re = jnp.concatenate(rows_re, axis=0)
                im = jnp.concatenate(rows_im, axis=0)
                for p, (a, b) in enumerate(zip(split3(re), split3(im))):
                    top = pl.ds(at, 2 * SUB)
                    bot = pl.ds(at + LANE, 2 * SUB)
                    wmat[slot, 0, p, top, 0:LANE] = a
                    wmat[slot, 0, p, top, LANE:] = b
                    wmat[slot, 0, p, bot, 0:LANE] = -b
                    wmat[slot, 0, p, bot, LANE:] = a
                    wmat[slot, 1, p, top, 0:LANE] = a
                    wmat[slot, 1, p, top, LANE:] = -b
                    wmat[slot, 1, p, bot, 0:LANE] = b
                    wmat[slot, 1, p, bot, LANE:] = a
                return 0
            lax.fori_loop(0, LANE // (2 * SUB), body, 0)

        def tile_rows(tile):
            return pl.ds(pl.multiple_of(tile * SUB, SUB), SUB)

        def load(ref, slot, tile):
            r = tile_rows(tile)
            return ref[slot, r, 0:LANE], ref[slot, r, LANE:]

        def store(ref, slot, tile, pair):
            r = tile_rows(tile)
            ref[slot, r, 0:LANE] = pair[0]
            ref[slot, r, LANE:] = pair[1]

        def mix_low(source, target, k, sign):
            c, t = ct[k, 0], ct[k, sign]

            def body(i, _):
                base, tile = (i // tiles) * lo, i % tiles
                v = [load(source, base + j, tile) for j in range(lo)]
                for b in lo_bits:
                    v = rot(v, b, c, t)
                for j in range(lo):
                    store(target, base + j, tile, v[j])
                return 0
            lax.fori_loop(0, hi * tiles, body, 0, unroll=2)

        def mid_pass(source, target, k_in, s_in, k_out, s_out, middle):
            if k_in is not None:
                c0, t0 = ct[k_in, 0], ct[k_in, s_in]
            if k_out is not None:
                c1, t1 = ct[k_out, 0], ct[k_out, s_out]

            def body(i, carry):
                base, tile = i // tiles, i % tiles
                slots = [base + j * lo for j in range(hi)]
                if source is None:
                    v = [None] * hi
                else:
                    v = [load(source, m, tile) for m in slots]
                if k_in is not None:
                    for b in hi_bits:
                        v = rot(v, b, c0, t0)
                v, carry = middle(v, slots, tile, carry)
                if k_out is not None:
                    for b in hi_bits:
                        v = rot(v, b, c1, t1)
                    for j in range(hi):
                        store(target, slots[j], tile, v[j])
                return carry
            return lax.fori_loop(0, lo * tiles, body, jnp.zeros((SUB, LANE), F32), unroll=2)

        def pre_mix_send(source, e, s, k, sign):
            c, t = ct[k, 0], ct[k, sign]
            half = n // 2

            def rows_body(i, _):
                base = i * lo
                v = [load(source, base + j // tiles, j % tiles) for j in range(lo * tiles)]
                for b in lo_bits:
                    v = rot(v, b * tiles, c, t)
                for b in tile_bits:
                    v = rot(v, b, c, t)
                for j in range(lo * tiles):
                    re, im = v[j]
                    for b in range(3):
                        fr, fi = sub_flip(re, b), sub_flip(im, b)
                        re, im = c * re + t * fi, c * im - t * fr
                    m = j // tiles
                    store(tmp, (m % 2) * half + i * (lo // 2) + m // 2, j % tiles, (re, im))
                return 0
            lax.fori_loop(0, hi, rows_body, 0)

            def lanes(core):
                at = pl.ds(pl.multiple_of(core * half, half), half)
                m = half * rows
                x = tmp[at].reshape(m, 2 * LANE)
                xh, xm, xl = split3(x)
                w = [wmat[k, sign - 1, p] for p in range(3)]
                a = mm(jnp.concatenate([xh, xm, xl], axis=0), w[0])
                b = mm(jnp.concatenate([xh, xm], axis=0), w[1])
                y = a[:m] + (b[:m] + a[m:2 * m]) + (mm(xh, w[2]) + b[m:] + a[2 * m:])
                src[e, s, at] = y.reshape(half, rows, 2 * LANE)

            def send_slot(ty, tx, part):
                r = pl.ds(part * SUB, SUB)
                send(src.at[e, s, by_core(ty, tx), r], dst.at[e, s, me, r], (e, s), ty, tx)
            other_core = lax.rem(me_core + 1, 2)
            lanes(other_core)
            lanes(me_core)
            def near(order, want):
                return [o for o in order if (o[0] == 0 or o[1] == 0) == want]
            peers_in_order(send_slot, near(ORDER_OTHER, True), other_core)
            peers_in_order(send_slot, near(ORDER_LIKE, True), me_core)

            @pl.when(e + s == 0)
            def _():
                hear_rows()
            peers_in_order(send_slot, near(ORDER_OTHER, False), other_core)
            peers_in_order(send_slot, near(ORDER_LIKE, False), me_core)
            dst[e, s, me] = src[e, s, by_core(qy, qx)]

        def im_dot(a, b):
            return a[0] * b[1] - a[1] * b[0]

        def slot_dot(bra, ket):
            def group(slots, tile, bits, a):
                x = [load(bra, m, tile) for m in slots]
                y = [load(ket, m, tile) for m in slots]
                for j in range(len(slots)):
                    re = sum(y[j ^ b][0] for b in bits[1:]) + y[j ^ bits[0]][0] if len(bits) > 1 else y[j ^ bits[0]][0]
                    im = sum(y[j ^ b][1] for b in bits[1:]) + y[j ^ bits[0]][1] if len(bits) > 1 else y[j ^ bits[0]][1]
                    a = a + im_dot(x[j], (re, im))
                return a

            def low(i, a):
                return group([(i // tiles) * lo + j for j in range(lo)], i % tiles, lo_bits, a)

            def high(i, a):
                return group([i // tiles + j * lo for j in range(hi)], i % tiles, hi_bits, a)
            a = lax.fori_loop(0, hi * tiles, low, jnp.zeros((SUB, LANE), F32))
            return lax.fori_loop(0, lo * tiles, high, a)

        def fold(x):
            while x.shape[0] > SUB:
                half = x.shape[0] // 2
                x = x[:half] + x[half:]
            return x

        def inner_x(x):
            xh, xm, xl = split3(x)
            y = mm(xh, adj[...]) + mm(xm, adj[...]) + mm(xl, adj[...])
            return y

        def tile_flips(v):
            out = []
            for j in range(len(v)):
                parts_ = []
                for comp in range(2):
                    x = v[j][comp]
                    f = sub_flip(x, 0) + sub_flip(x, 1) + sub_flip(x, 2)
                    for b in tile_bits:
                        f = f + v[j ^ b][comp]
                    parts_.append(f)
                out.append(tuple(parts_))
            return out

        def inner_apply(ket, target):
            def body(i, _):
                at = pl.ds(pl.multiple_of(i * lo, lo), lo)
                y = inner_x(ket[at].reshape(lo * rows, 2 * LANE))
                target[at] = y.reshape(lo, rows, 2 * LANE)
                return 0
            lax.fori_loop(0, hi, body, 0)

            def add(i, _):
                v = [load(ket, i, j) for j in range(tiles)]
                f = tile_flips(v)
                for j in range(tiles):
                    y = load(target, i, j)
                    store(target, i, j, (y[0] + f[j][0], y[1] + f[j][1]))
                return 0
            lax.fori_loop(0, n, add, 0)

        def inner_dots(bra, ket, cost):
            inner_apply(ket, tmp)

            def body(i, carry):
                a, g = carry
                for j in range(tiles):
                    x = load(bra, i, j)
                    a = a + im_dot(x, load(tmp, i, j))
                    g = g + cost[i, tile_rows(j), :] * im_dot(x, load(ket, i, j))
                return a, g
            z = jnp.zeros((SUB, LANE), F32)
            return lax.fori_loop(0, n, body, (z, z))

        def two_dots(bra, ket_b, ket_c):
            def body(i, carry):
                a, g = carry
                for j in range(tiles):
                    x = load(bra, i, j)
                    a = a + im_dot(x, load(ket_b, i, j))
                    g = g + im_dot(x, load(ket_c, i, j))
                return a, g
            z = jnp.zeros((SUB, LANE), F32)
            return lax.fori_loop(0, n, body, (z, z), unroll=8)

        def slot_x(source, target):
            def low(i, _):
                base, tile = (i // tiles) * lo, i % tiles
                y = [load(source, base + j, tile) for j in range(lo)]
                for j in range(lo):
                    o = load(target, base + j, tile)
                    store(target, base + j, tile, tuple(o[c] + (y[j ^ 1][c] + y[j ^ 2][c] + y[j ^ 4][c]) for c in range(2)))
                return 0
            lax.fori_loop(0, hi * tiles, low, 0)

            def high(i, _):
                base, tile = i // tiles, i % tiles
                y = [load(source, base + j * lo, tile) for j in range(hi)]
                for j in range(hi):
                    o = load(target, base + j * lo, tile)
                    store(target, base + j * lo, tile, tuple(o[c] + (y[j ^ 1][c] + y[j ^ 2][c]) for c in range(2)))
                return 0
            lax.fori_loop(0, lo * tiles, high, 0)

        def slot_mix_all(ref, k):
            mix_low(ref, ref, k, 1)
            mid_pass(ref, ref, None, 1, k, 1, lambda v, slots, tile, a: (v, a))

        def fill_table(ref, cost, s, l, scale):
            g = gamma_ref[s, l]

            def body(i, _):
                for j in range(tiles):
                    sn, cs = sincos(cost[i, tile_rows(j), :] * g)
                    if scale is None:
                        store(ref, i, j, (cs, sn))
                    else:
                        store(ref, i, j, (cs * scale, sn * -scale))
                return 0
            lax.fori_loop(0, n, body, 0)

        def kk(s, l):
            return s * num_layers + l

        def add_acc(s, q, a, init=False):
            row = s * 8 + q
            acc[row] = a if init else acc[row] + a


        def each_set(f):
            lax.fori_loop(0, num_sets, lambda s, _: (f(s), 0)[1], 0)

        def first_state(s):
            weights(kk(s, 0), kk(s, 0))
            fill_table(keep.at[0, s], cost_ref, s, 0, norm)

        first_state(0)
        pl.semaphore_wait(barrier, nx - 1 + 2 * (ny - 1))

        def tell(i, _):
            pl.semaphore_signal(row_sem, inc=1, device_id={'qy': lax.rem(qy + i, ny), 'qx': qx}, device_id_type=MESH_ID)
            return 0
        lax.fori_loop(1, ny, tell, 0)

        def send_cost(ty, tx):
            send(cost_ref.at[ty * nx + tx], cost_b.at[me], (6, 0), ty, tx)
        line_peers(send_cost)
        cost_b[me] = cost_ref[me]

        def hear_rows():
            pl.semaphore_wait(row_sem, ny - 1)
            cross_peers(send_cost)


        def set_weights(i, _):
            k = (i // (num_layers - 1)) * num_layers + 1 + i % (num_layers - 1)
            weights(k, k)
            return 0

        def forward_mid(before, after, table):
            def middle(v, slots, tile, a):
                out = []
                for m, (re, im) in zip(slots, v):
                    store(before, m, tile, (re, im))
                    cs, sn = load(table, m, tile)
                    p = (re * cs + im * sn, im * cs - re * sn)
                    store(after, m, tile, p)
                    out.append(p)
                return out, a
            return middle

        def backward_mid(before, after, table):
            def middle(v, slots, tile, a):
                out = []
                for m, (re, im) in zip(slots, v):
                    store(before, m, tile, (re, im))
                    cs, sn = load(table, m, tile)
                    p = (re * cs - im * sn, im * cs + re * sn)
                    store(after, m, tile, p)
                    out.append(p)
                return out, a
            return middle

        def turn_mid(psi, lam):
            def middle(v, slots, tile, a):
                out = []
                for m, (re, im) in zip(slots, v):
                    store(psi, m, tile, (re, im))
                    w = cost_b[m, tile_rows(tile), :]
                    p = (w * re, w * im)
                    a = a + (p[0] * re + p[1] * im)
                    store(lam, m, tile, p)
                    out.append(p)
                return out, a
            return middle

        def stage(e, s):
            k_out = kk(s, e - (e // 3) * (2 * e - 5))
            s_out = 1 + e // 3
            k_in = kk(s, e - 1 - (e // 4) * (2 * e - 7))
            s_in = 1 + e // 4
            before, after = keep.at[2 * e - 1, s], keep.at[2 * e, s]

            @pl.when(e == 0)
            def _():
                @pl.when(s > 0)
                def _():
                    first_state(s)
                mid_pass(keep.at[0, s], other, None, 1, k_out, s_out, lambda v, slots, tile, a: (v, a))

            @pl.when(e > 0)
            def _():
                wait_bytes(dst.at[e - 1, s], recv_sem.at[e - 1, s])
                mix_low(dst.at[e - 1, s], other, k_in, s_in)

                @pl.when(e < 3)
                def _():
                    mid_pass(other, other, k_in, s_in, k_out, s_out, forward_mid(before, after, tab.at[e - 1, s]))

                @pl.when(e == 3)
                def _():
                    add_acc(s, 0, mid_pass(other, other, k_in, s_in, k_out, s_out, turn_mid(before, after)), True)

                @pl.when(e > 3)
                def _():
                    mid_pass(other, other, k_in, s_in, k_out, s_out, backward_mid(before, after, tab.at[5 - e, s]))

            pre_mix_send(other, e, s, k_out, s_out)

            @pl.when(e * num_sets + s == 1)
            def _():
                lax.fori_loop(0, num_sets * (num_layers - 1), set_weights, 0)
                each_set(lambda i: fill_table(tab.at[1, i], cost_ref, i, 2, None))
                wait_bytes(cost_b, recv_sem.at[6, 0])
                each_set(lambda i: fill_table(tab.at[0, i], cost_b, i, 1, None))

            @pl.when(e == 2)
            def _():
                inner_apply(keep.at[0, s], psi_b.at[s])
                slot_x(keep.at[0, s], psi_b.at[s])
                slot_mix_all(psi_b.at[s], kk(s, 0))

                def times_cost(i, _):
                    for j in range(tiles):
                        re, im = load(keep.at[0, s], i, j)
                        w = cost_ref[i, tile_rows(j), :]
                        store(psi_c.at[s], i, j, (w * re, w * im))
                    return 0
                lax.fori_loop(0, n, times_cost, 0)
                slot_mix_all(psi_c.at[s], kk(s, 0))

            @pl.when(e == 3)
            def _():
                add_acc(s, 6, slot_dot(after, before), True)

            @pl.when(e > 3)
            def _():
                ket = keep.at[12 - 2 * e, s]
                ket_before = keep.at[11 - 2 * e, s]

                def add_dots(cost):
                    b, g = inner_dots(before, ket, cost)
                    acc[s * 8 + 10 - e] = acc[s * 8 + 10 - e] + (b + slot_dot(before, ket))
                    acc[s * 8 + 7 - e] = 2.0 * g
                    acc[s * 8 + 9 - e] = slot_dot(after, ket_before)
                pl.when(e == 4)(lambda: add_dots(cost_ref))
                pl.when(e == 5)(lambda: add_dots(cost_b))

        def each_exchange(e, _):
            each_set(lambda s: stage(e, s))
            return 0
        lax.fori_loop(0, 2 * num_layers, each_exchange, 0)

        lane = lax.broadcasted_iota(jnp.int32, (1, LANE), 1)

        def place(q, a):
            total = jnp.sum(jnp.sum(a, axis=0, keepdims=True), axis=1, keepdims=True)
            return jnp.where(lane == q, total, 0.0)

        def partial(s):
            wait_bytes(dst.at[5, s], recv_sem.at[5, s])
            b, g = two_dots(dst.at[5, s], psi_b.at[s], psi_c.at[s])
            return place(4, acc[s * 8 + 4] + b) + place(1, 2.0 * g)

        rest = []
        for s in range(num_sets):
            rest.append(sum(place(q, acc[s * 8 + q]) for q in (2, 3, 5, 6)) + place(0, acc[s * 8]))
        for s in range(num_sets):
            mine[s:s + 1, :] = rest[s] + partial(s)

        parts[me] = mine[...]
        each_peer_far_first(lambda ty, tx: send(mine, parts.at[me], (6, 1), ty, tx))
        for e in range(6):
            for s in range(num_sets):
                wait_bytes(src.at[e, s], send_sem.at[e, s])
        wait_bytes(cost_b, send_sem.at[6, 0])
        wait_bytes(parts, recv_sem.at[6, 1])
        out_ref[...] = jnp.sum(parts[...], axis=0)
        wait_bytes(parts, send_sem.at[6, 1])

    return kernel


def solution(mesh):
    ny, nx = mesh.shape['qy'], mesh.shape['qx']
    n = ny * nx

    def device_fn(cost, gamma, beta):
        size = cost.shape[0]
        num_sets, num_layers = gamma.shape
        rows = size // (LANE * n)
        bits = (size * n).bit_length() - 1
        norm = 2.0 ** (-0.5 * bits)
        state = (n, rows, 2 * LANE)
        smem = pl.BlockSpec(memory_space=pltpu.SMEM)
        parts = pl.pallas_call(
            make_kernel(ny, nx, num_sets, num_layers, rows, norm),
            out_shape=jax.ShapeDtypeStruct((num_sets, LANE), F32),
            in_specs=[pl.BlockSpec(memory_space=pltpu.VMEM), smem, smem],
            out_specs=pl.BlockSpec(memory_space=pltpu.VMEM),
            scratch_shapes=[
                pltpu.VMEM((n, rows, LANE), F32),
                pltpu.VMEM((6, num_sets) + state, F32),
                pltpu.VMEM((6, num_sets) + state, F32),
                pltpu.VMEM((11, num_sets) + state, F32),
                pltpu.VMEM((2, num_sets) + state, F32),
                pltpu.VMEM((num_sets,) + state, F32),
                pltpu.VMEM((num_sets,) + state, F32),
                pltpu.VMEM((num_sets * num_layers, 2, 3, 2 * LANE, 2 * LANE), BF16),
                pltpu.VMEM((2 * LANE, 2 * LANE), BF16),
                pltpu.VMEM((LANE, LANE), jnp.int32),
                pltpu.VMEM((num_sets * num_layers, 3, SUB, LANE), F32),
                pltpu.VMEM((num_sets * 8, SUB, LANE), F32),
                pltpu.VMEM((num_sets, LANE), F32),
                pltpu.VMEM((n, num_sets, LANE), F32),
                pltpu.VMEM(state, F32),
                pltpu.VMEM(state, F32),
                pltpu.SemaphoreType.DMA((7, 2)),
                pltpu.SemaphoreType.DMA((7, 2)),
                pltpu.SemaphoreType.REGULAR,
            ],
            compiler_params=pltpu.CompilerParams(collective_id=0, has_side_effects=True, vmem_limit_bytes=60 * 2 ** 20),
            name='qaoa',
        )(cost.reshape(n, rows, LANE), gamma, beta)

        def finish(parts_ref, e_ref, g_ref):
            for s in range(num_sets):
                e_ref[s] = parts_ref[s, 0]
                for q in range(2 * num_layers):
                    g_ref[s, q] = parts_ref[s, 1 + q]

        return pl.pallas_call(
            finish,
            out_shape=(jax.ShapeDtypeStruct((num_sets,), F32), jax.ShapeDtypeStruct((num_sets, 2 * num_layers), F32)),
            in_specs=[smem],
            out_specs=(smem, smem),
            name='finish',
        )(parts)

    cost_spec = P(('inst', 'qy', 'qx'))
    angle_spec = P('inst', None)
    return jax.shard_map(device_fn, mesh=mesh, in_specs=(cost_spec, angle_spec, angle_spec), out_specs=(P('inst'), angle_spec), check_vma=False)
```
